32 devices in a mesh: dp: 1 (over z), tp: 4 (over y), ep: 8 (over x, core).
Axes of the slice: x: 4, y: 4, z: 1, core: 2. Of those that a mesh axis runs over, the one named last changes fastest.
The devices are a block of a 4x4x8 slice.
Arguments:
- tokens_in: bfloat16 [1024, 2048], P(('dp', 'ep', 'tp'))
- expert_ids: int32 [1024, 8], P(('dp', 'ep', 'tp'))
- router_gates: float32 [1024, 8], P(('dp', 'ep', 'tp'))
- w_gate: bfloat16 [64, 2048, 1024], P('ep', None, 'tp')
- w_up: bfloat16 [64, 2048, 1024], P('ep', None, 'tp')
- w_down: bfloat16 [64, 1024, 2048], P('ep', 'tp')
Outputs:
- output: bfloat16 [1024, 2048], P(('dp', 'ep', 'tp'))
All inputs are finite; a program needn't handle non-finite values.
Results may differ from the reference program's by a relative error of at most 0.00124.
Values are sent between devices in bfloat16 or wider.
A program may use at most 768 MiB of HBM per device.

```python
import jax
import jax.numpy as jnp
from jax import lax

TOKENS = 1024
D = 2048
FF = 1024
EXPERTS = 64
TOP = 8
GROUPS = 8
BLOCK_ROWS = 128

ROWS = TOKENS // GROUPS
LOCAL = EXPERTS // GROUPS
HALF = TOP // 2


def draw_routing(key):
    k_perm, k_shift, k_pick, k_cols = jax.random.split(key, 4)
    rank = jax.vmap(lambda sub_key: jax.random.permutation(sub_key, ROWS))(jax.random.split(k_perm, GROUPS))
    shifts = jax.random.randint(k_shift, (GROUPS, ROWS // GROUPS), 1, GROUPS)
    source = jnp.arange(GROUPS)[:, None]
    first = (source + rank % GROUPS) % GROUPS
    second = (first + jnp.take_along_axis(shifts, rank // GROUPS, axis=1)) % GROUPS
    shard_pair = jnp.stack([first, second], axis=-1)
    scores = jax.random.randint(k_pick, (GROUPS, ROWS, 2, LOCAL), 0, 1 << 20) * LOCAL + jnp.arange(LOCAL)
    picks = jnp.argsort(scores, axis=-1)[..., :HALF]
    expert_ids = (shard_pair[..., None] * LOCAL + picks).reshape(TOKENS, TOP)
    col_scores = jax.random.randint(k_cols, (TOKENS, TOP), 0, 1 << 20) * TOP + jnp.arange(TOP)
    col_order = jnp.argsort(col_scores, axis=-1)
    return jnp.take_along_axis(expert_ids, col_order, axis=1).astype(jnp.int32)


def setup_inputs(seed: int = 0, part: int = 0) -> dict:
    part_key = jax.random.fold_in(jax.random.key(seed), part)
    k_tok, k_route, k_gate = jax.random.split(part_key, 3)
    k_w1, k_w3, k_w2 = jax.random.split(jax.random.key(seed + 1), 3)
    tokens_in = jax.random.normal(k_tok, (TOKENS, D), jnp.float32).astype(jnp.bfloat16)
    expert_ids = draw_routing(k_route)
    router_gates = jax.random.uniform(k_gate, (TOKENS, TOP), jnp.float32, 0.5, 1.5)
    w_gate = (jax.random.normal(k_w1, (EXPERTS, D, FF), jnp.float32) * D ** -0.5).astype(jnp.bfloat16)
    w_up = (jax.random.normal(k_w3, (EXPERTS, D, FF), jnp.float32) * D ** -0.5).astype(jnp.bfloat16)
    w_down = (jax.random.normal(k_w2, (EXPERTS, FF, D), jnp.float32) * FF ** -0.5).astype(jnp.bfloat16)
    return {'tokens_in': tokens_in, 'expert_ids': expert_ids, 'router_gates': router_gates, 'w_gate': w_gate, 'w_up': w_up, 'w_down': w_down}


def reference(tokens_in, expert_ids, router_gates, w_gate, w_up, w_down):
    pair_count = TOKENS * TOP
    flat_exp = expert_ids.reshape(-1)
    sort_order = jnp.argsort(flat_exp, stable=True)
    sorted_exp = flat_exp[sort_order]
    counts = jnp.bincount(flat_exp, length=EXPERTS)
    starts = jnp.cumsum(counts) - counts
    padded = (counts + BLOCK_ROWS - 1) // BLOCK_ROWS * BLOCK_ROWS
    pad_ends = jnp.cumsum(padded)
    pad_starts = pad_ends - padded
    slot_dest = pad_starts[sorted_exp] + jnp.arange(pair_count) - starts[sorted_exp]
    block_count = (pair_count + BLOCK_ROWS - 1) // BLOCK_ROWS + EXPERTS
    slot_pair = jnp.full((block_count * BLOCK_ROWS,), -1, jnp.int32).at[slot_dest].set(sort_order.astype(jnp.int32))
    safe_pair = jnp.maximum(slot_pair, 0)
    slot_tok = (safe_pair // TOP).reshape(block_count, BLOCK_ROWS)
    slot_gate = jnp.where(slot_pair >= 0, router_gates.reshape(-1)[safe_pair], 0.0).reshape(block_count, BLOCK_ROWS)
    block_start = jnp.arange(block_count) * BLOCK_ROWS
    block_exp = jnp.minimum(jnp.sum(pad_ends[None, :] <= block_start[:, None], axis=1), EXPERTS - 1)

    def add_block(running, block):
        tok_ids, gate_vals, expert = block
        row_act = tokens_in[tok_ids]
        h_gate = jnp.dot(row_act, w_gate[expert], preferred_element_type=jnp.float32)
        h_up = jnp.dot(row_act, w_up[expert], preferred_element_type=jnp.float32)
        hidden = (jax.nn.silu(h_gate) * h_up).astype(jnp.bfloat16)
        out_rows = jnp.dot(hidden, w_down[expert], preferred_element_type=jnp.float32)
        return running.at[tok_ids].add(out_rows * gate_vals[:, None]), None

    total, ignored = lax.scan(add_block, jnp.zeros((TOKENS, D), jnp.float32), (slot_tok, slot_gate, block_exp))
    return total.astype(jnp.bfloat16)
```

```python
import functools

import jax
import jax.numpy as jnp
from jax import lax
from jax.experimental import pallas as pl
from jax.experimental.pallas import tpu as pltpu
from jax.sharding import PartitionSpec as P

TOKEN_AXES = ('dp', 'ep', 'tp')
LANES = 128
F32 = jnp.float32
BF16 = jnp.bfloat16


def split3(v):
    hi = v.astype(BF16)
    rest = v - hi.astype(F32)
    mid = rest.astype(BF16)
    low = (rest - mid.astype(F32)).astype(BF16)
    return hi, mid, low


def dot(a, b):
    return lax.dot_general(a, b, (((1,), (0,)), ((), ())), preferred_element_type=F32)


def dot_nt(a, b):
    return lax.dot_general(a, b, (((1,), (1,)), ((), ())), preferred_element_type=F32)


def moe_kernel(names, ep_n, tp_n, tok_hbm, ids_hbm, gate_hbm, wg_hbm, wu_hbm, wd_hbm, out_ref,
               wg, wu, wd, xg, idg, gg, xs, gs, xr, gr, acc_g, acc_u, hb, gb, ob, zr, yb, yr, slot_of, row_of,
               w_sem, in_sem, ag_ss, ag_rs, id_ss, id_rs, dx_ss, dx_rs, dg_ss, dg_rs, cx_ss, cx_rs, cy_ss, cy_rs):
    rows, d = tok_hbm.shape
    local = wg_hbm.shape[0]
    choices = ids_hbm.shape[1]
    shard_rows = rows * tp_n
    cap = 2 * shard_rows // ep_n
    slots = cap * ep_n
    kcs = 4
    kw = d // kcs

    ep = lax.axis_index('ep')
    tp = lax.axis_index('tp')

    def device(ep_i, tp_i):
        at = {'dp': lax.axis_index('dp'), 'ep': ep_i, 'tp': tp_i}
        return tuple(at[n] for n in names)

    chips = ep_n // 2
    x_peers = [(dx, cf) for dx in (2, 1, chips - 1, 0) for cf in (0, 1) if (dx, cf) != (0, 0)]

    def x_target(p):
        return lax.rem(ep // 2 + p[0], chips) * 2 + lax.rem(ep + p[1], 2)

    def y_target(dt):
        return lax.rem(tp + dt, tp_n)

    def rdma(src, dst, ss, rs, dev):
        return pltpu.make_async_remote_copy(src_ref=src, dst_ref=dst, send_sem=ss, recv_sem=rs,
                                            device_id=dev, device_id_type=pl.DeviceIdType.MESH)

    my_rows = pl.ds(pl.multiple_of(tp * rows, rows), rows)
    my_slots = pl.ds(pl.multiple_of(ep * cap, cap), cap)

    own = [pltpu.make_async_copy(ids_hbm, idg.at[my_rows], in_sem.at[0]),
           pltpu.make_async_copy(gate_hbm, gg.at[my_rows], in_sem.at[1]),
           pltpu.make_async_copy(tok_hbm, xg.at[my_rows], in_sem.at[2])]
    for c in own:
        c.start()

    bar = pltpu.get_barrier_semaphore()
    for dt in range(1, tp_n):
        pl.semaphore_signal(bar, inc=1, device_id=device(ep, y_target(dt)), device_id_type=pl.DeviceIdType.MESH)
    for p in x_peers:
        pl.semaphore_signal(bar, inc=1, device_id=device(x_target(p), tp), device_id_type=pl.DeviceIdType.MESH)
    loads = []
    for i, (src, dst) in enumerate(((wg_hbm, wg), (wu_hbm, wu), (wd_hbm, wd))):
        for e in range(local):
            loads.append(pltpu.make_async_copy(src.at[e], dst.at[e], w_sem.at[i, e]))
    for c in own:
        c.wait()
    pl.semaphore_wait(bar, tp_n - 1 + len(x_peers))

    id_cps, ag_cps = [], []
    for dt in range(1, tp_n):
        dev = device(ep, y_target(dt))
        id_cps.append(rdma(idg.at[my_rows], idg.at[my_rows], id_ss.at[0, dt - 1], id_rs.at[0, dt - 1], dev))
        id_cps.append(rdma(gg.at[my_rows], gg.at[my_rows], id_ss.at[1, dt - 1], id_rs.at[1, dt - 1], dev))
    for kc in range(kcs):
        for dt in (2, 1, 3):
            dev = device(ep, y_target(dt))
            part = xg.at[my_rows, pl.ds(kc * kw, kw)]
            ag_cps.append(rdma(part, part, ag_ss.at[kc, dt - 1], ag_rs.at[kc, dt - 1], dev))
    for c in id_cps + ag_cps:
        c.start()
    for c in loads:
        c.start()
    for c in id_cps:
        c.wait_recv()

    lane = lax.broadcasted_iota(jnp.int32, (shard_rows, LANES), 1)
    used = jnp.zeros((shard_rows, LANES), jnp.bool_)
    gate_of = jnp.zeros((shard_rows, LANES), F32)
    ids = idg[...]
    gates = gg[...]
    for j in range(choices):
        e_j = ids[:, j:j + 1]
        used = used | (e_j // local == lane)
        gate_of = gate_of + jnp.where(e_j == lane, gates[:, j:j + 1], 0.0)
    used_b = used.astype(F32).astype(BF16)
    before = (lax.broadcasted_iota(jnp.int32, (shard_rows, shard_rows), 0)
              > lax.broadcasted_iota(jnp.int32, (shard_rows, shard_rows), 1)).astype(F32).astype(BF16)
    rank = dot(before, used_b).astype(BF16)
    s_iota = lax.broadcasted_iota(jnp.int32, (slots, LANES), 0)
    expand = (s_iota // cap == lax.broadcasted_iota(jnp.int32, (slots, LANES), 1)).astype(F32).astype(BF16)
    in_slot = lax.broadcasted_iota(jnp.int32, (slots, shard_rows), 0) % cap
    s1 = (dot_nt(expand, used_b) > 0.5) & (dot_nt(expand, rank) == in_slot.astype(F32))
    slot_of[...] = s1.astype(F32).astype(BF16)
    in_slot_t = lax.broadcasted_iota(jnp.int32, (shard_rows, slots), 1) % cap
    s2 = (dot_nt(used_b, expand) > 0.5) & (dot_nt(rank, expand) == in_slot_t.astype(F32))
    row_of[...] = s2.astype(F32).astype(BF16)

    dx_cps, dg_cps = [], []
    for kc in range(kcs):
        cols = pl.ds(kc * kw, kw)
        for dt in range(1, tp_n):
            ag_cps[kc * (tp_n - 1) + {2: 0, 1: 1, 3: 2}[dt]].wait_recv()
        xs[:, cols] = dot(slot_of[...], xg[:, cols]).astype(BF16)
        for i, p in enumerate(x_peers):
            to = x_target(p)
            src = xs.at[pl.ds(pl.multiple_of(to * cap, cap), cap), cols]
            c = rdma(src, xr.at[my_slots, cols], dx_ss.at[kc, i], dx_rs.at[kc, i], device(to, tp))
            c.start()
            dx_cps.append(c)
        xr[my_slots, cols] = xs[my_slots, cols]
        if kc == 0:
            g1, g2, g3 = split3(gate_of)
            gs[...] = dot(slot_of[...], g1) + dot(slot_of[...], g2) + dot(slot_of[...], g3)
            gr[my_slots, :] = gs[my_slots, :]
            for i, p in enumerate(x_peers):
                to = x_target(p)
                src = gs.at[pl.ds(pl.multiple_of(to * cap, cap), cap)]
                c = rdma(src, gr.at[my_slots], dg_ss.at[i], dg_rs.at[i], device(to, tp))
                c.start()
                dg_cps.append(c)

    for c in loads:
        c.wait()
    g_lane = lax.broadcasted_iota(jnp.int32, (slots, LANES), 1)
    for kc in range(kcs):
        cols = pl.ds(kc * kw, kw)
        for i in range(len(x_peers)):
            dx_cps[kc * len(x_peers) + i].wait_recv()
        if kc == 0:
            for c in dg_cps:
                c.wait_recv()

            def spread(e, carry):
                col = jnp.sum(jnp.where(g_lane == ep * local + e, gr[...], 0.0), axis=1, keepdims=True)
                gb[e] = jnp.broadcast_to(col, (slots, LANES))
                return carry

            lax.fori_loop(0, local, spread, 0)

        def up(e, carry, kc=kc, cols=cols):
            x = xr[:, cols]
            a = dot(x, wg[e, cols, :])
            b = dot(x, wu[e, cols, :])
            if kc > 0:
                a = a + acc_g[e]
                b = b + acc_u[e]
            if kc < kcs - 1:
                acc_g[e] = a
                acc_u[e] = b
            else:
                h = a * jax.nn.sigmoid(a) * b
                g = gb[e]
                on = jnp.concatenate([g] * (h.shape[1] // LANES), axis=1) > 0.0
                hb[e] = jnp.where(on, h, 0.0).astype(BF16)
            return carry

        lax.fori_loop(0, local, up, 0)

    cx_cps, cy_cps = [], []
    for kc in range(kcs):
        cols = pl.ds(kc * kw, kw)

        def down(e, carry, cols=cols):
            g = gb[e]
            o = dot(hb[e], wd[e, :, cols]) * jnp.concatenate([g] * (kw // LANES), axis=1)

            @pl.when(e == 0)
            def _():
                ob[:, cols] = o

            @pl.when(e > 0)
            def _():
                ob[:, cols] = ob[:, cols] + o

            return carry

        lax.fori_loop(0, local, down, 0)
        for i, p in enumerate(x_peers):
            to = x_target(p)
            src = ob.at[pl.ds(pl.multiple_of(to * cap, cap), cap), cols]
            c = rdma(src, zr.at[my_slots, cols], cx_ss.at[kc, i], cx_rs.at[kc, i], device(to, tp))
            c.start()
            cx_cps.append(c)
        zr[my_slots, cols] = ob[my_slots, cols]

    for kc in range(kcs):
        cols = pl.ds(kc * kw, kw)
        for i in range(len(x_peers)):
            cx_cps[kc * len(x_peers) + i].wait_recv()
        z1, z2, z3 = split3(zr[:, cols])
        pick = row_of[...]
        yb[:, cols] = dot(pick, z3) + dot(pick, z2) + dot(pick, z1)
        for dt in (2, 1, 3):
            to = y_target(dt)
            src = yb.at[pl.ds(pl.multiple_of(to * rows, rows), rows), cols]
            c = rdma(src, yr.at[dt - 1, :, cols], cy_ss.at[kc, dt - 1], cy_rs.at[kc, dt - 1], device(ep, to))
            c.start()
            cy_cps.append(c)
    for kc in range(kcs):
        cols = pl.ds(kc * kw, kw)
        for i in range(tp_n - 1):
            cy_cps[kc * (tp_n - 1) + i].wait_recv()
        total = yb[my_rows, cols]
        for i in range(tp_n - 1):
            total = total + yr[i, :, cols]
        out_ref[:, cols] = total.astype(BF16)

    for c in id_cps + ag_cps + dx_cps + dg_cps + cx_cps + cy_cps:
        c.wait_send()


def solution(mesh):
    ep_n = mesh.shape['ep']
    tp_n = mesh.shape['tp']
    names = tuple(mesh.axis_names)

    def block(tok, ids, gates, w_gate, w_up, w_down):
        rows, d = tok.shape
        local, _, hid = w_gate.shape
        shard_rows = rows * tp_n
        slots = 2 * shard_rows
        kcs = 4
        nx = ep_n - 1
        ny = tp_n - 1
        any_spec = pl.BlockSpec(memory_space=pl.ANY)
        dma = pltpu.SemaphoreType.DMA
        return pl.pallas_call(
            functools.partial(moe_kernel, names, ep_n, tp_n),
            out_shape=jax.ShapeDtypeStruct((rows, d), BF16),
            in_specs=[any_spec] * 6,
            out_specs=pl.BlockSpec(memory_space=pltpu.VMEM),
            scratch_shapes=[
                pltpu.VMEM((local, d, hid), BF16),
                pltpu.VMEM((local, d, hid), BF16),
                pltpu.VMEM((local, hid, d), BF16),
                pltpu.VMEM((shard_rows, d), BF16),
                pltpu.VMEM((shard_rows, ids.shape[1]), jnp.int32),
                pltpu.VMEM((shard_rows, gates.shape[1]), F32),
                pltpu.VMEM((slots, d), BF16),
                pltpu.VMEM((slots, LANES), F32),
                pltpu.VMEM((slots, d), BF16),
                pltpu.VMEM((slots, LANES), F32),
                pltpu.VMEM((local, slots, hid), F32),
                pltpu.VMEM((local, slots, hid), F32),
                pltpu.VMEM((local, slots, hid), BF16),
                pltpu.VMEM((local, slots, LANES), F32),
                pltpu.VMEM((slots, d), F32),
                pltpu.VMEM((slots, d), F32),
                pltpu.VMEM((shard_rows, d), F32),
                pltpu.VMEM((ny, rows, d), F32),
                pltpu.VMEM((slots, shard_rows), BF16),
                pltpu.VMEM((shard_rows, slots), BF16),
                dma((3, local)), dma((3,)),
                dma((kcs, ny)), dma((kcs, ny)),
                dma((2, ny)), dma((2, ny)),
                dma((kcs, nx)), dma((kcs, nx)),
                dma((nx,)), dma((nx,)),
                dma((kcs, nx)), dma((kcs, nx)),
                dma((kcs, ny)), dma((kcs, ny)),
            ],
            compiler_params=pltpu.CompilerParams(collective_id=0, has_side_effects=True,
                                                 vmem_limit_bytes=60 * 1024 * 1024),
        )(tok, ids, gates, w_gate, w_up, w_down)

    return jax.shard_map(
        block,
        mesh=mesh,
        in_specs=(P(TOKEN_AXES, None), P(TOKEN_AXES, None), P(TOKEN_AXES, None),
                  P('ep', None, 'tp'), P('ep', None, 'tp'), P('ep', 'tp', None)),
        out_specs=P(TOKEN_AXES, None),
        check_vma=False,
    )
```

```python
import functools

import jax
import jax.numpy as jnp
from jax import lax
from jax.experimental import pallas as pl
from jax.experimental.pallas import tpu as pltpu
from jax.sharding import PartitionSpec as P

TOKEN_AXES = ('dp', 'ep', 'tp')
LANES = 128
F32 = jnp.float32
BF16 = jnp.bfloat16


def split3(v):
    hi = v.astype(BF16)
    rest = v - hi.astype(F32)
    mid = rest.astype(BF16)
    low = (rest - mid.astype(F32)).astype(BF16)
    return hi, mid, low


def dot(a, b):
    return lax.dot_general(a, b, (((1,), (0,)), ((), ())), preferred_element_type=F32)


def dot_nt(a, b):
    return lax.dot_general(a, b, (((1,), (1,)), ((), ())), preferred_element_type=F32)


def moe_kernel(names, ep_n, tp_n, tok_hbm, ids_hbm, gate_hbm, wg_hbm, wu_hbm, wd_hbm, out_ref,
               wg, wu, wd, xg, idg, gg, xs, gs, xr, gr, acc_g, acc_u, hb, gb, ob, zr, yb, yr, slot_of, row_of, gcols,
               w_sem, in_sem, ag_ss, ag_rs, id_ss, id_rs, dx_ss, dx_rs, dg_ss, dg_rs, cx_ss, cx_rs, cy_ss, cy_rs):
    rows, d = tok_hbm.shape
    local = wg_hbm.shape[0]
    choices = ids_hbm.shape[0]
    shard_rows = rows * tp_n
    cap = 2 * shard_rows // ep_n
    slots = cap * ep_n
    per_tile = LANES // cap
    kcs = 4
    kw = d // kcs

    ep = lax.axis_index('ep')
    tp = lax.axis_index('tp')

    def device(ep_i, tp_i):
        at = {'dp': lax.axis_index('dp'), 'ep': ep_i, 'tp': tp_i}
        return tuple(at[n] for n in names)

    chips = ep_n // 2
    x_peers = [(dx, cf) for dx in (2, 1, chips - 1, 0) for cf in (0, 1) if (dx, cf) != (0, 0)]

    def x_target(p):
        return lax.rem(ep // 2 + p[0], chips) * 2 + lax.rem(ep + p[1], 2)

    def y_target(dt):
        return lax.rem(tp + dt, tp_n)

    def rdma(src, dst, ss, rs, dev):
        return pltpu.make_async_remote_copy(src_ref=src, dst_ref=dst, send_sem=ss, recv_sem=rs,
                                            device_id=dev, device_id_type=pl.DeviceIdType.MESH)

    my_rows = pl.ds(pl.multiple_of(tp * rows, rows), rows)
    my_slots = pl.ds(pl.multiple_of(ep * cap, cap), cap)

    own = [pltpu.make_async_copy(ids_hbm, idg.at[tp], in_sem.at[0]),
           pltpu.make_async_copy(gate_hbm, gg.at[tp], in_sem.at[1]),
           pltpu.make_async_copy(tok_hbm, xg.at[my_rows], in_sem.at[2])]
    for c in own:
        c.start()

    bar = pltpu.get_barrier_semaphore()
    for dt in range(1, tp_n):
        pl.semaphore_signal(bar, inc=1, device_id=device(ep, y_target(dt)), device_id_type=pl.DeviceIdType.MESH)
    for p in x_peers:
        pl.semaphore_signal(bar, inc=1, device_id=device(x_target(p), tp), device_id_type=pl.DeviceIdType.MESH)
    loads = []
    for i, (src, dst) in enumerate(((wg_hbm, wg), (wu_hbm, wu), (wd_hbm, wd))):
        for e in range(local):
            loads.append(pltpu.make_async_copy(src.at[e], dst.at[e], w_sem.at[i, e]))
    for c in own:
        c.wait()
    pl.semaphore_wait(bar, tp_n - 1 + len(x_peers))

    id_cps, ag_cps = [], []
    for dt in range(1, tp_n):
        dev = device(ep, y_target(dt))
        id_cps.append(rdma(idg.at[tp], idg.at[tp], id_ss.at[0, dt - 1], id_rs.at[0, dt - 1], dev))
        id_cps.append(rdma(gg.at[tp], gg.at[tp], id_ss.at[1, dt - 1], id_rs.at[1, dt - 1], dev))
    for kc in range(kcs):
        for dt in (2, 1, 3):
            dev = device(ep, y_target(dt))
            part = xg.at[my_rows, pl.ds(kc * kw, kw)]
            ag_cps.append(rdma(part, part, ag_ss.at[kc, dt - 1], ag_rs.at[kc, dt - 1], dev))
    for c in id_cps + ag_cps:
        c.start()
    for c in loads:
        c.start()
    for c in id_cps:
        c.wait_recv()

    ids = jnp.concatenate([idg[q] for q in range(tp_n)], axis=1)
    gates = jnp.concatenate([gg[q] for q in range(tp_n)], axis=1)
    b_iota = lax.broadcasted_iota(jnp.int32, (ep_n, shard_rows), 0)
    used = jnp.zeros((ep_n, shard_rows), F32)
    for j in range(choices):
        used = jnp.where(ids[j:j + 1, :] // local == b_iota, 1.0, used)
    before = (lax.broadcasted_iota(jnp.int32, (shard_rows, shard_rows), 0)
              < lax.broadcasted_iota(jnp.int32, (shard_rows, shard_rows), 1)).astype(F32).astype(BF16)
    rank = dot(used.astype(BF16), before)
    place = jnp.where(used > 0.0, rank, -1.0)
    in_slot = lax.broadcasted_iota(jnp.int32, (cap, shard_rows), 0).astype(F32)
    for b in range(ep_n):
        hit = jnp.where(place[b:b + 1, :] == in_slot, 1.0, 0.0)
        slot_of[pl.ds(b * cap, cap), :] = hit.astype(BF16)

    dx_cps, dg_cps = [], []
    for kc in range(kcs):
        cols = pl.ds(kc * kw, kw)
        for dt in range(1, tp_n):
            ag_cps[kc * (tp_n - 1) + {2: 0, 1: 1, 3: 2}[dt]].wait_recv()
        xs[:, cols] = dot(slot_of[...], xg[:, cols]).astype(BF16)
        for i, p in enumerate(x_peers):
            to = x_target(p)
            src = xs.at[pl.ds(pl.multiple_of(to * cap, cap), cap), cols]
            c = rdma(src, xr.at[my_slots, cols], dx_ss.at[kc, i], dx_rs.at[kc, i], device(to, tp))
            c.start()
            dx_cps.append(c)
        xr[my_slots, cols] = xs[my_slots, cols]
        if kc == 0:
            e_iota = lax.broadcasted_iota(jnp.int32, (ep_n * local, shard_rows), 0)
            gate_of = jnp.zeros((ep_n * local, shard_rows), F32)
            for j in range(choices):
                gate_of = jnp.where(ids[j:j + 1, :] == e_iota, gates[j:j + 1, :], gate_of)
            g1, g2, g3 = split3(gate_of)
            gs[...] = dot_nt(g3, slot_of[...]) + dot_nt(g2, slot_of[...]) + dot_nt(g1, slot_of[...])

            def gate_tile(b):
                return (pl.ds(pl.multiple_of(b * local, local), local),
                        pl.ds(pl.multiple_of(b // per_tile * LANES, LANES), LANES))

            for i, p in enumerate(x_peers):
                to = x_target(p)
                c = rdma(gs.at[gate_tile(to)], gr.at[ep], dg_ss.at[i], dg_rs.at[i], device(to, tp))
                c.start()
                dg_cps.append(c)
            gr[ep] = gs[gate_tile(ep)]
    row_of[...] = jnp.transpose(slot_of[...].astype(F32)).astype(BF16)

    for c in loads:
        c.wait()
    for kc in range(kcs):
        cols = pl.ds(kc * kw, kw)
        for i in range(len(x_peers)):
            dx_cps[kc * len(x_peers) + i].wait_recv()
        if kc == 0:
            for c in dg_cps:
                c.wait_recv()

            lanes_of_mine = pl.ds(pl.multiple_of(lax.rem(ep, per_tile) * cap, cap), cap)
            for a in range(ep_n):
                gcols[...] = jnp.transpose(jnp.concatenate([gr[a]] * (LANES // local), axis=0))
                cols_a = gcols[lanes_of_mine, :]
                for e in range(local):
                    gb[e, pl.ds(a * cap, cap), :] = jnp.broadcast_to(cols_a[:, e:e + 1], (cap, LANES))

        def up(e, carry, kc=kc, cols=cols):
            x = xr[:, cols]
            a = dot(x, wg[e, cols, :])
            b = dot(x, wu[e, cols, :])
            if kc > 0:
                a = a + acc_g[e]
                b = b + acc_u[e]
            if kc < kcs - 1:
                acc_g[e] = a
                acc_u[e] = b
            else:
                h = a * jax.nn.sigmoid(a) * b
                g = gb[e]
                on = jnp.concatenate([g] * (h.shape[1] // LANES), axis=1) > 0.0
                hb[e] = jnp.where(on, h, 0.0).astype(BF16)
            return carry

        lax.fori_loop(0, local, up, 0, unroll=True)

    cx_cps, cy_cps = [], []
    for kc in range(kcs):
        cols = pl.ds(kc * kw, kw)

        total = None
        for e in range(local):
            o = dot(hb[e], wd[e, :, cols]) * jnp.concatenate([gb[e]] * (kw // LANES), axis=1)
            total = o if total is None else total + o
        ob[:, cols] = total
        for i, p in enumerate(x_peers):
            to = x_target(p)
            src = ob.at[pl.ds(pl.multiple_of(to * cap, cap), cap), cols]
            c = rdma(src, zr.at[my_slots, cols], cx_ss.at[kc, i], cx_rs.at[kc, i], device(to, tp))
            c.start()
            cx_cps.append(c)
        zr[my_slots, cols] = ob[my_slots, cols]

    for kc in range(kcs):
        cols = pl.ds(kc * kw, kw)
        for i in range(len(x_peers)):
            cx_cps[kc * len(x_peers) + i].wait_recv()
        z1, z2, z3 = split3(zr[:, cols])
        pick = row_of[...]
        yb[:, cols] = dot(pick, z3) + dot(pick, z2) + dot(pick, z1)
        for dt in (2, 1, 3):
            to = y_target(dt)
            src = yb.at[pl.ds(pl.multiple_of(to * rows, rows), rows), cols]
            c = rdma(src, yr.at[dt - 1, :, cols], cy_ss.at[kc, dt - 1], cy_rs.at[kc, dt - 1], device(ep, to))
            c.start()
            cy_cps.append(c)
    for kc in range(kcs):
        cols = pl.ds(kc * kw, kw)
        for i in range(tp_n - 1):
            cy_cps[kc * (tp_n - 1) + i].wait_recv()
        total = yb[my_rows, cols]
        for i in range(tp_n - 1):
            total = total + yr[i, :, cols]
        out_ref[:, cols] = total.astype(BF16)

    for c in id_cps + ag_cps + dx_cps + dg_cps + cx_cps + cy_cps:
        c.wait_send()


def solution(mesh):
    ep_n = mesh.shape['ep']
    tp_n = mesh.shape['tp']
    names = tuple(mesh.axis_names)

    def block(tok, ids, gates, w_gate, w_up, w_down):
        rows, d = tok.shape
        local, _, hid = w_gate.shape
        shard_rows = rows * tp_n
        slots = 2 * shard_rows
        kcs = 4
        nx = ep_n - 1
        ny = tp_n - 1
        any_spec = pl.BlockSpec(memory_space=pl.ANY)
        dma = pltpu.SemaphoreType.DMA
        return pl.pallas_call(
            functools.partial(moe_kernel, names, ep_n, tp_n),
            out_shape=pltpu.VMEM((rows, d), BF16),
            in_specs=[any_spec] * 6,
            out_specs=pl.BlockSpec(memory_space=pltpu.VMEM),
            scratch_shapes=[
                pltpu.VMEM((local, d, hid), BF16),
                pltpu.VMEM((local, d, hid), BF16),
                pltpu.VMEM((local, hid, d), BF16),
                pltpu.VMEM((shard_rows, d), BF16),
                pltpu.VMEM((tp_n, ids.shape[1], rows), jnp.int32),
                pltpu.VMEM((tp_n, gates.shape[1], rows), F32),
                pltpu.VMEM((slots, d), BF16),
                pltpu.VMEM((ep_n * local, slots), F32),
                pltpu.VMEM((slots, d), BF16),
                pltpu.VMEM((ep_n, local, LANES), F32),
                pltpu.VMEM((local, slots, hid), F32),
                pltpu.VMEM((local, slots, hid), F32),
                pltpu.VMEM((local, slots, hid), BF16),
                pltpu.VMEM((local, slots, LANES), F32),
                pltpu.VMEM((slots, d), F32),
                pltpu.VMEM((slots, d), F32),
                pltpu.VMEM((shard_rows, d), F32),
                pltpu.VMEM((ny, rows, d), F32),
                pltpu.VMEM((slots, shard_rows), BF16),
                pltpu.VMEM((shard_rows, slots), BF16),
                pltpu.VMEM((LANES, LANES), F32),
                dma((3, local)), dma((3,)),
                dma((kcs, ny)), dma((kcs, ny)),
                dma((2, ny)), dma((2, ny)),
                dma((kcs, nx)), dma((kcs, nx)),
                dma((nx,)), dma((nx,)),
                dma((kcs, nx)), dma((kcs, nx)),
                dma((kcs, ny)), dma((kcs, ny)),
            ],
            compiler_params=pltpu.CompilerParams(collective_id=0, has_side_effects=True,
                                                 vmem_limit_bytes=60 * 1024 * 1024),
        )(tok, ids.T, gates.T, w_gate, w_up, w_down)

    return jax.shard_map(
        block,
        mesh=mesh,
        in_specs=(P(TOKEN_AXES, None), P(TOKEN_AXES, None), P(TOKEN_AXES, None),
                  P('ep', None, 'tp'), P('ep', None, 'tp'), P('ep', 'tp', None)),
        out_specs=P(TOKEN_AXES, None),
        check_vma=False,
    )
```

```python
import functools

import jax
import jax.numpy as jnp
from jax import lax
from jax.experimental import pallas as pl
from jax.experimental.pallas import tpu as pltpu
from jax.sharding import PartitionSpec as P

TOKEN_AXES = ('dp', 'ep', 'tp')
LANES = 128
F32 = jnp.float32
BF16 = jnp.bfloat16


def split3(v):
    hi = v.astype(BF16)
    rest = v - hi.astype(F32)
    mid = rest.astype(BF16)
    low = (rest - mid.astype(F32)).astype(BF16)
    return hi, mid, low


def dot(a, b):
    return lax.dot_general(a, b, (((1,), (0,)), ((), ())), preferred_element_type=F32)


def dot_nt(a, b):
    return lax.dot_general(a, b, (((1,), (1,)), ((), ())), preferred_element_type=F32)


def moe_kernel(names, ep_n, tp_n, tok_hbm, ids_hbm, gate_hbm, wg_hbm, wu_hbm, wd_hbm, out_ref,
               wg, wu, wd, xg, idg, gg, xs, gs, xr, gr, acc_g, acc_u, hb, gb, ob, zr, yb, yr, yf, zs, slot_of, row_of, gcols,
               w_sem, in_sem, ag_ss, ag_rs, id_ss, id_rs, dx_ss, dx_rs, dg_ss, dg_rs, cx_ss, cx_rs, yf_ss, yf_rs, zf_ss, zf_rs, cy_ss, cy_rs):
    rows, d = tok_hbm.shape
    local = wg_hbm.shape[0]
    choices = ids_hbm.shape[0]
    shard_rows = rows * tp_n
    cap = 2 * shard_rows // ep_n
    slots = cap * ep_n
    per_tile = LANES // cap
    kcs = 4
    kw = d // kcs

    ep = lax.axis_index('ep')
    tp = lax.axis_index('tp')

    def device(ep_i, tp_i):
        at = {'dp': lax.axis_index('dp'), 'ep': ep_i, 'tp': tp_i}
        return tuple(at[n] for n in names)

    chips = ep_n // 2
    x_peers = [(dx, cf) for dx in (2, 1, chips - 1, 0) for cf in (0, 1) if (dx, cf) != (0, 0)]

    far = [p for p in x_peers if 2 * p[0] == chips]
    near = [p for p in x_peers if 2 * p[0] != chips]
    qw = kw // tp_n

    def x_target(p):
        return lax.rem(ep // 2 + p[0], chips) * 2 + lax.rem(ep + p[1], 2)

    def y_target(dt):
        return lax.rem(tp + dt, tp_n)

    def rdma(src, dst, ss, rs, dev):
        return pltpu.make_async_remote_copy(src_ref=src, dst_ref=dst, send_sem=ss, recv_sem=rs,
                                            device_id=dev, device_id_type=pl.DeviceIdType.MESH)

    my_rows = pl.ds(pl.multiple_of(tp * rows, rows), rows)
    my_slots = pl.ds(pl.multiple_of(ep * cap, cap), cap)

    def slots_of(e):
        return pl.ds(pl.multiple_of(e * cap, cap), cap)

    def quarter(kc, t):
        return pl.ds(pl.multiple_of(kc * kw + t * qw, qw), qw)

    own = [pltpu.make_async_copy(ids_hbm, idg.at[tp], in_sem.at[0]),
           pltpu.make_async_copy(gate_hbm, gg.at[tp], in_sem.at[1]),
           pltpu.make_async_copy(tok_hbm, xg.at[my_rows], in_sem.at[2])]
    for c in own:
        c.start()

    for p in far:
        zr[slots_of(x_target(p)), :] = jnp.zeros((cap, d), F32)

    bar = pltpu.get_barrier_semaphore()
    for dt in range(1, tp_n):
        pl.semaphore_signal(bar, inc=1, device_id=device(ep, y_target(dt)), device_id_type=pl.DeviceIdType.MESH)
    for p in x_peers:
        pl.semaphore_signal(bar, inc=1, device_id=device(x_target(p), tp), device_id_type=pl.DeviceIdType.MESH)
    loads = []
    for i, (src, dst) in enumerate(((wg_hbm, wg), (wu_hbm, wu), (wd_hbm, wd))):
        for e in range(local):
            loads.append(pltpu.make_async_copy(src.at[e], dst.at[e], w_sem.at[i, e]))
    for c in own:
        c.wait()
    pl.semaphore_wait(bar, tp_n - 1 + len(x_peers))

    id_cps, ag_cps = [], []
    for dt in range(1, tp_n):
        dev = device(ep, y_target(dt))
        id_cps.append(rdma(idg.at[tp], idg.at[tp], id_ss.at[0, dt - 1], id_rs.at[0, dt - 1], dev))
        id_cps.append(rdma(gg.at[tp], gg.at[tp], id_ss.at[1, dt - 1], id_rs.at[1, dt - 1], dev))
    for kc in range(kcs):
        for dt in (2, 1, 3):
            dev = device(ep, y_target(dt))
            part = xg.at[my_rows, pl.ds(kc * kw, kw)]
            ag_cps.append(rdma(part, part, ag_ss.at[kc, dt - 1], ag_rs.at[kc, dt - 1], dev))
    for c in id_cps + ag_cps:
        c.start()
    for c in loads:
        c.start()
    for c in id_cps:
        c.wait_recv()

    ids = jnp.concatenate([idg[q] for q in range(tp_n)], axis=1)
    gates = jnp.concatenate([gg[q] for q in range(tp_n)], axis=1)
    b_iota = lax.broadcasted_iota(jnp.int32, (ep_n, shard_rows), 0)
    used = jnp.zeros((ep_n, shard_rows), F32)
    for j in range(choices):
        used = jnp.where(ids[j:j + 1, :] // local == b_iota, 1.0, used)
    before = (lax.broadcasted_iota(jnp.int32, (shard_rows, shard_rows), 0)
              < lax.broadcasted_iota(jnp.int32, (shard_rows, shard_rows), 1)).astype(F32).astype(BF16)
    rank = dot(used.astype(BF16), before)
    place = jnp.where(used > 0.0, rank, -1.0)
    in_slot = lax.broadcasted_iota(jnp.int32, (cap, shard_rows), 0).astype(F32)
    for b in range(ep_n):
        hit = jnp.where(place[b:b + 1, :] == in_slot, 1.0, 0.0)
        slot_of[pl.ds(b * cap, cap), :] = hit.astype(BF16)

    dx_cps, dg_cps = [], []
    for kc in range(kcs):
        cols = pl.ds(kc * kw, kw)
        for dt in range(1, tp_n):
            ag_cps[kc * (tp_n - 1) + {2: 0, 1: 1, 3: 2}[dt]].wait_recv()
        xs[:, cols] = dot(slot_of[...], xg[:, cols]).astype(BF16)
        for i, p in enumerate(x_peers):
            to = x_target(p)
            src = xs.at[pl.ds(pl.multiple_of(to * cap, cap), cap), cols]
            c = rdma(src, xr.at[my_slots, cols], dx_ss.at[kc, i], dx_rs.at[kc, i], device(to, tp))
            c.start()
            dx_cps.append(c)
        xr[my_slots, cols] = xs[my_slots, cols]
        if kc == 0:
            e_iota = lax.broadcasted_iota(jnp.int32, (ep_n * local, shard_rows), 0)
            gate_of = jnp.zeros((ep_n * local, shard_rows), F32)
            for j in range(choices):
                gate_of = jnp.where(ids[j:j + 1, :] == e_iota, gates[j:j + 1, :], gate_of)
            g1, g2, g3 = split3(gate_of)
            gs[...] = dot_nt(g3, slot_of[...]) + dot_nt(g2, slot_of[...]) + dot_nt(g1, slot_of[...])

            def gate_tile(b):
                return (pl.ds(pl.multiple_of(b * local, local), local),
                        pl.ds(pl.multiple_of(b // per_tile * LANES, LANES), LANES))

            for i, p in enumerate(x_peers):
                to = x_target(p)
                c = rdma(gs.at[gate_tile(to)], gr.at[ep], dg_ss.at[i], dg_rs.at[i], device(to, tp))
                c.start()
                dg_cps.append(c)
            gr[ep] = gs[gate_tile(ep)]
    row_of[...] = jnp.transpose(slot_of[...].astype(F32)).astype(BF16)

    for c in loads:
        c.wait()
    for kc in range(kcs):
        cols = pl.ds(kc * kw, kw)
        for i in range(len(x_peers)):
            dx_cps[kc * len(x_peers) + i].wait_recv()
        if kc == 0:
            for c in dg_cps:
                c.wait_recv()

            lanes_of_mine = pl.ds(pl.multiple_of(lax.rem(ep, per_tile) * cap, cap), cap)
            for a in range(ep_n):
                gcols[...] = jnp.transpose(jnp.concatenate([gr[a]] * (LANES // local), axis=0))
                cols_a = gcols[lanes_of_mine, :]
                for e in range(local):
                    gb[e, pl.ds(a * cap, cap), :] = jnp.broadcast_to(cols_a[:, e:e + 1], (cap, LANES))

        def up(e, carry, kc=kc, cols=cols):
            x = xr[:, cols]
            a = dot(x, wg[e, cols, :])
            b = dot(x, wu[e, cols, :])
            if kc > 0:
                a = a + acc_g[e]
                b = b + acc_u[e]
            if kc < kcs - 1:
                acc_g[e] = a
                acc_u[e] = b
            else:
                h = a * jax.nn.sigmoid(a) * b
                g = gb[e]
                on = jnp.concatenate([g] * (h.shape[1] // LANES), axis=1) > 0.0
                hb[e] = jnp.where(on, h, 0.0).astype(BF16)
            return carry

        lax.fori_loop(0, local, up, 0, unroll=True)

    cx_cps, yf_cps, zf_cps, cy_cps = [], [], [], []

    def down(kc):
        cols = pl.ds(kc * kw, kw)
        total = None
        for e in range(local):
            o = dot(hb[e], wd[e, :, cols]) * jnp.concatenate([gb[e]] * (kw // LANES), axis=1)
            total = o if total is None else total + o
        ob[:, cols] = total
        zr[my_slots, cols] = ob[my_slots, cols]
        for j, p in enumerate(far):
            for dt in (2, 1, 3):
                q = y_target(dt)
                c = rdma(ob.at[slots_of(x_target(p)), quarter(kc, q)], yf.at[dt - 1, j, :, pl.ds(kc * qw, qw)],
                         yf_ss.at[kc, j, dt - 1], yf_rs.at[kc, j, dt - 1], device(ep, q))
                c.start()
                yf_cps.append(c)

    def send_near(kc):
        cols = pl.ds(kc * kw, kw)
        for i, p in enumerate(near):
            to = x_target(p)
            c = rdma(ob.at[slots_of(to), cols], zr.at[my_slots, cols], cx_ss.at[kc, i], cx_rs.at[kc, i], device(to, tp))
            c.start()
            cx_cps.append(c)

    def send_far(kc):
        part = pl.ds(kc * qw, qw)
        per = len(far) * (tp_n - 1)
        for c in yf_cps[kc * per:(kc + 1) * per]:
            c.wait_recv()
        for j, p in enumerate(far):
            to = x_target(p)
            total = ob[slots_of(to), quarter(kc, tp)]
            for i in range(tp_n - 1):
                total = total + yf[i, j, :, part]
            zs[j, :, part] = total
            c = rdma(zs.at[j, :, part], zr.at[my_slots, quarter(kc, tp)], zf_ss.at[kc, j], zf_rs.at[kc, j],
                     device(to, tp))
            c.start()
            zf_cps.append(c)

    lead = kcs // 2
    for kc in range(kcs):
        down(kc)
        if kc < lead:
            send_near(kc)
    for kc in range(kcs):
        send_far(kc)
        if kc + lead < kcs:
            send_near(kc + lead)

    for kc in range(kcs):
        cols = pl.ds(kc * kw, kw)
        for c in cx_cps[kc * len(near):(kc + 1) * len(near)] + zf_cps[kc * len(far):(kc + 1) * len(far)]:
            c.wait_recv()
        z1, z2, z3 = split3(zr[:, cols])
        pick = row_of[...]
        yb[:, cols] = dot(pick, z3) + dot(pick, z2) + dot(pick, z1)
        for dt in (2, 1, 3):
            to = y_target(dt)
            src = yb.at[pl.ds(pl.multiple_of(to * rows, rows), rows), cols]
            c = rdma(src, yr.at[dt - 1, :, cols], cy_ss.at[kc, dt - 1], cy_rs.at[kc, dt - 1], device(ep, to))
            c.start()
            cy_cps.append(c)
    for kc in range(kcs):
        cols = pl.ds(kc * kw, kw)
        for i in range(tp_n - 1):
            cy_cps[kc * (tp_n - 1) + i].wait_recv()
        total = yb[my_rows, cols]
        for i in range(tp_n - 1):
            total = total + yr[i, :, cols]
        out_ref[:, cols] = total.astype(BF16)

    for c in id_cps + ag_cps + dx_cps + dg_cps + cx_cps + yf_cps + zf_cps + cy_cps:
        c.wait_send()


def solution(mesh):
    ep_n = mesh.shape['ep']
    tp_n = mesh.shape['tp']
    names = tuple(mesh.axis_names)

    def block(tok, ids, gates, w_gate, w_up, w_down):
        rows, d = tok.shape
        local, _, hid = w_gate.shape
        shard_rows = rows * tp_n
        slots = 2 * shard_rows
        kcs = 4
        nx = ep_n - 1
        ny = tp_n - 1
        any_spec = pl.BlockSpec(memory_space=pl.ANY)
        dma = pltpu.SemaphoreType.DMA
        return pl.pallas_call(
            functools.partial(moe_kernel, names, ep_n, tp_n),
            out_shape=pltpu.VMEM((rows, d), BF16),
            in_specs=[any_spec] * 6,
            out_specs=pl.BlockSpec(memory_space=pltpu.VMEM),
            scratch_shapes=[
                pltpu.VMEM((local, d, hid), BF16),
                pltpu.VMEM((local, d, hid), BF16),
                pltpu.VMEM((local, hid, d), BF16),
                pltpu.VMEM((shard_rows, d), BF16),
                pltpu.VMEM((tp_n, ids.shape[1], rows), jnp.int32),
                pltpu.VMEM((tp_n, gates.shape[1], rows), F32),
                pltpu.VMEM((slots, d), BF16),
                pltpu.VMEM((ep_n * local, slots), F32),
                pltpu.VMEM((slots, d), BF16),
                pltpu.VMEM((ep_n, local, LANES), F32),
                pltpu.VMEM((local, slots, hid), F32),
                pltpu.VMEM((local, slots, hid), F32),
                pltpu.VMEM((local, slots, hid), BF16),
                pltpu.VMEM((local, slots, LANES), F32),
                pltpu.VMEM((slots, d), F32),
                pltpu.VMEM((slots, d), F32),
                pltpu.VMEM((shard_rows, d), F32),
                pltpu.VMEM((ny, rows, d), F32),
                pltpu.VMEM((ny, 2, slots // ep_n, d // tp_n), F32),
                pltpu.VMEM((2, slots // ep_n, d // tp_n), F32),
                pltpu.VMEM((slots, shard_rows), BF16),
                pltpu.VMEM((shard_rows, slots), BF16),
                pltpu.VMEM((LANES, LANES), F32),
                dma((3, local)), dma((3,)),
                dma((kcs, ny)), dma((kcs, ny)),
                dma((2, ny)), dma((2, ny)),
                dma((kcs, nx)), dma((kcs, nx)),
                dma((nx,)), dma((nx,)),
                dma((kcs, nx - 2)), dma((kcs, nx - 2)),
                dma((kcs, 2, ny)), dma((kcs, 2, ny)),
                dma((kcs, 2)), dma((kcs, 2)),
                dma((kcs, ny)), dma((kcs, ny)),
            ],
            compiler_params=pltpu.CompilerParams(collective_id=0, has_side_effects=True,
                                                 vmem_limit_bytes=60 * 1024 * 1024),
        )(tok, ids.T, gates.T, w_gate, w_up, w_down)

    return jax.shard_map(
        block,
        mesh=mesh,
        in_specs=(P(TOKEN_AXES, None), P(TOKEN_AXES, None), P(TOKEN_AXES, None),
                  P('ep', None, 'tp'), P('ep', None, 'tp'), P('ep', 'tp', None)),
        out_specs=P(TOKEN_AXES, None),
        check_vma=False,
    )
```

```python
import functools

import jax
import jax.numpy as jnp
from jax import lax
from jax.experimental import pallas as pl
from jax.experimental.pallas import tpu as pltpu
from jax.sharding import PartitionSpec as P

TOKEN_AXES = ('dp', 'ep', 'tp')
LANES = 128
F32 = jnp.float32
BF16 = jnp.bfloat16


def split3(v):
    hi = v.astype(BF16)
    rest = v - hi.astype(F32)
    mid = rest.astype(BF16)
    low = (rest - mid.astype(F32)).astype(BF16)
    return hi, mid, low


def dot(a, b):
    return lax.dot_general(a, b, (((1,), (0,)), ((), ())), preferred_element_type=F32)


def dot_nt(a, b):
    return lax.dot_general(a, b, (((1,), (1,)), ((), ())), preferred_element_type=F32)


def moe_kernel(names, ep_n, tp_n, tok_hbm, ids_hbm, gate_hbm, wg_hbm, wu_hbm, wd_hbm, out_ref,
               wg, wu, wd, xg, idg, gg, xs, gs, xr, gr, acc_g, acc_u, hb, gb, ob, zr, yb, yr, yf, zs, slot_of, row_of, gcols,
               w_sem, in_sem, ag_ss, ag_rs, id_ss, id_rs, dx_ss, dx_rs, dg_ss, dg_rs, df_ss, df_rs, dq_ss, dq_rs, cx_ss, cx_rs, yf_ss, yf_rs, zf_ss, zf_rs, cy_ss, cy_rs):
    rows, d = tok_hbm.shape
    local = wg_hbm.shape[0]
    choices = ids_hbm.shape[0]
    shard_rows = rows * tp_n
    cap = 2 * shard_rows // ep_n
    slots = cap * ep_n
    per_tile = LANES // cap
    kcs = 4
    kw = d // kcs

    ep = lax.axis_index('ep')
    tp = lax.axis_index('tp')

    def device(ep_i, tp_i):
        at = {'dp': lax.axis_index('dp'), 'ep': ep_i, 'tp': tp_i}
        return tuple(at[n] for n in names)

    chips = ep_n // 2
    x_peers = [(dx, cf) for dx in (2, 1, chips - 1, 0) for cf in (0, 1) if (dx, cf) != (0, 0)]

    far = [p for p in x_peers if 2 * p[0] == chips]
    near = [p for p in x_peers if 2 * p[0] != chips]
    qw = kw // tp_n

    def x_target(p):
        return lax.rem(ep // 2 + p[0], chips) * 2 + lax.rem(ep + p[1], 2)

    def y_target(dt):
        return lax.rem(tp + dt, tp_n)

    def rdma(src, dst, ss, rs, dev):
        return pltpu.make_async_remote_copy(src_ref=src, dst_ref=dst, send_sem=ss, recv_sem=rs,
                                            device_id=dev, device_id_type=pl.DeviceIdType.MESH)

    my_rows = pl.ds(pl.multiple_of(tp * rows, rows), rows)
    my_slots = pl.ds(pl.multiple_of(ep * cap, cap), cap)

    def slots_of(e):
        return pl.ds(pl.multiple_of(e * cap, cap), cap)

    turns = (0, 1, tp_n - 1, 2)
    far_chip = lax.rem(ep // 2 + chips // 2, chips)
    far_slots = pl.ds(pl.multiple_of(far_chip * (2 * cap), 2 * cap), 2 * cap)

    def chunk(t):
        return pl.ds(pl.multiple_of(t * kw, kw), kw)

    def quarter(kc, t):
        return pl.ds(pl.multiple_of(kc * kw + t * qw, qw), qw)

    own = [pltpu.make_async_copy(ids_hbm, idg.at[tp], in_sem.at[0]),
           pltpu.make_async_copy(gate_hbm, gg.at[tp], in_sem.at[1]),
           pltpu.make_async_copy(tok_hbm, xg.at[my_rows], in_sem.at[2])]
    for c in own:
        c.start()

    for p in far:
        zr[slots_of(x_target(p)), :] = jnp.zeros((cap, d), F32)

    bar = pltpu.get_barrier_semaphore()
    for dt in range(1, tp_n):
        pl.semaphore_signal(bar, inc=1, device_id=device(ep, y_target(dt)), device_id_type=pl.DeviceIdType.MESH)
    for p in x_peers:
        pl.semaphore_signal(bar, inc=1, device_id=device(x_target(p), tp), device_id_type=pl.DeviceIdType.MESH)
    loads = []
    for i, (src, dst) in enumerate(((wg_hbm, wg), (wu_hbm, wu), (wd_hbm, wd))):
        for e in range(local):
            loads.append(pltpu.make_async_copy(src.at[e], dst.at[e], w_sem.at[i, e]))
    for c in own:
        c.wait()
    pl.semaphore_wait(bar, tp_n - 1 + len(x_peers))

    id_cps, ag_cps = [], []
    for dt in range(1, tp_n):
        dev = device(ep, y_target(dt))
        id_cps.append(rdma(idg.at[tp], idg.at[tp], id_ss.at[0, dt - 1], id_rs.at[0, dt - 1], dev))
        id_cps.append(rdma(gg.at[tp], gg.at[tp], id_ss.at[1, dt - 1], id_rs.at[1, dt - 1], dev))
    for kc in range(kcs):
        for dt in (2, 1, 3):
            dev = device(ep, y_target(dt))
            part = xg.at[my_rows, chunk(y_target(dt + turns[kc]))]
            ag_cps.append(rdma(part, part, ag_ss.at[kc, dt - 1], ag_rs.at[kc, dt - 1], dev))
    for c in id_cps + ag_cps:
        c.start()
    for c in loads:
        c.start()
    for c in id_cps:
        c.wait_recv()

    ids = jnp.concatenate([idg[q] for q in range(tp_n)], axis=1)
    gates = jnp.concatenate([gg[q] for q in range(tp_n)], axis=1)
    b_iota = lax.broadcasted_iota(jnp.int32, (ep_n, shard_rows), 0)
    used = jnp.zeros((ep_n, shard_rows), F32)
    for j in range(choices):
        used = jnp.where(ids[j:j + 1, :] // local == b_iota, 1.0, used)
    before = (lax.broadcasted_iota(jnp.int32, (shard_rows, shard_rows), 0)
              < lax.broadcasted_iota(jnp.int32, (shard_rows, shard_rows), 1)).astype(F32).astype(BF16)
    rank = dot(used.astype(BF16), before)
    place = jnp.where(used > 0.0, rank, -1.0)
    in_slot = lax.broadcasted_iota(jnp.int32, (cap, shard_rows), 0).astype(F32)
    for b in range(ep_n):
        hit = jnp.where(place[b:b + 1, :] == in_slot, 1.0, 0.0)
        slot_of[pl.ds(b * cap, cap), :] = hit.astype(BF16)

    dx_cps, dg_cps, df_cps = [], [], []
    for kc in range(kcs):
        cols = chunk(y_target(turns[kc]))
        for dt in range(1, tp_n):
            ag_cps[kc * (tp_n - 1) + {2: 0, 1: 1, 3: 2}[dt]].wait_recv()
        xs[:, cols] = dot(slot_of[...], xg[:, cols]).astype(BF16)
        if kc == 0:
            for i, p in enumerate(far):
                to = x_target(p)
                c = rdma(xs.at[slots_of(to), cols], xr.at[my_slots, cols], df_ss.at[i], df_rs.at[i], device(to, tp))
                c.start()
                df_cps.append(c)
        for i, p in enumerate(near):
            to = x_target(p)
            c = rdma(xs.at[slots_of(to), cols], xr.at[my_slots, cols], dx_ss.at[kc, i], dx_rs.at[kc, i], device(to, tp))
            c.start()
            dx_cps.append(c)
        xr[my_slots, cols] = xs[my_slots, cols]
        if kc == 0:
            e_iota = lax.broadcasted_iota(jnp.int32, (ep_n * local, shard_rows), 0)
            gate_of = jnp.zeros((ep_n * local, shard_rows), F32)
            for j in range(choices):
                gate_of = jnp.where(ids[j:j + 1, :] == e_iota, gates[j:j + 1, :], gate_of)
            g1, g2, g3 = split3(gate_of)
            gs[...] = dot_nt(g3, slot_of[...]) + dot_nt(g2, slot_of[...]) + dot_nt(g1, slot_of[...])

            def gate_tile(b):
                return (pl.ds(pl.multiple_of(b * local, local), local),
                        pl.ds(pl.multiple_of(b // per_tile * LANES, LANES), LANES))

            for i, p in enumerate(x_peers):
                to = x_target(p)
                c = rdma(gs.at[gate_tile(to)], gr.at[ep], dg_ss.at[i], dg_rs.at[i], device(to, tp))
                c.start()
                dg_cps.append(c)
            gr[ep] = gs[gate_tile(ep)]
    row_of[...] = jnp.transpose(slot_of[...].astype(F32)).astype(BF16)

    for c in df_cps:
        c.wait_recv()
    dq_cps = {}
    for dt in (3, 1, 2):
        part = xr.at[far_slots, chunk(tp)]
        dq_cps[dt] = rdma(part, part, dq_ss.at[dt - 1], dq_rs.at[dt - 1], device(ep, y_target(dt)))
        dq_cps[dt].start()
    for c in loads:
        c.wait()
    for kc in range(kcs):
        cols = chunk(y_target(turns[kc]))
        for c in dx_cps[kc * len(near):(kc + 1) * len(near)]:
            c.wait_recv()
        if kc > 0:
            dq_cps[tp_n - turns[kc]].wait_recv()
        if kc == 0:
            for c in dg_cps:
                c.wait_recv()

            lanes_of_mine = pl.ds(pl.multiple_of(lax.rem(ep, per_tile) * cap, cap), cap)
            for a in range(ep_n):
                gcols[...] = jnp.transpose(jnp.concatenate([gr[a]] * (LANES // local), axis=0))
                cols_a = gcols[lanes_of_mine, :]
                for e in range(local):
                    gb[e, pl.ds(a * cap, cap), :] = jnp.broadcast_to(cols_a[:, e:e + 1], (cap, LANES))

        def up(e, carry, kc=kc, cols=cols):
            x = xr[:, cols]
            a = dot(x, wg[e, cols, :])
            b = dot(x, wu[e, cols, :])
            if kc > 0:
                a = a + acc_g[e]
                b = b + acc_u[e]
            if kc < kcs - 1:
                acc_g[e] = a
                acc_u[e] = b
            else:
                h = a * jax.nn.sigmoid(a) * b
                g = gb[e]
                on = jnp.concatenate([g] * (h.shape[1] // LANES), axis=1) > 0.0
                hb[e] = jnp.where(on, h, 0.0).astype(BF16)
            return carry

        lax.fori_loop(0, local, up, 0, unroll=True)

    cx_cps, yf_cps, zf_cps, cy_cps = [], [], [], []

    def down(kc):
        cols = pl.ds(kc * kw, kw)
        total = None
        for e in range(local):
            o = dot(hb[e], wd[e, :, cols]) * jnp.concatenate([gb[e]] * (kw // LANES), axis=1)
            total = o if total is None else total + o
        ob[:, cols] = total
        zr[my_slots, cols] = ob[my_slots, cols]
        for j, p in enumerate(far):
            for dt in (2, 1, 3):
                q = y_target(dt)
                c = rdma(ob.at[slots_of(x_target(p)), quarter(kc, q)], yf.at[dt - 1, j, :, pl.ds(kc * qw, qw)],
                         yf_ss.at[kc, j, dt - 1], yf_rs.at[kc, j, dt - 1], device(ep, q))
                c.start()
                yf_cps.append(c)

    def send_near(kc):
        cols = pl.ds(kc * kw, kw)
        for i, p in enumerate(near):
            to = x_target(p)
            c = rdma(ob.at[slots_of(to), cols], zr.at[my_slots, cols], cx_ss.at[kc, i], cx_rs.at[kc, i], device(to, tp))
            c.start()
            cx_cps.append(c)

    def send_far(kc):
        part = pl.ds(kc * qw, qw)
        per = len(far) * (tp_n - 1)
        for c in yf_cps[kc * per:(kc + 1) * per]:
            c.wait_recv()
        for j, p in enumerate(far):
            to = x_target(p)
            total = ob[slots_of(to), quarter(kc, tp)]
            for i in range(tp_n - 1):
                total = total + yf[i, j, :, part]
            zs[j, :, part] = total
            c = rdma(zs.at[j, :, part], zr.at[my_slots, quarter(kc, tp)], zf_ss.at[kc, j], zf_rs.at[kc, j],
                     device(to, tp))
            c.start()
            zf_cps.append(c)

    lead = kcs // 2
    for kc in range(kcs):
        down(kc)
        if kc < lead:
            send_near(kc)
    for kc in range(kcs):
        send_far(kc)
        if kc + lead < kcs:
            send_near(kc + lead)

    for kc in range(kcs):
        cols = pl.ds(kc * kw, kw)
        for c in cx_cps[kc * len(near):(kc + 1) * len(near)] + zf_cps[kc * len(far):(kc + 1) * len(far)]:
            c.wait_recv()
        z1, z2, z3 = split3(zr[:, cols])
        pick = row_of[...]
        yb[:, cols] = dot(pick, z3) + dot(pick, z2) + dot(pick, z1)
        for dt in (2, 1, 3):
            to = y_target(dt)
            src = yb.at[pl.ds(pl.multiple_of(to * rows, rows), rows), cols]
            c = rdma(src, yr.at[dt - 1, :, cols], cy_ss.at[kc, dt - 1], cy_rs.at[kc, dt - 1], device(ep, to))
            c.start()
            cy_cps.append(c)
    for kc in range(kcs):
        cols = pl.ds(kc * kw, kw)
        for i in range(tp_n - 1):
            cy_cps[kc * (tp_n - 1) + i].wait_recv()
        total = yb[my_rows, cols]
        for i in range(tp_n - 1):
            total = total + yr[i, :, cols]
        out_ref[:, cols] = total.astype(BF16)

    for c in id_cps + ag_cps + dx_cps + dg_cps + df_cps + list(dq_cps.values()) + cx_cps + yf_cps + zf_cps + cy_cps:
        c.wait_send()


def solution(mesh):
    ep_n = mesh.shape['ep']
    tp_n = mesh.shape['tp']
    names = tuple(mesh.axis_names)

    def block(tok, ids, gates, w_gate, w_up, w_down):
        rows, d = tok.shape
        local, _, hid = w_gate.shape
        shard_rows = rows * tp_n
        slots = 2 * shard_rows
        kcs = 4
        nx = ep_n - 1
        ny = tp_n - 1
        any_spec = pl.BlockSpec(memory_space=pl.ANY)
        dma = pltpu.SemaphoreType.DMA
        return pl.pallas_call(
            functools.partial(moe_kernel, names, ep_n, tp_n),
            out_shape=pltpu.VMEM((rows, d), BF16),
            in_specs=[any_spec] * 6,
            out_specs=pl.BlockSpec(memory_space=pltpu.VMEM),
            scratch_shapes=[
                pltpu.VMEM((local, d, hid), BF16),
                pltpu.VMEM((local, d, hid), BF16),
                pltpu.VMEM((local, hid, d), BF16),
                pltpu.VMEM((shard_rows, d), BF16),
                pltpu.VMEM((tp_n, ids.shape[1], rows), jnp.int32),
                pltpu.VMEM((tp_n, gates.shape[1], rows), F32),
                pltpu.VMEM((slots, d), BF16),
                pltpu.VMEM((ep_n * local, slots), F32),
                pltpu.VMEM((slots, d), BF16),
                pltpu.VMEM((ep_n, local, LANES), F32),
                pltpu.VMEM((local, slots, hid), F32),
                pltpu.VMEM((local, slots, hid), F32),
                pltpu.VMEM((local, slots, hid), BF16),
                pltpu.VMEM((local, slots, LANES), F32),
                pltpu.VMEM((slots, d), F32),
                pltpu.VMEM((slots, d), F32),
                pltpu.VMEM((shard_rows, d), F32),
                pltpu.VMEM((ny, rows, d), F32),
                pltpu.VMEM((ny, 2, slots // ep_n, d // tp_n), F32),
                pltpu.VMEM((2, slots // ep_n, d // tp_n), F32),
                pltpu.VMEM((slots, shard_rows), BF16),
                pltpu.VMEM((shard_rows, slots), BF16),
                pltpu.VMEM((LANES, LANES), F32),
                dma((3, local)), dma((3,)),
                dma((kcs, ny)), dma((kcs, ny)),
                dma((2, ny)), dma((2, ny)),
                dma((kcs, nx - 2)), dma((kcs, nx - 2)),
                dma((nx,)), dma((nx,)),
                dma((2,)), dma((2,)),
                dma((ny,)), dma((ny,)),
                dma((kcs, nx - 2)), dma((kcs, nx - 2)),
                dma((kcs, 2, ny)), dma((kcs, 2, ny)),
                dma((kcs, 2)), dma((kcs, 2)),
                dma((kcs, ny)), dma((kcs, ny)),
            ],
            compiler_params=pltpu.CompilerParams(collective_id=0, has_side_effects=True,
                                                 vmem_limit_bytes=60 * 1024 * 1024),
        )(tok, ids.T, gates.T, w_gate, w_up, w_down)

    return jax.shard_map(
        block,
        mesh=mesh,
        in_specs=(P(TOKEN_AXES, None), P(TOKEN_AXES, None), P(TOKEN_AXES, None),
                  P('ep', None, 'tp'), P('ep', None, 'tp'), P('ep', 'tp', None)),
        out_specs=P(TOKEN_AXES, None),
        check_vma=False,
    )
```

```python
import functools

import jax
import jax.numpy as jnp
from jax import lax
from jax.experimental import pallas as pl
from jax.experimental.pallas import tpu as pltpu
from jax.sharding import PartitionSpec as P

TOKEN_AXES = ('dp', 'ep', 'tp')
LANES = 128
CHUNKS = 4
F32 = jnp.float32
BF16 = jnp.bfloat16
MESH = pl.DeviceIdType.MESH


def split3(v):
    hi = v.astype(BF16)
    rest = v - hi.astype(F32)
    mid = rest.astype(BF16)
    low = (rest - mid.astype(F32)).astype(BF16)
    return hi, mid, low


def dot(a, b):
    return lax.dot_general(a, b, (((1,), (0,)), ((), ())), preferred_element_type=F32)


def dot_nt(a, b):
    return lax.dot_general(a, b, (((1,), (1,)), ((), ())), preferred_element_type=F32)


def arrived(ref, sem):
    pltpu.make_async_copy(ref, ref, sem).wait()


def moe_kernel(names, ep_n, tp_n, tok_hbm, ids_hbm, gate_hbm, wg_hbm, wu_hbm, wd_hbm, out_ref,
               wg, wu, wd, xg, idg, gg, xs, gs, xr, gr, acc_g, acc_u, hb, gb, ob, zr, yb, yr, yf, zs,
               slot_of, row_of, gcols,
               w_sem, in_sem, id_sem, ag_rs, dg_rs, df_rs, dx_rs, dq_rs, cx_rs, yf_rs, zf_rs, cy_rs, out_sem):
    rows, d = tok_hbm.shape
    local = wg_hbm.shape[0]
    choices = ids_hbm.shape[0]
    shard_rows = rows * tp_n
    cap = 2 * shard_rows // ep_n
    slots = cap * ep_n
    per_tile = LANES // cap
    kw = d // CHUNKS
    qw = kw // tp_n
    chips = ep_n // 2

    ep = lax.axis_index('ep')
    tp = lax.axis_index('tp')

    def device(ep_i, tp_i):
        at = {'dp': lax.axis_index('dp'), 'ep': ep_i, 'tp': tp_i}
        return tuple(at[n] for n in names)

    far = [(chips // 2, 0), (chips // 2, 1)]
    near = [(1, 0), (1, 1), (chips - 1, 0), (chips - 1, 1), (0, 1)]
    x_peers = far + near
    turns = (0, 1, tp_n - 1, 2)

    def x_target(p):
        return lax.rem(ep // 2 + p[0], chips) * 2 + lax.rem(ep + p[1], 2)

    def y_target(dt):
        return lax.rem(tp + dt, tp_n)

    def send(src, dst, ss, rs, dev):
        pltpu.make_async_remote_copy(src_ref=src, dst_ref=dst, send_sem=ss, recv_sem=rs,
                                     device_id=dev, device_id_type=MESH).start()

    def rows_at(i, n):
        return pl.ds(pl.multiple_of(i * n, n), n)

    def slots_of(e):
        return rows_at(e, cap)

    def chunk(t):
        return pl.ds(pl.multiple_of(t * kw, kw), kw)

    def quarter(kc, t):
        return pl.ds(pl.multiple_of(kc * kw + t * qw, qw), qw)

    my_rows = rows_at(tp, rows)
    my_slots = slots_of(ep)
    far_slots = rows_at(lax.rem(ep // 2 + chips // 2, chips), 2 * cap)
    near_rows = pl.ds(0, len(near) * cap)
    others = tp_n - 1

    own = [pltpu.make_async_copy(ids_hbm, idg.at[tp], in_sem.at[0]),
           pltpu.make_async_copy(gate_hbm, gg.at[tp], in_sem.at[1]),
           pltpu.make_async_copy(tok_hbm, xg.at[my_rows], in_sem.at[2])]
    for c in own:
        c.start()

    zr[far_slots, :] = jnp.zeros((2 * cap, d), F32)

    bar = pltpu.get_barrier_semaphore()
    for dt in range(1, tp_n):
        pl.semaphore_signal(bar, inc=1, device_id=device(ep, y_target(dt)), device_id_type=MESH)
    for p in x_peers:
        pl.semaphore_signal(bar, inc=1, device_id=device(x_target(p), tp), device_id_type=MESH)
    for c in own:
        c.wait()
    pl.semaphore_wait(bar, others + len(x_peers))

    for dt in range(1, tp_n):
        dev = device(ep, y_target(dt))
        send(idg.at[tp], idg.at[tp], id_sem.at[0], id_sem.at[1], dev)
        send(gg.at[tp], gg.at[tp], id_sem.at[2], id_sem.at[3], dev)
    for kc in range(CHUNKS):
        for dt in (2, 1, 3):
            part = xg.at[my_rows, chunk(y_target(dt + turns[kc]))]
            send(part, part, out_sem.at[0], ag_rs.at[kc], device(ep, y_target(dt)))
    for i, (src, dst) in enumerate(((wg_hbm, wg), (wu_hbm, wu), (wd_hbm, wd))):
        for e in range(local):
            pltpu.make_async_copy(src.at[e], dst.at[e], w_sem.at[i]).start()
    arrived(idg.at[pl.ds(0, others)], id_sem.at[1])
    arrived(gg.at[pl.ds(0, others)], id_sem.at[3])

    ids = jnp.concatenate([idg[q] for q in range(tp_n)], axis=1)
    gates = jnp.concatenate([gg[q] for q in range(tp_n)], axis=1)
    b_iota = lax.broadcasted_iota(jnp.int32, (ep_n, shard_rows), 0)
    used = jnp.zeros((ep_n, shard_rows), F32)
    for j in range(choices):
        used = jnp.where(ids[j:j + 1, :] // local == b_iota, 1.0, used)
    before = (lax.broadcasted_iota(jnp.int32, (shard_rows, shard_rows), 0)
              < lax.broadcasted_iota(jnp.int32, (shard_rows, shard_rows), 1)).astype(F32).astype(BF16)
    rank = dot(used.astype(BF16), before)
    place = jnp.where(used > 0.0, rank, -1.0)
    in_slot = lax.broadcasted_iota(jnp.int32, (cap, shard_rows), 0).astype(F32)
    for b in range(ep_n):
        hit = jnp.where(place[b:b + 1, :] == in_slot, 1.0, 0.0)
        slot_of[pl.ds(b * cap, cap), :] = hit.astype(BF16)

    e_iota = lax.broadcasted_iota(jnp.int32, (ep_n * local, shard_rows), 0)
    gate_of = jnp.zeros((ep_n * local, shard_rows), F32)
    for j in range(choices):
        gate_of = jnp.where(ids[j:j + 1, :] == e_iota, gates[j:j + 1, :], gate_of)
    g1, g2, g3 = split3(gate_of)
    gs[...] = dot_nt(g3, slot_of[...]) + dot_nt(g2, slot_of[...]) + dot_nt(g1, slot_of[...])

    def gate_tile(b):
        return (rows_at(b, local), rows_at(b // per_tile, LANES))

    for p in x_peers:
        to = x_target(p)
        send(gs.at[gate_tile(to)], gr.at[ep], out_sem.at[1], dg_rs.at[0], device(to, tp))
    gr[ep] = gs[gate_tile(ep)]

    for kc in range(CHUNKS):
        cols = chunk(y_target(turns[kc]))
        arrived(xg.at[pl.ds(0, others * rows), pl.ds(0, kw)], ag_rs.at[kc])
        xs[:, cols] = dot(slot_of[...], xg[:, cols]).astype(BF16)
        if kc == 0:
            for p in far:
                to = x_target(p)
                send(xs.at[slots_of(to), cols], xr.at[my_slots, cols], out_sem.at[2], df_rs.at[0], device(to, tp))
        for p in near:
            to = x_target(p)
            send(xs.at[slots_of(to), cols], xr.at[my_slots, cols], out_sem.at[3], dx_rs.at[kc], device(to, tp))
        xr[my_slots, cols] = xs[my_slots, cols]
    row_of[...] = jnp.transpose(slot_of[...].astype(F32)).astype(BF16)

    arrived(xs.at[pl.ds(0, 2 * cap), pl.ds(0, kw)], df_rs.at[0])
    for dt in (3, 1, 2):
        part = xr.at[far_slots, chunk(tp)]
        send(part, part, out_sem.at[4], dq_rs.at[dt - 1], device(ep, y_target(dt)))

    arrived(gr.at[pl.ds(0, len(x_peers))], dg_rs.at[0])
    lanes_of_mine = rows_at(lax.rem(ep, per_tile), cap)
    for a in range(ep_n):
        gcols[...] = jnp.transpose(jnp.concatenate([gr[a]] * (LANES // local), axis=0))
        cols_a = gcols[lanes_of_mine, :]
        for e in range(local):
            gb[e, pl.ds(a * cap, cap), :] = jnp.broadcast_to(cols_a[:, e:e + 1], (cap, LANES))

    arrived(wg, w_sem.at[0])
    arrived(wu, w_sem.at[1])
    for kc in range(CHUNKS):
        cols = chunk(y_target(turns[kc]))
        arrived(xr.at[near_rows, pl.ds(0, kw)], dx_rs.at[kc])
        if kc > 0:
            arrived(xr.at[pl.ds(0, 2 * cap), pl.ds(0, kw)], dq_rs.at[tp_n - turns[kc] - 1])

        def up(e, carry, kc=kc, cols=cols):
            x = xr[:, cols]
            a = dot(x, wg[e, cols, :])
            b = dot(x, wu[e, cols, :])
            if kc > 0:
                a = a + acc_g[e]
                b = b + acc_u[e]
            if kc < CHUNKS - 1:
                acc_g[e] = a
                acc_u[e] = b
            else:
                h = a * jax.nn.sigmoid(a) * b
                on = jnp.concatenate([gb[e]] * (h.shape[1] // LANES), axis=1) > 0.0
                hb[e] = jnp.where(on, h, 0.0).astype(BF16)
            return carry

        lax.fori_loop(0, local, up, 0, unroll=True)

    arrived(wd, w_sem.at[2])

    def down(kc):
        cols = pl.ds(kc * kw, kw)
        total = None
        for e in range(local):
            o = dot(hb[e], wd[e, :, cols]) * jnp.concatenate([gb[e]] * (kw // LANES), axis=1)
            total = o if total is None else total + o
        ob[:, cols] = total
        zr[my_slots, cols] = ob[my_slots, cols]
        for j, p in enumerate(far):
            for dt in (2, 1, 3):
                q = y_target(dt)
                send(ob.at[slots_of(x_target(p)), quarter(kc, q)], yf.at[dt - 1, j, :, pl.ds(kc * qw, qw)],
                     out_sem.at[5], yf_rs.at[kc], device(ep, q))

    def send_near(kc):
        cols = pl.ds(kc * kw, kw)
        for p in near:
            to = x_target(p)
            send(ob.at[slots_of(to), cols], zr.at[my_slots, cols], out_sem.at[6], cx_rs.at[kc], device(to, tp))

    def send_far(kc):
        part = pl.ds(kc * qw, qw)
        arrived(ob.at[pl.ds(0, others * 2 * cap), pl.ds(0, qw)], yf_rs.at[kc])
        for j, p in enumerate(far):
            to = x_target(p)
            total = ob[slots_of(to), quarter(kc, tp)]
            for i in range(others):
                total = total + yf[i, j, :, part]
            zs[j, :, part] = total
            send(zs.at[j, :, part], zr.at[my_slots, quarter(kc, tp)], out_sem.at[7], zf_rs.at[kc], device(to, tp))

    lead = CHUNKS // 2
    for kc in range(CHUNKS):
        down(kc)
        if kc < lead:
            send_near(kc)
    for kc in range(CHUNKS):
        send_far(kc)
        if kc + lead < CHUNKS:
            send_near(kc + lead)

    for kc in range(CHUNKS):
        cols = pl.ds(kc * kw, kw)
        arrived(zr.at[near_rows, cols], cx_rs.at[kc])
        arrived(zs.at[:, :, pl.ds(0, qw)], zf_rs.at[kc])
        z1, z2, z3 = split3(zr[:, cols])
        pick = row_of[...]
        yb[:, cols] = dot(pick, z3) + dot(pick, z2) + dot(pick, z1)
        for dt in (2, 1, 3):
            to = y_target(dt)
            send(yb.at[rows_at(to, rows), cols], yr.at[dt - 1, :, cols], out_sem.at[8], cy_rs.at[kc], device(ep, to))
    for kc in range(CHUNKS):
        cols = pl.ds(kc * kw, kw)
        arrived(yr.at[:, :, cols], cy_rs.at[kc])
        total = yb[my_rows, cols]
        for i in range(others):
            total = total + yr[i, :, cols]
        out_ref[:, cols] = total.astype(BF16)

    arrived(idg.at[pl.ds(0, others)], id_sem.at[0])
    arrived(gg.at[pl.ds(0, others)], id_sem.at[2])
    arrived(xg.at[pl.ds(0, others * rows)], out_sem.at[0])
    arrived(gr.at[pl.ds(0, len(x_peers))], out_sem.at[1])
    arrived(xs.at[pl.ds(0, 2 * cap), pl.ds(0, kw)], out_sem.at[2])
    arrived(xs.at[near_rows], out_sem.at[3])
    arrived(xs.at[pl.ds(0, others * 2 * cap), pl.ds(0, kw)], out_sem.at[4])
    arrived(yf, out_sem.at[5])
    arrived(ob.at[near_rows], out_sem.at[6])
    arrived(zs, out_sem.at[7])
    arrived(yr, out_sem.at[8])


def solution(mesh):
    ep_n = mesh.shape['ep']
    tp_n = mesh.shape['tp']
    names = tuple(mesh.axis_names)

    def block(tok, ids, gates, w_gate, w_up, w_down):
        rows, d = tok.shape
        local, _, hid = w_gate.shape
        choices = ids.shape[1]
        shard_rows = rows * tp_n
        slots = 2 * shard_rows
        cap = slots // ep_n
        ny = tp_n - 1
        any_spec = pl.BlockSpec(memory_space=pl.ANY)
        dma = pltpu.SemaphoreType.DMA
        return pl.pallas_call(
            functools.partial(moe_kernel, names, ep_n, tp_n),
            out_shape=pltpu.VMEM((rows, d), BF16),
            in_specs=[any_spec] * 6,
            out_specs=pl.BlockSpec(memory_space=pltpu.VMEM),
            scratch_shapes=[
                pltpu.VMEM((local, d, hid), BF16),
                pltpu.VMEM((local, d, hid), BF16),
                pltpu.VMEM((local, hid, d), BF16),
                pltpu.VMEM((shard_rows, d), BF16),
                pltpu.VMEM((tp_n, choices, rows), jnp.int32),
                pltpu.VMEM((tp_n, choices, rows), F32),
                pltpu.VMEM((slots, d), BF16),
                pltpu.VMEM((ep_n * local, slots), F32),
                pltpu.VMEM((slots, d), BF16),
                pltpu.VMEM((ep_n, local, LANES), F32),
                pltpu.VMEM((local, slots, hid), F32),
                pltpu.VMEM((local, slots, hid), F32),
                pltpu.VMEM((local, slots, hid), BF16),
                pltpu.VMEM((local, slots, LANES), F32),
                pltpu.VMEM((slots, d), F32),
                pltpu.VMEM((slots, d), F32),
                pltpu.VMEM((shard_rows, d), F32),
                pltpu.VMEM((ny, rows, d), F32),
                pltpu.VMEM((ny, 2, cap, d // tp_n), F32),
                pltpu.VMEM((2, cap, d // tp_n), F32),
                pltpu.VMEM((slots, shard_rows), BF16),
                pltpu.VMEM((shard_rows, slots), BF16),
                pltpu.VMEM((LANES, LANES), F32),
                dma((3,)), dma((3,)), dma((4,)), dma((CHUNKS,)), dma((1,)), dma((1,)), dma((CHUNKS,)), dma((ny,)),
                dma((CHUNKS,)), dma((CHUNKS,)), dma((CHUNKS,)), dma((CHUNKS,)), dma((9,)),
            ],
            compiler_params=pltpu.CompilerParams(collective_id=0, has_side_effects=True,
                                                 vmem_limit_bytes=60 * 1024 * 1024),
        )(tok, ids.T, gates.T, w_gate, w_up, w_down)

    return jax.shard_map(
        block,
        mesh=mesh,
        in_specs=(P(TOKEN_AXES, None), P(TOKEN_AXES, None), P(TOKEN_AXES, None),
                  P('ep', None, 'tp'), P('ep', None, 'tp'), P('ep', 'tp', None)),
        out_specs=P(TOKEN_AXES, None),
        check_vma=False,
    )
```

```python
import functools

import jax
import jax.numpy as jnp
from jax import lax
from jax.experimental import pallas as pl
from jax.experimental.pallas import tpu as pltpu
from jax.sharding import PartitionSpec as P

TOKEN_AXES = ('dp', 'ep', 'tp')
LANES = 128
CHUNKS = 4
F32 = jnp.float32
BF16 = jnp.bfloat16
MESH = pl.DeviceIdType.MESH


def split3(v):
    hi = v.astype(BF16)
    rest = v - hi.astype(F32)
    mid = rest.astype(BF16)
    low = (rest - mid.astype(F32)).astype(BF16)
    return hi, mid, low


def dot(a, b):
    return lax.dot_general(a, b, (((1,), (0,)), ((), ())), preferred_element_type=F32)


def dot_nt(a, b):
    return lax.dot_general(a, b, (((1,), (1,)), ((), ())), preferred_element_type=F32)


def arrived(ref, sem):
    pltpu.make_async_copy(ref, ref, sem).wait()


def moe_kernel(names, ep_n, tp_n, tok_hbm, ids_hbm, gate_hbm, wg_hbm, wu_hbm, wd_hbm, out_ref,
               wg, wu, wd, xg, idg, gg, xs, gs, xr, gr, acc_g, acc_u, hb, gb, ob, zr, yb, yr, yf, zs,
               slot_of, row_of, gcols,
               w_sem, in_sem, id_sem, ag_rs, dg_rs, df_rs, dx_rs, dq_rs, cx_rs, yf_rs, zf_rs, cy_rs, out_sem):
    rows, d = tok_hbm.shape
    local = wg_hbm.shape[0]
    choices = ids_hbm.shape[0]
    shard_rows = rows * tp_n
    cap = 2 * shard_rows // ep_n
    slots = cap * ep_n
    per_tile = LANES // cap
    kw = d // CHUNKS
    qw = kw // tp_n
    chips = ep_n // 2

    ep = lax.axis_index('ep')
    tp = lax.axis_index('tp')

    def device(ep_i, tp_i):
        at = {'dp': lax.axis_index('dp'), 'ep': ep_i, 'tp': tp_i}
        return tuple(at[n] for n in names)

    far = [(chips // 2, 0), (chips // 2, 1)]
    near = [(1, 0), (1, 1), (chips - 1, 0), (chips - 1, 1), (0, 1)]
    x_peers = far + near
    turns = (0, 1, tp_n - 1, 2)

    def x_target(p):
        return lax.rem(ep // 2 + p[0], chips) * 2 + lax.rem(ep + p[1], 2)

    def y_target(dt):
        return lax.rem(tp + dt, tp_n)

    def send(src, dst, ss, rs, dev):
        pltpu.make_async_remote_copy(src_ref=src, dst_ref=dst, send_sem=ss, recv_sem=rs,
                                     device_id=dev, device_id_type=MESH).start()

    def rows_at(i, n):
        return pl.ds(pl.multiple_of(i * n, n), n)

    def slots_of(e):
        return rows_at(e, cap)

    def chunk(t):
        return pl.ds(pl.multiple_of(t * kw, kw), kw)

    def half(t, h):
        return pl.ds(pl.multiple_of(t * kw + h * (kw // 2), kw // 2), kw // 2)

    def quarter(kc, t):
        return pl.ds(pl.multiple_of(kc * kw + t * qw, qw), qw)

    my_rows = rows_at(tp, rows)
    my_slots = slots_of(ep)
    far_slots = rows_at(lax.rem(ep // 2 + chips // 2, chips), 2 * cap)
    near_rows = pl.ds(0, len(near) * cap)
    others = tp_n - 1

    own = [pltpu.make_async_copy(ids_hbm, idg.at[tp], in_sem.at[0]),
           pltpu.make_async_copy(gate_hbm, gg.at[tp], in_sem.at[1]),
           pltpu.make_async_copy(tok_hbm, xg.at[my_rows], in_sem.at[2])]
    for c in own:
        c.start()

    zr[far_slots, :] = jnp.zeros((2 * cap, d), F32)

    bar = pltpu.get_barrier_semaphore()
    for dt in range(1, tp_n):
        pl.semaphore_signal(bar, inc=1, device_id=device(ep, y_target(dt)), device_id_type=MESH)
    for p in x_peers:
        pl.semaphore_signal(bar, inc=1, device_id=device(x_target(p), tp), device_id_type=MESH)
    for c in own:
        c.wait()
    pl.semaphore_wait(bar, others + len(x_peers))

    for dt in range(1, tp_n):
        dev = device(ep, y_target(dt))
        send(idg.at[tp], idg.at[tp], id_sem.at[0], id_sem.at[1], dev)
        send(gg.at[tp], gg.at[tp], id_sem.at[2], id_sem.at[3], dev)
    for h in range(2):
        for dt in (2, 1, 3):
            part = xg.at[my_rows, half(y_target(dt), h)]
            send(part, part, out_sem.at[0], ag_rs.at[h], device(ep, y_target(dt)))
    for kc in range(1, CHUNKS):
        for dt in (2, 1, 3):
            part = xg.at[my_rows, chunk(y_target(dt + turns[kc]))]
            send(part, part, out_sem.at[0], ag_rs.at[kc + 1], device(ep, y_target(dt)))
    for i, (src, dst) in enumerate(((wg_hbm, wg), (wu_hbm, wu), (wd_hbm, wd))):
        for e in range(local):
            pltpu.make_async_copy(src.at[e], dst.at[e], w_sem.at[i]).start()
    arrived(idg.at[pl.ds(0, others)], id_sem.at[1])
    arrived(gg.at[pl.ds(0, others)], id_sem.at[3])

    ids = jnp.concatenate([idg[q] for q in range(tp_n)], axis=1)
    gates = jnp.concatenate([gg[q] for q in range(tp_n)], axis=1)
    b_iota = lax.broadcasted_iota(jnp.int32, (ep_n, shard_rows), 0)
    used = jnp.zeros((ep_n, shard_rows), F32)
    for j in range(choices):
        used = jnp.where(ids[j:j + 1, :] // local == b_iota, 1.0, used)
    before = (lax.broadcasted_iota(jnp.int32, (shard_rows, shard_rows), 0)
              < lax.broadcasted_iota(jnp.int32, (shard_rows, shard_rows), 1)).astype(F32).astype(BF16)
    rank = dot(used.astype(BF16), before)
    place = jnp.where(used > 0.0, rank, -1.0)
    in_slot = lax.broadcasted_iota(jnp.int32, (cap, shard_rows), 0).astype(F32)
    for b in range(ep_n):
        hit = jnp.where(place[b:b + 1, :] == in_slot, 1.0, 0.0)
        slot_of[pl.ds(b * cap, cap), :] = hit.astype(BF16)

    e_iota = lax.broadcasted_iota(jnp.int32, (ep_n * local, shard_rows), 0)
    gate_of = jnp.zeros((ep_n * local, shard_rows), F32)
    for j in range(choices):
        gate_of = jnp.where(ids[j:j + 1, :] == e_iota, gates[j:j + 1, :], gate_of)
    g1, g2, g3 = split3(gate_of)
    gs[...] = dot_nt(g3, slot_of[...]) + dot_nt(g2, slot_of[...]) + dot_nt(g1, slot_of[...])

    def gate_tile(b):
        return (rows_at(b, local), rows_at(b // per_tile, LANES))

    for p in x_peers:
        to = x_target(p)
        send(gs.at[gate_tile(to)], gr.at[ep], out_sem.at[1], dg_rs.at[0], device(to, tp))
    gr[ep] = gs[gate_tile(ep)]

    for h in range(2):
        cols = half(tp, h)
        arrived(xg.at[pl.ds(0, others * rows), pl.ds(0, kw // 2)], ag_rs.at[h])
        xs[:, cols] = dot(slot_of[...], xg[:, cols]).astype(BF16)
        for p in far:
            to = x_target(p)
            send(xs.at[slots_of(to), cols], xr.at[my_slots, cols], out_sem.at[2], df_rs.at[h], device(to, tp))
    for kc in range(CHUNKS):
        cols = chunk(y_target(turns[kc]))
        if kc > 0:
            arrived(xg.at[pl.ds(0, others * rows), pl.ds(0, kw)], ag_rs.at[kc + 1])
            xs[:, cols] = dot(slot_of[...], xg[:, cols]).astype(BF16)
        for p in near:
            to = x_target(p)
            send(xs.at[slots_of(to), cols], xr.at[my_slots, cols], out_sem.at[3], dx_rs.at[kc], device(to, tp))
        xr[my_slots, cols] = xs[my_slots, cols]
    row_of[...] = jnp.transpose(slot_of[...].astype(F32)).astype(BF16)

    for h in range(2):
        arrived(xs.at[pl.ds(0, 2 * cap), pl.ds(0, kw // 2)], df_rs.at[h])
        for dt in (3, 1, 2):
            part = xr.at[far_slots, half(tp, h)]
            send(part, part, out_sem.at[4], dq_rs.at[dt - 1], device(ep, y_target(dt)))

    arrived(gr.at[pl.ds(0, len(x_peers))], dg_rs.at[0])
    lanes_of_mine = rows_at(lax.rem(ep, per_tile), cap)
    for a in range(ep_n):
        gcols[...] = jnp.transpose(jnp.concatenate([gr[a]] * (LANES // local), axis=0))
        cols_a = gcols[lanes_of_mine, :]
        for e in range(local):
            gb[e, pl.ds(a * cap, cap), :] = jnp.broadcast_to(cols_a[:, e:e + 1], (cap, LANES))

    arrived(wg, w_sem.at[0])
    arrived(wu, w_sem.at[1])
    for kc in range(CHUNKS):
        cols = chunk(y_target(turns[kc]))
        arrived(xr.at[near_rows, pl.ds(0, kw)], dx_rs.at[kc])
        if kc > 0:
            arrived(xr.at[pl.ds(0, 2 * cap), pl.ds(0, kw)], dq_rs.at[tp_n - turns[kc] - 1])

        def up(e, carry, kc=kc, cols=cols):
            x = xr[:, cols]
            a = dot(x, wg[e, cols, :])
            b = dot(x, wu[e, cols, :])
            if kc > 0:
                a = a + acc_g[e]
                b = b + acc_u[e]
            if kc < CHUNKS - 1:
                acc_g[e] = a
                acc_u[e] = b
            else:
                h = a * jax.nn.sigmoid(a) * b
                on = jnp.concatenate([gb[e]] * (h.shape[1] // LANES), axis=1) > 0.0
                hb[e] = jnp.where(on, h, 0.0).astype(BF16)
            return carry

        lax.fori_loop(0, local, up, 0, unroll=True)

    arrived(wd, w_sem.at[2])

    def down(kc):
        cols = pl.ds(kc * kw, kw)
        total = None
        for e in range(local):
            o = dot(hb[e], wd[e, :, cols]) * jnp.concatenate([gb[e]] * (kw // LANES), axis=1)
            total = o if total is None else total + o
        ob[:, cols] = total
        zr[my_slots, cols] = ob[my_slots, cols]
        for j, p in enumerate(far):
            for dt in (2, 1, 3):
                q = y_target(dt)
                send(ob.at[slots_of(x_target(p)), quarter(kc, q)], yf.at[dt - 1, j, :, pl.ds(kc * qw, qw)],
                     out_sem.at[5], yf_rs.at[kc], device(ep, q))

    def send_near(kc):
        cols = pl.ds(kc * kw, kw)
        for p in near:
            to = x_target(p)
            send(ob.at[slots_of(to), cols], zr.at[my_slots, cols], out_sem.at[6], cx_rs.at[kc], device(to, tp))

    def send_far(kc):
        part = pl.ds(kc * qw, qw)
        arrived(ob.at[pl.ds(0, others * 2 * cap), pl.ds(0, qw)], yf_rs.at[kc])
        for j, p in enumerate(far):
            to = x_target(p)
            total = ob[slots_of(to), quarter(kc, tp)]
            for i in range(others):
                total = total + yf[i, j, :, part]
            zs[j, :, part] = total
            send(zs.at[j, :, part], zr.at[my_slots, quarter(kc, tp)], out_sem.at[7], zf_rs.at[kc], device(to, tp))

    lead = CHUNKS // 2
    for kc in range(CHUNKS):
        down(kc)
        if kc < lead:
            send_near(kc)
    send_far(0)
    for kc in range(1, CHUNKS):
        send_far(kc)
        if kc + lead <= CHUNKS:
            send_near(kc + lead - 1)

    for kc in range(CHUNKS):
        cols = pl.ds(kc * kw, kw)
        arrived(zr.at[near_rows, cols], cx_rs.at[kc])
        arrived(zs.at[:, :, pl.ds(0, qw)], zf_rs.at[kc])
        z1, z2, z3 = split3(zr[:, cols])
        pick = row_of[...]
        yb[:, cols] = dot(pick, z3) + dot(pick, z2) + dot(pick, z1)
        for dt in (2, 1, 3):
            to = y_target(dt)
            send(yb.at[rows_at(to, rows), cols], yr.at[dt - 1, :, cols], out_sem.at[8], cy_rs.at[kc], device(ep, to))
    for kc in range(CHUNKS):
        cols = pl.ds(kc * kw, kw)
        arrived(yr.at[:, :, cols], cy_rs.at[kc])
        total = yb[my_rows, cols]
        for i in range(others):
            total = total + yr[i, :, cols]
        out_ref[:, cols] = total.astype(BF16)

    arrived(idg.at[pl.ds(0, others)], id_sem.at[0])
    arrived(gg.at[pl.ds(0, others)], id_sem.at[2])
    arrived(xg.at[pl.ds(0, others * rows)], out_sem.at[0])
    arrived(gr.at[pl.ds(0, len(x_peers))], out_sem.at[1])
    arrived(xs.at[pl.ds(0, 2 * cap), pl.ds(0, kw)], out_sem.at[2])
    arrived(xs.at[near_rows], out_sem.at[3])
    arrived(xs.at[pl.ds(0, others * 2 * cap), pl.ds(0, kw)], out_sem.at[4])
    arrived(yf, out_sem.at[5])
    arrived(ob.at[near_rows], out_sem.at[6])
    arrived(zs, out_sem.at[7])
    arrived(yr, out_sem.at[8])


def solution(mesh):
    ep_n = mesh.shape['ep']
    tp_n = mesh.shape['tp']
    names = tuple(mesh.axis_names)

    def block(tok, ids, gates, w_gate, w_up, w_down):
        rows, d = tok.shape
        local, _, hid = w_gate.shape
        choices = ids.shape[1]
        shard_rows = rows * tp_n
        slots = 2 * shard_rows
        cap = slots // ep_n
        ny = tp_n - 1
        any_spec = pl.BlockSpec(memory_space=pl.ANY)
        dma = pltpu.SemaphoreType.DMA
        return pl.pallas_call(
            functools.partial(moe_kernel, names, ep_n, tp_n),
            out_shape=pltpu.VMEM((rows, d), BF16),
            in_specs=[any_spec] * 6,
            out_specs=pl.BlockSpec(memory_space=pltpu.VMEM),
            scratch_shapes=[
                pltpu.VMEM((local, d, hid), BF16),
                pltpu.VMEM((local, d, hid), BF16),
                pltpu.VMEM((local, hid, d), BF16),
                pltpu.VMEM((shard_rows, d), BF16),
                pltpu.VMEM((tp_n, choices, rows), jnp.int32),
                pltpu.VMEM((tp_n, choices, rows), F32),
                pltpu.VMEM((slots, d), BF16),
                pltpu.VMEM((ep_n * local, slots), F32),
                pltpu.VMEM((slots, d), BF16),
                pltpu.VMEM((ep_n, local, LANES), F32),
                pltpu.VMEM((local, slots, hid), F32),
                pltpu.VMEM((local, slots, hid), F32),
                pltpu.VMEM((local, slots, hid), BF16),
                pltpu.VMEM((local, slots, LANES), F32),
                pltpu.VMEM((slots, d), F32),
                pltpu.VMEM((slots, d), F32),
                pltpu.VMEM((shard_rows, d), F32),
                pltpu.VMEM((ny, rows, d), F32),
                pltpu.VMEM((ny, 2, cap, d // tp_n), F32),
                pltpu.VMEM((2, cap, d // tp_n), F32),
                pltpu.VMEM((slots, shard_rows), BF16),
                pltpu.VMEM((shard_rows, slots), BF16),
                pltpu.VMEM((LANES, LANES), F32),
                dma((3,)), dma((3,)), dma((4,)), dma((CHUNKS + 1,)), dma((1,)), dma((2,)), dma((CHUNKS,)), dma((ny,)),
                dma((CHUNKS,)), dma((CHUNKS,)), dma((CHUNKS,)), dma((CHUNKS,)), dma((9,)),
            ],
            compiler_params=pltpu.CompilerParams(collective_id=0, has_side_effects=True,
                                                 vmem_limit_bytes=60 * 1024 * 1024),
        )(tok, ids.T, gates.T, w_gate, w_up, w_down)

    return jax.shard_map(
        block,
        mesh=mesh,
        in_specs=(P(TOKEN_AXES, None), P(TOKEN_AXES, None), P(TOKEN_AXES, None),
                  P('ep', None, 'tp'), P('ep', None, 'tp'), P('ep', 'tp', None)),
        out_specs=P(TOKEN_AXES, None),
        check_vma=False,
    )
```

```python
import functools

import jax
import jax.numpy as jnp
from jax import lax
from jax.experimental import pallas as pl
from jax.experimental.pallas import tpu as pltpu
from jax.sharding import PartitionSpec as P

TOKEN_AXES = ('dp', 'ep', 'tp')
LANES = 128
CHUNKS = 4
STRAIGHT = 2
F32 = jnp.float32
BF16 = jnp.bfloat16
MESH = pl.DeviceIdType.MESH


def split3(v):
    hi = v.astype(BF16)
    rest = v - hi.astype(F32)
    mid = rest.astype(BF16)
    low = (rest - mid.astype(F32)).astype(BF16)
    return hi, mid, low


def dot(a, b):
    return lax.dot_general(a, b, (((1,), (0,)), ((), ())), preferred_element_type=F32)


def dot_nt(a, b):
    return lax.dot_general(a, b, (((1,), (1,)), ((), ())), preferred_element_type=F32)


def arrived(ref, sem):
    pltpu.make_async_copy(ref, ref, sem).wait()


def moe_kernel(names, ep_n, tp_n, tok_hbm, ids_hbm, gate_hbm, wg_hbm, wu_hbm, wd_hbm, out_ref,
               wg, wu, wd, xg, idg, gg, xs, gs, xr, gr, acc_g, acc_u, hb, gb, ob, zr, yb, yr, pr, zs,
               slot_of, row_of, gcols,
               w_sem, in_sem, id_sem, ag_rs, dg_rs, df_rs, dx_rs, dq_rs, pr_rs, cx_rs, cy_rs, out_sem):
    rows, d = tok_hbm.shape
    local = wg_hbm.shape[0]
    choices = ids_hbm.shape[0]
    shard_rows = rows * tp_n
    cap = 2 * shard_rows // ep_n
    slots = cap * ep_n
    per_tile = LANES // cap
    kw = d // CHUNKS
    unit = 2 * LANES
    units = d // unit
    chips = ep_n // 2

    ep = lax.axis_index('ep')
    tp = lax.axis_index('tp')

    def device(ep_i, tp_i):
        at = {'dp': lax.axis_index('dp'), 'ep': ep_i, 'tp': tp_i}
        return tuple(at[n] for n in names)

    far = [(chips // 2, 0), (chips // 2, 1)]
    near = [(1, 0), (1, 1), (chips - 1, 0), (chips - 1, 1), (0, 1)]
    x_peers = far + near
    turns = (0, 1, tp_n - 1, 2)

    def x_target(p):
        return lax.rem(ep // 2 + p[0], chips) * 2 + lax.rem(ep + p[1], 2)

    def y_target(dt):
        return lax.rem(tp + dt, tp_n)

    def send(src, dst, ss, rs, dev):
        pltpu.make_async_remote_copy(src_ref=src, dst_ref=dst, send_sem=ss, recv_sem=rs,
                                     device_id=dev, device_id_type=MESH).start()

    def rows_at(i, n):
        return pl.ds(pl.multiple_of(i * n, n), n)

    def slots_of(e):
        return rows_at(e, cap)

    def chunk(t):
        return pl.ds(pl.multiple_of(t * kw, kw), kw)

    def half(t, h):
        return pl.ds(pl.multiple_of(t * kw + h * (kw // 2), kw // 2), kw // 2)

    my_rows = rows_at(tp, rows)
    my_slots = slots_of(ep)
    far_slots = rows_at(lax.rem(ep // 2 + chips // 2, chips), 2 * cap)
    near_rows = pl.ds(0, len(near) * cap)
    others = tp_n - 1

    own = [pltpu.make_async_copy(ids_hbm, idg.at[tp], in_sem.at[0]),
           pltpu.make_async_copy(gate_hbm, gg.at[tp], in_sem.at[1]),
           pltpu.make_async_copy(tok_hbm, xg.at[my_rows], in_sem.at[2])]
    for c in own:
        c.start()

    bar = pltpu.get_barrier_semaphore()
    for dt in range(1, tp_n):
        pl.semaphore_signal(bar, inc=1, device_id=device(ep, y_target(dt)), device_id_type=MESH)
    for p in x_peers:
        pl.semaphore_signal(bar, inc=1, device_id=device(x_target(p), tp), device_id_type=MESH)
    for c in own:
        c.wait()
    pl.semaphore_wait(bar, others + len(x_peers))

    for dt in range(1, tp_n):
        dev = device(ep, y_target(dt))
        send(idg.at[tp], idg.at[tp], id_sem.at[0], id_sem.at[1], dev)
        send(gg.at[tp], gg.at[tp], id_sem.at[2], id_sem.at[3], dev)
    for h in range(2):
        for dt in (2, 1, 3):
            part = xg.at[my_rows, half(y_target(dt), h)]
            send(part, part, out_sem.at[0], ag_rs.at[h], device(ep, y_target(dt)))
    for kc in range(1, CHUNKS):
        for dt in (2, 1, 3):
            part = xg.at[my_rows, chunk(y_target(dt + turns[kc]))]
            send(part, part, out_sem.at[0], ag_rs.at[kc + 1], device(ep, y_target(dt)))
    for i, (src, dst) in enumerate(((wg_hbm, wg), (wu_hbm, wu), (wd_hbm, wd))):
        for e in range(local):
            pltpu.make_async_copy(src.at[e], dst.at[e], w_sem.at[i]).start()
    arrived(idg.at[pl.ds(0, others)], id_sem.at[1])
    arrived(gg.at[pl.ds(0, others)], id_sem.at[3])

    ids = jnp.concatenate([idg[q] for q in range(tp_n)], axis=1)
    gates = jnp.concatenate([gg[q] for q in range(tp_n)], axis=1)
    b_iota = lax.broadcasted_iota(jnp.int32, (ep_n, shard_rows), 0)
    used = jnp.zeros((ep_n, shard_rows), F32)
    for j in range(choices):
        used = jnp.where(ids[j:j + 1, :] // local == b_iota, 1.0, used)
    before = (lax.broadcasted_iota(jnp.int32, (shard_rows, shard_rows), 0)
              < lax.broadcasted_iota(jnp.int32, (shard_rows, shard_rows), 1)).astype(F32).astype(BF16)
    rank = dot(used.astype(BF16), before)
    place = jnp.where(used > 0.0, rank, -1.0)
    in_slot = lax.broadcasted_iota(jnp.int32, (cap, shard_rows), 0).astype(F32)
    for b in range(ep_n):
        hit = jnp.where(place[b:b + 1, :] == in_slot, 1.0, 0.0)
        slot_of[pl.ds(b * cap, cap), :] = hit.astype(BF16)

    e_iota = lax.broadcasted_iota(jnp.int32, (ep_n * local, shard_rows), 0)
    gate_of = jnp.zeros((ep_n * local, shard_rows), F32)
    for j in range(choices):
        gate_of = jnp.where(ids[j:j + 1, :] == e_iota, gates[j:j + 1, :], gate_of)
    g1, g2, g3 = split3(gate_of)
    gs[...] = dot_nt(g3, slot_of[...]) + dot_nt(g2, slot_of[...]) + dot_nt(g1, slot_of[...])

    def gate_tile(b):
        return (rows_at(b, local), rows_at(b // per_tile, LANES))

    for p in x_peers:
        to = x_target(p)
        send(gs.at[gate_tile(to)], gr.at[ep], out_sem.at[1], dg_rs.at[0], device(to, tp))
    gr[ep] = gs[gate_tile(ep)]

    for h in range(2):
        cols = half(tp, h)
        arrived(xg.at[pl.ds(0, others * rows), pl.ds(0, kw // 2)], ag_rs.at[h])
        xs[:, cols] = dot(slot_of[...], xg[:, cols]).astype(BF16)
        for p in far:
            to = x_target(p)
            send(xs.at[slots_of(to), cols], xr.at[my_slots, cols], out_sem.at[2], df_rs.at[h], device(to, tp))
    for kc in range(CHUNKS):
        cols = chunk(y_target(turns[kc]))
        if kc > 0:
            arrived(xg.at[pl.ds(0, others * rows), pl.ds(0, kw)], ag_rs.at[kc + 1])
            xs[:, cols] = dot(slot_of[...], xg[:, cols]).astype(BF16)
        for p in near:
            to = x_target(p)
            send(xs.at[slots_of(to), cols], xr.at[my_slots, cols], out_sem.at[3], dx_rs.at[kc], device(to, tp))
        xr[my_slots, cols] = xs[my_slots, cols]
    row_of[...] = jnp.transpose(slot_of[...].astype(F32)).astype(BF16)

    for h in range(2):
        arrived(xs.at[pl.ds(0, 2 * cap), pl.ds(0, kw // 2)], df_rs.at[h])
        for dt in (3, 1, 2):
            part = xr.at[far_slots, half(tp, h)]
            send(part, part, out_sem.at[4], dq_rs.at[dt - 1], device(ep, y_target(dt)))

    arrived(gr.at[pl.ds(0, len(x_peers))], dg_rs.at[0])
    lanes_of_mine = rows_at(lax.rem(ep, per_tile), cap)
    for a in range(ep_n):
        gcols[...] = jnp.transpose(jnp.concatenate([gr[a]] * (LANES // local), axis=0))
        cols_a = gcols[lanes_of_mine, :]
        for e in range(local):
            gb[e, pl.ds(a * cap, cap), :] = jnp.broadcast_to(cols_a[:, e:e + 1], (cap, LANES))

    arrived(wg, w_sem.at[0])
    arrived(wu, w_sem.at[1])
    for kc in range(CHUNKS):
        cols = chunk(y_target(turns[kc]))
        arrived(xr.at[near_rows, pl.ds(0, kw)], dx_rs.at[kc])
        if kc > 0:
            arrived(xr.at[pl.ds(0, 2 * cap), pl.ds(0, kw)], dq_rs.at[tp_n - turns[kc] - 1])

        def up(e, carry, kc=kc, cols=cols):
            x = xr[:, cols]
            a = dot(x, wg[e, cols, :])
            b = dot(x, wu[e, cols, :])
            if kc > 0:
                a = a + acc_g[e]
                b = b + acc_u[e]
            if kc < CHUNKS - 1:
                acc_g[e] = a
                acc_u[e] = b
            else:
                h = a * jax.nn.sigmoid(a) * b
                on = jnp.concatenate([gb[e]] * (h.shape[1] // LANES), axis=1) > 0.0
                hb[e] = jnp.where(on, h, 0.0).astype(BF16)
            return carry

        lax.fori_loop(0, local, up, 0, unroll=True)

    arrived(wd, w_sem.at[2])
    parity = lax.rem(tp, 2)
    pairs = (tp + 1 - 2 * parity, y_target(tp_n - 1 + 2 * parity))
    group = slots // 2

    def span(u):
        return pl.ds(u * unit, unit)

    def mine(u):
        return pl.ds(pl.multiple_of(u * unit + parity * LANES, LANES), LANES)

    def theirs(u):
        return pl.ds(pl.multiple_of(u * unit + (1 - parity) * LANES, LANES), LANES)

    def packed(u):
        return pl.ds((u - STRAIGHT) * LANES, LANES)

    def down(u):
        cols = span(u)
        total = None
        for e in range(local):
            o = dot(hb[e], wd[e, :, cols]) * jnp.concatenate([gb[e]] * (unit // LANES), axis=1)
            total = o if total is None else total + o
        ob[:, cols] = total
        if u < STRAIGHT:
            for p in x_peers:
                to = x_target(p)
                send(ob.at[slots_of(to), cols], zr.at[my_slots, cols], out_sem.at[5], cx_rs.at[u], device(to, tp))
            zr[my_slots, cols] = ob[my_slots, cols]
        else:
            for g, to in enumerate(pairs):
                part = pl.ds(g * group, group)
                send(ob.at[part, theirs(u)], pr.at[part, packed(u)], out_sem.at[6], pr_rs.at[u], device(ep, to))

    def pair_sum(u):
        arrived(pr.at[:, packed(u)], pr_rs.at[u])
        zs[:, packed(u)] = ob[:, mine(u)] + pr[:, packed(u)]
        for p in x_peers:
            to = x_target(p)
            send(zs.at[slots_of(to), packed(u)], zr.at[my_slots, mine(u)], out_sem.at[5], cx_rs.at[u], device(to, tp))
        zr[my_slots, mine(u)] = zs[my_slots, packed(u)]

    def combine(u):
        cols, width = (span(u), unit) if u < STRAIGHT else (mine(u), LANES)
        arrived(zr.at[pl.ds(0, len(x_peers) * cap), pl.ds(0, width)], cx_rs.at[u])
        z1, z2, z3 = split3(zr[:, cols])
        pick = row_of[...]
        yb[:, cols] = dot(pick, z3) + dot(pick, z2) + dot(pick, z1)
        for dt in (2, 1, 3):
            to = y_target(dt)
            send(yb.at[rows_at(to, rows), cols], yr.at[dt - 1, :, cols], out_sem.at[7], cy_rs.at[u], device(ep, to))

    def finish(u):
        width = unit if u < STRAIGHT else LANES
        arrived(yr.at[:, :, pl.ds(0, width)], cy_rs.at[u])
        if u < STRAIGHT:
            cols = span(u)
            out_ref[:, cols] = (yb[my_rows, cols] + yr[0, :, cols] + yr[1, :, cols] + yr[2, :, cols]).astype(BF16)
        else:
            out_ref[:, mine(u)] = (yb[my_rows, mine(u)] + yr[1, :, mine(u)]).astype(BF16)
            out_ref[:, theirs(u)] = (yr[0, :, theirs(u)] + yr[2, :, theirs(u)]).astype(BF16)

    for u in (0, 2, 3, 1, 4, 5, 6, 7):
        down(u)
    for step, u in ((pair_sum, 2), (combine, 0), (pair_sum, 3), (pair_sum, 4), (combine, 1), (pair_sum, 5),
                    (combine, 2), (pair_sum, 6), (combine, 3), (pair_sum, 7), (combine, 4), (combine, 5),
                    (combine, 6), (combine, 7)):
        step(u)
    for u in range(units):
        finish(u)

    arrived(idg.at[pl.ds(0, others)], id_sem.at[0])
    arrived(gg.at[pl.ds(0, others)], id_sem.at[2])
    arrived(xg.at[pl.ds(0, others * rows)], out_sem.at[0])
    arrived(gr.at[pl.ds(0, len(x_peers))], out_sem.at[1])
    arrived(xs.at[pl.ds(0, 2 * cap), pl.ds(0, kw)], out_sem.at[2])
    arrived(xs.at[near_rows], out_sem.at[3])
    arrived(xs.at[pl.ds(0, others * 2 * cap), pl.ds(0, kw)], out_sem.at[4])
    paired = units - STRAIGHT
    sent = pl.ds(0, STRAIGHT * unit + paired * LANES)
    arrived(ob.at[pl.ds(0, len(x_peers) * cap), sent], out_sem.at[5])
    arrived(pr, out_sem.at[6])
    arrived(yr.at[:, :, sent], out_sem.at[7])


def solution(mesh):
    ep_n = mesh.shape['ep']
    tp_n = mesh.shape['tp']
    names = tuple(mesh.axis_names)

    def block(tok, ids, gates, w_gate, w_up, w_down):
        rows, d = tok.shape
        local, _, hid = w_gate.shape
        choices = ids.shape[1]
        shard_rows = rows * tp_n
        slots = 2 * shard_rows
        cap = slots // ep_n
        ny = tp_n - 1
        units = d // (2 * LANES)
        any_spec = pl.BlockSpec(memory_space=pl.ANY)
        dma = pltpu.SemaphoreType.DMA
        return pl.pallas_call(
            functools.partial(moe_kernel, names, ep_n, tp_n),
            out_shape=pltpu.VMEM((rows, d), BF16),
            in_specs=[any_spec] * 6,
            out_specs=pl.BlockSpec(memory_space=pltpu.VMEM),
            scratch_shapes=[
                pltpu.VMEM((local, d, hid), BF16),
                pltpu.VMEM((local, d, hid), BF16),
                pltpu.VMEM((local, hid, d), BF16),
                pltpu.VMEM((shard_rows, d), BF16),
                pltpu.VMEM((tp_n, choices, rows), jnp.int32),
                pltpu.VMEM((tp_n, choices, rows), F32),
                pltpu.VMEM((slots, d), BF16),
                pltpu.VMEM((ep_n * local, slots), F32),
                pltpu.VMEM((slots, d), BF16),
                pltpu.VMEM((ep_n, local, LANES), F32),
                pltpu.VMEM((local, slots, hid), F32),
                pltpu.VMEM((local, slots, hid), F32),
                pltpu.VMEM((local, slots, hid), BF16),
                pltpu.VMEM((local, slots, LANES), F32),
                pltpu.VMEM((slots, d), F32),
                pltpu.VMEM((slots, d), F32),
                pltpu.VMEM((shard_rows, d), F32),
                pltpu.VMEM((ny, rows, d), F32),
                pltpu.VMEM((slots, d // 2 - STRAIGHT * LANES), F32),
                pltpu.VMEM((slots, d // 2 - STRAIGHT * LANES), F32),
                pltpu.VMEM((slots, shard_rows), BF16),
                pltpu.VMEM((shard_rows, slots), BF16),
                pltpu.VMEM((LANES, LANES), F32),
                dma((3,)), dma((3,)), dma((4,)), dma((CHUNKS + 1,)), dma((1,)), dma((2,)), dma((CHUNKS,)), dma((ny,)),
                dma((units,)), dma((units,)), dma((units,)), dma((8,)),
            ],
            compiler_params=pltpu.CompilerParams(collective_id=0, has_side_effects=True,
                                                 vmem_limit_bytes=60 * 1024 * 1024),
        )(tok, ids.T, gates.T, w_gate, w_up, w_down)

    return jax.shard_map(
        block,
        mesh=mesh,
        in_specs=(P(TOKEN_AXES, None), P(TOKEN_AXES, None), P(TOKEN_AXES, None),
                  P('ep', None, 'tp'), P('ep', None, 'tp'), P('ep', 'tp', None)),
        out_specs=P(TOKEN_AXES, None),
        check_vma=False,
    )
```

```python
import functools

import jax
import jax.numpy as jnp
from jax import lax
from jax.experimental import pallas as pl
from jax.experimental.pallas import tpu as pltpu
from jax.sharding import PartitionSpec as P

TOKEN_AXES = ('dp', 'ep', 'tp')
LANES = 128
CHUNKS = 4
STRAIGHT = 2
F32 = jnp.float32
BF16 = jnp.bfloat16
MESH = pl.DeviceIdType.MESH


def split3(v):
    hi = v.astype(BF16)
    rest = v - hi.astype(F32)
    mid = rest.astype(BF16)
    low = (rest - mid.astype(F32)).astype(BF16)
    return hi, mid, low


def dot(a, b):
    return lax.dot_general(a, b, (((1,), (0,)), ((), ())), preferred_element_type=F32)


def dot_nt(a, b):
    return lax.dot_general(a, b, (((1,), (1,)), ((), ())), preferred_element_type=F32)


def arrived(ref, sem):
    pltpu.make_async_copy(ref, ref, sem).wait()


def moe_kernel(names, ep_n, tp_n, tok_hbm, ids_hbm, gate_hbm, wg_hbm, wu_hbm, wd_hbm, out_ref,
               wg, wu, wd, xg, idg, gg, xs, gs, xr, gr, acc_g, acc_u, hb, gb, ob, zr, yb, yr, pr, zs,
               slot_of, row_of, gcols,
               w_sem, in_sem, id_sem, ag_rs, dg_rs, df_rs, dx_rs, dq_rs, pr_rs, cx_rs, cy_rs, out_sem):
    rows, d = tok_hbm.shape
    local = wg_hbm.shape[0]
    choices = ids_hbm.shape[0]
    shard_rows = rows * tp_n
    cap = 2 * shard_rows // ep_n
    slots = cap * ep_n
    per_tile = LANES // cap
    kw = d // CHUNKS
    unit = 2 * LANES
    units = d // unit
    chips = ep_n // 2

    ep = lax.axis_index('ep')
    tp = lax.axis_index('tp')

    def device(ep_i, tp_i):
        at = {'dp': lax.axis_index('dp'), 'ep': ep_i, 'tp': tp_i}
        return tuple(at[n] for n in names)

    far = [(chips // 2, 0), (chips // 2, 1)]
    near = [(1, 0), (1, 1), (chips - 1, 0), (chips - 1, 1), (0, 1)]
    x_peers = far + near
    turns = (0, 1, tp_n - 1, 2)

    def x_target(p):
        return lax.rem(ep // 2 + p[0], chips) * 2 + lax.rem(ep + p[1], 2)

    def y_target(dt):
        return lax.rem(tp + dt, tp_n)

    def send(src, dst, ss, rs, dev):
        pltpu.make_async_remote_copy(src_ref=src, dst_ref=dst, send_sem=ss, recv_sem=rs,
                                     device_id=dev, device_id_type=MESH).start()

    def rows_at(i, n):
        return pl.ds(pl.multiple_of(i * n, n), n)

    def slots_of(e):
        return rows_at(e, cap)

    def chunk(t):
        return pl.ds(pl.multiple_of(t * kw, kw), kw)

    def half(t, h):
        return pl.ds(pl.multiple_of(t * kw + h * (kw // 2), kw // 2), kw // 2)

    my_rows = rows_at(tp, rows)
    my_slots = slots_of(ep)
    far_slots = rows_at(lax.rem(ep // 2 + chips // 2, chips), 2 * cap)
    near_rows = pl.ds(0, len(near) * cap)
    others = tp_n - 1

    own = [pltpu.make_async_copy(ids_hbm, idg.at[tp], in_sem.at[0]),
           pltpu.make_async_copy(gate_hbm, gg.at[tp], in_sem.at[1]),
           pltpu.make_async_copy(tok_hbm, xg.at[my_rows], in_sem.at[2])]
    for c in own:
        c.start()

    bar = pltpu.get_barrier_semaphore()
    for dt in range(1, tp_n):
        pl.semaphore_signal(bar, inc=1, device_id=device(ep, y_target(dt)), device_id_type=MESH)
    for p in x_peers:
        pl.semaphore_signal(bar, inc=1, device_id=device(x_target(p), tp), device_id_type=MESH)
    for c in own:
        c.wait()
    pl.semaphore_wait(bar, others + len(x_peers))

    for dt in range(1, tp_n):
        dev = device(ep, y_target(dt))
        send(idg.at[tp], idg.at[tp], id_sem.at[0], id_sem.at[1], dev)
        send(gg.at[tp], gg.at[tp], id_sem.at[2], id_sem.at[3], dev)
    for h in range(2):
        for dt in (2, 1, 3):
            part = xg.at[my_rows, half(y_target(dt), h)]
            send(part, part, out_sem.at[0], ag_rs.at[h], device(ep, y_target(dt)))
    for kc in range(1, CHUNKS):
        for dt in (2, 1, 3):
            part = xg.at[my_rows, chunk(y_target(dt + turns[kc]))]
            send(part, part, out_sem.at[0], ag_rs.at[kc + 1], device(ep, y_target(dt)))
    for i, (src, dst) in enumerate(((wg_hbm, wg), (wu_hbm, wu), (wd_hbm, wd))):
        for e in range(local):
            pltpu.make_async_copy(src.at[e], dst.at[e], w_sem.at[i]).start()
    arrived(idg.at[pl.ds(0, others)], id_sem.at[1])
    arrived(gg.at[pl.ds(0, others)], id_sem.at[3])

    ids = jnp.concatenate([idg[q] for q in range(tp_n)], axis=1)
    gates = jnp.concatenate([gg[q] for q in range(tp_n)], axis=1)
    b_iota = lax.broadcasted_iota(jnp.int32, (ep_n, shard_rows), 0)
    used = jnp.zeros((ep_n, shard_rows), F32)
    for j in range(choices):
        used = jnp.where(ids[j:j + 1, :] // local == b_iota, 1.0, used)
    before = (lax.broadcasted_iota(jnp.int32, (shard_rows, shard_rows), 0)
              < lax.broadcasted_iota(jnp.int32, (shard_rows, shard_rows), 1)).astype(F32).astype(BF16)
    rank = dot(used.astype(BF16), before)
    place = jnp.where(used > 0.0, rank, -1.0)
    in_slot = lax.broadcasted_iota(jnp.int32, (cap, shard_rows), 0).astype(F32)
    for b in range(ep_n):
        hit = jnp.where(place[b:b + 1, :] == in_slot, 1.0, 0.0)
        slot_of[pl.ds(b * cap, cap), :] = hit.astype(BF16)

    e_iota = lax.broadcasted_iota(jnp.int32, (ep_n * local, shard_rows), 0)
    gate_of = jnp.zeros((ep_n * local, shard_rows), F32)
    for j in range(choices):
        gate_of = jnp.where(ids[j:j + 1, :] == e_iota, gates[j:j + 1, :], gate_of)
    g1, g2, g3 = split3(gate_of)
    gs[...] = dot_nt(g3, slot_of[...]) + dot_nt(g2, slot_of[...]) + dot_nt(g1, slot_of[...])

    def gate_tile(b):
        return (rows_at(b, local), rows_at(b // per_tile, LANES))

    for p in x_peers:
        to = x_target(p)
        send(gs.at[gate_tile(to)], gr.at[ep], out_sem.at[1], dg_rs.at[0], device(to, tp))
    gr[ep] = gs[gate_tile(ep)]

    for h in range(2):
        cols = half(tp, h)
        arrived(xg.at[pl.ds(0, others * rows), pl.ds(0, kw // 2)], ag_rs.at[h])
        xs[:, cols] = dot(slot_of[...], xg[:, cols]).astype(BF16)
        for p in far:
            to = x_target(p)
            send(xs.at[slots_of(to), cols], xr.at[my_slots, cols], out_sem.at[2], df_rs.at[h], device(to, tp))
    def pack(kc):
        cols = chunk(y_target(turns[kc]))
        if kc > 0:
            arrived(xg.at[pl.ds(0, others * rows), pl.ds(0, kw)], ag_rs.at[kc + 1])
            xs[:, cols] = dot(slot_of[...], xg[:, cols]).astype(BF16)
        for p in near:
            to = x_target(p)
            send(xs.at[slots_of(to), cols], xr.at[my_slots, cols], out_sem.at[3], dx_rs.at[kc], device(to, tp))
        xr[my_slots, cols] = xs[my_slots, cols]

    def spread(cols, dts):
        for dt in dts:
            part = xr.at[far_slots, cols]
            send(part, part, out_sem.at[4], dq_rs.at[dt - 1], device(ep, y_target(dt)))

    for kc in range(CHUNKS - 1):
        pack(kc)
    for h in range(2):
        arrived(xs.at[pl.ds(0, 2 * cap), pl.ds(0, kw // 2)], df_rs.at[h])
        spread(half(tp, h), (3, 1))
    spread(chunk(tp), (2,))
    pack(CHUNKS - 1)
    row_of[...] = jnp.transpose(slot_of[...].astype(F32)).astype(BF16)

    arrived(gr.at[pl.ds(0, len(x_peers))], dg_rs.at[0])
    lanes_of_mine = rows_at(lax.rem(ep, per_tile), cap)
    for a in range(ep_n):
        gcols[...] = jnp.transpose(jnp.concatenate([gr[a]] * (LANES // local), axis=0))
        cols_a = gcols[lanes_of_mine, :]
        for e in range(local):
            gb[e, pl.ds(a * cap, cap), :] = jnp.broadcast_to(cols_a[:, e:e + 1], (cap, LANES))

    arrived(wg, w_sem.at[0])
    arrived(wu, w_sem.at[1])
    for kcs in ((0,), (1,), (2, 3)):
        for kc in kcs:
            arrived(xr.at[near_rows, pl.ds(0, kw)], dx_rs.at[kc])
            if kc > 0:
                arrived(xr.at[pl.ds(0, 2 * cap), pl.ds(0, kw)], dq_rs.at[tp_n - turns[kc] - 1])

        def up(e, carry, kcs=kcs):
            a = b = None
            for kc in kcs:
                cols = chunk(y_target(turns[kc]))
                x = xr[:, cols]
                a_k = dot(x, wg[e, cols, :])
                b_k = dot(x, wu[e, cols, :])
                a = a_k if a is None else a + a_k
                b = b_k if b is None else b + b_k
            if kcs[0] > 0:
                a = a + acc_g[e]
                b = b + acc_u[e]
            if kcs[-1] < CHUNKS - 1:
                acc_g[e] = a
                acc_u[e] = b
            else:
                h = a * jax.nn.sigmoid(a) * b
                on = jnp.concatenate([gb[e]] * (h.shape[1] // LANES), axis=1) > 0.0
                hb[e] = jnp.where(on, h, 0.0).astype(BF16)
            return carry

        lax.fori_loop(0, local, up, 0, unroll=True)

    arrived(wd, w_sem.at[2])
    parity = lax.rem(tp, 2)
    pairs = (tp + 1 - 2 * parity, y_target(tp_n - 1 + 2 * parity))
    group = slots // 2

    def span(u):
        return pl.ds(u * unit, unit)

    def mine(u):
        return pl.ds(pl.multiple_of(u * unit + parity * LANES, LANES), LANES)

    def theirs(u):
        return pl.ds(pl.multiple_of(u * unit + (1 - parity) * LANES, LANES), LANES)

    def packed(u):
        return pl.ds((u - STRAIGHT) * LANES, LANES)

    def down(u):
        cols = span(u)
        total = None
        for e in range(local):
            o = dot(hb[e], wd[e, :, cols]) * jnp.concatenate([gb[e]] * (unit // LANES), axis=1)
            total = o if total is None else total + o
        ob[:, cols] = total
        if u < STRAIGHT:
            for p in x_peers:
                to = x_target(p)
                send(ob.at[slots_of(to), cols], zr.at[my_slots, cols], out_sem.at[5], cx_rs.at[u], device(to, tp))
            zr[my_slots, cols] = ob[my_slots, cols]
        else:
            for g, to in enumerate(pairs):
                part = pl.ds(g * group, group)
                send(ob.at[part, theirs(u)], pr.at[part, packed(u)], out_sem.at[6], pr_rs.at[u], device(ep, to))

    def pair_sum(u):
        arrived(pr.at[:, packed(u)], pr_rs.at[u])
        zs[:, packed(u)] = ob[:, mine(u)] + pr[:, packed(u)]
        for p in x_peers:
            to = x_target(p)
            send(zs.at[slots_of(to), packed(u)], zr.at[my_slots, mine(u)], out_sem.at[5], cx_rs.at[u], device(to, tp))
        zr[my_slots, mine(u)] = zs[my_slots, packed(u)]

    def combine(u):
        cols, width = (span(u), unit) if u < STRAIGHT else (mine(u), LANES)
        arrived(zr.at[pl.ds(0, len(x_peers) * cap), pl.ds(0, width)], cx_rs.at[u])
        z1, z2, z3 = split3(zr[:, cols])
        pick = row_of[...]
        yb[:, cols] = dot(pick, z3) + dot(pick, z2) + dot(pick, z1)
        for dt in (2, 1, 3):
            to = y_target(dt)
            send(yb.at[rows_at(to, rows), cols], yr.at[dt - 1, :, cols], out_sem.at[7], cy_rs.at[u], device(ep, to))

    def finish(u):
        width = unit if u < STRAIGHT else LANES
        arrived(yr.at[:, :, pl.ds(0, width)], cy_rs.at[u])
        if u < STRAIGHT:
            cols = span(u)
            out_ref[:, cols] = (yb[my_rows, cols] + yr[0, :, cols] + yr[1, :, cols] + yr[2, :, cols]).astype(BF16)
        else:
            out_ref[:, mine(u)] = (yb[my_rows, mine(u)] + yr[1, :, mine(u)]).astype(BF16)
            out_ref[:, theirs(u)] = (yr[0, :, theirs(u)] + yr[2, :, theirs(u)]).astype(BF16)

    for u in (0, 2, 3, 1, 4, 5, 6, 7):
        down(u)
    for step, u in ((pair_sum, 2), (combine, 0), (pair_sum, 3), (pair_sum, 4), (combine, 1), (pair_sum, 5),
                    (combine, 2), (pair_sum, 6), (combine, 3), (pair_sum, 7), (combine, 4), (combine, 5),
                    (combine, 6), (combine, 7)):
        step(u)
    for u in range(units):
        finish(u)

    arrived(idg.at[pl.ds(0, others)], id_sem.at[0])
    arrived(gg.at[pl.ds(0, others)], id_sem.at[2])
    arrived(xg.at[pl.ds(0, others * rows)], out_sem.at[0])
    arrived(gr.at[pl.ds(0, len(x_peers))], out_sem.at[1])
    arrived(xs.at[pl.ds(0, 2 * cap), pl.ds(0, kw)], out_sem.at[2])
    arrived(xs.at[near_rows], out_sem.at[3])
    arrived(xs.at[pl.ds(0, others * 2 * cap), pl.ds(0, kw)], out_sem.at[4])
    paired = units - STRAIGHT
    sent = pl.ds(0, STRAIGHT * unit + paired * LANES)
    arrived(ob.at[pl.ds(0, len(x_peers) * cap), sent], out_sem.at[5])
    arrived(pr, out_sem.at[6])
    arrived(yr.at[:, :, sent], out_sem.at[7])


def solution(mesh):
    ep_n = mesh.shape['ep']
    tp_n = mesh.shape['tp']
    names = tuple(mesh.axis_names)

    def block(tok, ids, gates, w_gate, w_up, w_down):
        rows, d = tok.shape
        local, _, hid = w_gate.shape
        choices = ids.shape[1]
        shard_rows = rows * tp_n
        slots = 2 * shard_rows
        cap = slots // ep_n
        ny = tp_n - 1
        units = d // (2 * LANES)
        any_spec = pl.BlockSpec(memory_space=pl.ANY)
        dma = pltpu.SemaphoreType.DMA
        return pl.pallas_call(
            functools.partial(moe_kernel, names, ep_n, tp_n),
            out_shape=pltpu.VMEM((rows, d), BF16),
            in_specs=[any_spec] * 6,
            out_specs=pl.BlockSpec(memory_space=pltpu.VMEM),
            scratch_shapes=[
                pltpu.VMEM((local, d, hid), BF16),
                pltpu.VMEM((local, d, hid), BF16),
                pltpu.VMEM((local, hid, d), BF16),
                pltpu.VMEM((shard_rows, d), BF16),
                pltpu.VMEM((tp_n, choices, rows), jnp.int32),
                pltpu.VMEM((tp_n, choices, rows), F32),
                pltpu.VMEM((slots, d), BF16),
                pltpu.VMEM((ep_n * local, slots), F32),
                pltpu.VMEM((slots, d), BF16),
                pltpu.VMEM((ep_n, local, LANES), F32),
                pltpu.VMEM((local, slots, hid), F32),
                pltpu.VMEM((local, slots, hid), F32),
                pltpu.VMEM((local, slots, hid), BF16),
                pltpu.VMEM((local, slots, LANES), F32),
                pltpu.VMEM((slots, d), F32),
                pltpu.VMEM((slots, d), F32),
                pltpu.VMEM((shard_rows, d), F32),
                pltpu.VMEM((ny, rows, d), F32),
                pltpu.VMEM((slots, d // 2 - STRAIGHT * LANES), F32),
                pltpu.VMEM((slots, d // 2 - STRAIGHT * LANES), F32),
                pltpu.VMEM((slots, shard_rows), BF16),
                pltpu.VMEM((shard_rows, slots), BF16),
                pltpu.VMEM((LANES, LANES), F32),
                dma((3,)), dma((3,)), dma((4,)), dma((CHUNKS + 1,)), dma((1,)), dma((2,)), dma((CHUNKS,)), dma((ny,)),
                dma((units,)), dma((units,)), dma((units,)), dma((8,)),
            ],
            compiler_params=pltpu.CompilerParams(collective_id=0, has_side_effects=True,
                                                 vmem_limit_bytes=60 * 1024 * 1024),
        )(tok, ids.T, gates.T, w_gate, w_up, w_down)

    return jax.shard_map(
        block,
        mesh=mesh,
        in_specs=(P(TOKEN_AXES, None), P(TOKEN_AXES, None), P(TOKEN_AXES, None),
                  P('ep', None, 'tp'), P('ep', None, 'tp'), P('ep', 'tp', None)),
        out_specs=P(TOKEN_AXES, None),
        check_vma=False,
    )
```

```python
import functools

import jax
import jax.numpy as jnp
from jax import lax
from jax.experimental import pallas as pl
from jax.experimental.pallas import tpu as pltpu
from jax.sharding import PartitionSpec as P

TOKEN_AXES = ('dp', 'ep', 'tp')
LANES = 128
CHUNKS = 4
STRAIGHT = 2
F32 = jnp.float32
BF16 = jnp.bfloat16
MESH = pl.DeviceIdType.MESH


def split3(v):
    hi = v.astype(BF16)
    rest = v - hi.astype(F32)
    mid = rest.astype(BF16)
    low = (rest - mid.astype(F32)).astype(BF16)
    return hi, mid, low


def dot(a, b):
    return lax.dot_general(a, b, (((1,), (0,)), ((), ())), preferred_element_type=F32)


def dot_nt(a, b):
    return lax.dot_general(a, b, (((1,), (1,)), ((), ())), preferred_element_type=F32)


def arrived(ref, sem):
    pltpu.make_async_copy(ref, ref, sem).wait()


def moe_kernel(names, ep_n, tp_n, tok_hbm, ids_hbm, gate_hbm, wg_hbm, wu_hbm, wd_hbm, out_ref,
               wg, wu, wd, xg, idg, gg, xs, gs, xr, gr, acc_g, acc_u, hb, gb, ob, zr, yb, yr, pr, zs,
               slot_of, row_of, gcols,
               w_sem, in_sem, id_sem, ag_rs, dg_rs, df_rs, dx_rs, dq_rs, pr_rs, cx_rs, cy_rs, out_sem):
    rows, d = tok_hbm.shape
    local = wg_hbm.shape[0]
    choices = ids_hbm.shape[0]
    shard_rows = rows * tp_n
    cap = 2 * shard_rows // ep_n
    slots = cap * ep_n
    per_tile = LANES // cap
    kw = d // CHUNKS
    unit = 2 * LANES
    units = d // unit
    chips = ep_n // 2

    ep = lax.axis_index('ep')
    tp = lax.axis_index('tp')

    def device(ep_i, tp_i):
        at = {'dp': lax.axis_index('dp'), 'ep': ep_i, 'tp': tp_i}
        return tuple(at[n] for n in names)

    far = [(chips // 2, 0), (chips // 2, 1)]
    near = [(1, 0), (1, 1), (chips - 1, 0), (chips - 1, 1), (0, 1)]
    x_peers = far + near
    turns = (0, 1, tp_n - 1, 2)

    def x_target(p):
        return lax.rem(ep // 2 + p[0], chips) * 2 + lax.rem(ep + p[1], 2)

    def y_target(dt):
        return lax.rem(tp + dt, tp_n)

    def send(src, dst, ss, rs, dev):
        pltpu.make_async_remote_copy(src_ref=src, dst_ref=dst, send_sem=ss, recv_sem=rs,
                                     device_id=dev, device_id_type=MESH).start()

    def rows_at(i, n):
        return pl.ds(pl.multiple_of(i * n, n), n)

    def slots_of(e):
        return rows_at(e, cap)

    def chunk(t):
        return pl.ds(pl.multiple_of(t * kw, kw), kw)

    def half(t, h):
        return pl.ds(pl.multiple_of(t * kw + h * (kw // 2), kw // 2), kw // 2)

    my_rows = rows_at(tp, rows)
    my_slots = slots_of(ep)
    far_slots = rows_at(lax.rem(ep // 2 + chips // 2, chips), 2 * cap)
    near_rows = pl.ds(0, len(near) * cap)
    others = tp_n - 1

    own = [pltpu.make_async_copy(ids_hbm, idg.at[tp], in_sem.at[0]),
           pltpu.make_async_copy(gate_hbm, gg.at[tp], in_sem.at[1]),
           pltpu.make_async_copy(tok_hbm, xg.at[my_rows], in_sem.at[2])]
    for c in own:
        c.start()

    bar = pltpu.get_barrier_semaphore()
    for dt in range(1, tp_n):
        pl.semaphore_signal(bar, inc=1, device_id=device(ep, y_target(dt)), device_id_type=MESH)
    for p in x_peers:
        pl.semaphore_signal(bar, inc=1, device_id=device(x_target(p), tp), device_id_type=MESH)
    for c in own:
        c.wait()
    pl.semaphore_wait(bar, others + len(x_peers))

    for dt in range(1, tp_n):
        dev = device(ep, y_target(dt))
        send(idg.at[tp], idg.at[tp], id_sem.at[0], id_sem.at[1], dev)
        send(gg.at[tp], gg.at[tp], id_sem.at[2], id_sem.at[3], dev)
    for h in range(2):
        for dt in (2, 1, 3):
            part = xg.at[my_rows, half(y_target(dt), h)]
            send(part, part, out_sem.at[0], ag_rs.at[h], device(ep, y_target(dt)))
    for kc in range(1, CHUNKS):
        for dt in (2, 1, 3):
            part = xg.at[my_rows, chunk(y_target(dt + turns[kc]))]
            send(part, part, out_sem.at[0], ag_rs.at[kc + 1], device(ep, y_target(dt)))
    for i, (src, dst) in enumerate(((wg_hbm, wg), (wu_hbm, wu), (wd_hbm, wd))):
        for e in range(local):
            pltpu.make_async_copy(src.at[e], dst.at[e], w_sem.at[i]).start()
    arrived(idg.at[pl.ds(0, others)], id_sem.at[1])
    arrived(gg.at[pl.ds(0, others)], id_sem.at[3])

    ids = jnp.concatenate([idg[q] for q in range(tp_n)], axis=1)
    gates = jnp.concatenate([gg[q] for q in range(tp_n)], axis=1)
    b_iota = lax.broadcasted_iota(jnp.int32, (ep_n, shard_rows), 0)
    used = jnp.zeros((ep_n, shard_rows), F32)
    for j in range(choices):
        used = jnp.where(ids[j:j + 1, :] // local == b_iota, 1.0, used)
    before = (lax.broadcasted_iota(jnp.int32, (shard_rows, shard_rows), 0)
              < lax.broadcasted_iota(jnp.int32, (shard_rows, shard_rows), 1)).astype(F32).astype(BF16)
    rank = dot(used.astype(BF16), before)
    place = jnp.where(used > 0.0, rank, -1.0)
    in_slot = lax.broadcasted_iota(jnp.int32, (cap, shard_rows), 0).astype(F32)
    for b in range(ep_n):
        hit = jnp.where(place[b:b + 1, :] == in_slot, 1.0, 0.0)
        slot_of[pl.ds(b * cap, cap), :] = hit.astype(BF16)

    e_iota = lax.broadcasted_iota(jnp.int32, (ep_n * local, shard_rows), 0)
    gate_of = jnp.zeros((ep_n * local, shard_rows), F32)
    for j in range(choices):
        gate_of = jnp.where(ids[j:j + 1, :] == e_iota, gates[j:j + 1, :], gate_of)
    g1, g2, g3 = split3(gate_of)
    gs[...] = dot_nt(g3, slot_of[...]) + dot_nt(g2, slot_of[...]) + dot_nt(g1, slot_of[...])

    def gate_tile(b):
        return (rows_at(b, local), rows_at(b // per_tile, LANES))

    for p in x_peers:
        to = x_target(p)
        send(gs.at[gate_tile(to)], gr.at[ep], out_sem.at[1], dg_rs.at[0], device(to, tp))
    gr[ep] = gs[gate_tile(ep)]

    for h in range(2):
        cols = half(tp, h)
        arrived(xg.at[pl.ds(0, others * rows), pl.ds(0, kw // 2)], ag_rs.at[h])
        xs[:, cols] = dot(slot_of[...], xg[:, cols]).astype(BF16)
        for p in far:
            to = x_target(p)
            send(xs.at[slots_of(to), cols], xr.at[my_slots, cols], out_sem.at[2], df_rs.at[h], device(to, tp))
    def pack(kc):
        cols = chunk(y_target(turns[kc]))
        if kc > 0:
            arrived(xg.at[pl.ds(0, others * rows), pl.ds(0, kw)], ag_rs.at[kc + 1])
            xs[:, cols] = dot(slot_of[...], xg[:, cols]).astype(BF16)
        for p in near:
            to = x_target(p)
            send(xs.at[slots_of(to), cols], xr.at[my_slots, cols], out_sem.at[3], dx_rs.at[kc], device(to, tp))
        xr[my_slots, cols] = xs[my_slots, cols]

    def spread(cols, dts):
        for dt in dts:
            part = xr.at[far_slots, cols]
            send(part, part, out_sem.at[4], dq_rs.at[dt - 1], device(ep, y_target(dt)))

    for kc in range(CHUNKS):
        pack(kc)
    for h in range(2):
        arrived(xs.at[pl.ds(0, 2 * cap), pl.ds(0, kw // 2)], df_rs.at[h])
        spread(half(tp, h), (3, 1))
    spread(chunk(tp), (2,))
    row_of[...] = jnp.transpose(slot_of[...].astype(F32)).astype(BF16)

    arrived(gr.at[pl.ds(0, len(x_peers))], dg_rs.at[0])
    lanes_of_mine = rows_at(lax.rem(ep, per_tile), cap)
    for a in range(ep_n):
        gcols[...] = jnp.transpose(jnp.concatenate([gr[a]] * (LANES // local), axis=0))
        cols_a = gcols[lanes_of_mine, :]
        for e in range(local):
            gb[e, pl.ds(a * cap, cap), :] = jnp.broadcast_to(cols_a[:, e:e + 1], (cap, LANES))

    arrived(wg, w_sem.at[0])
    arrived(wu, w_sem.at[1])
    for kcs in ((0,), (1,), (2, 3)):
        for kc in kcs:
            arrived(xr.at[near_rows, pl.ds(0, kw)], dx_rs.at[kc])
            if kc > 0:
                arrived(xr.at[pl.ds(0, 2 * cap), pl.ds(0, kw)], dq_rs.at[tp_n - turns[kc] - 1])

        def up(e, carry, kcs=kcs):
            a = b = None
            for kc in kcs:
                cols = chunk(y_target(turns[kc]))
                x = xr[:, cols]
                a_k = dot(x, wg[e, cols, :])
                b_k = dot(x, wu[e, cols, :])
                a = a_k if a is None else a + a_k
                b = b_k if b is None else b + b_k
            if kcs[0] > 0:
                a = a + acc_g[e]
                b = b + acc_u[e]
            if kcs[-1] < CHUNKS - 1:
                acc_g[e] = a
                acc_u[e] = b
            else:
                h = a * jax.nn.sigmoid(a) * b
                on = jnp.concatenate([gb[e]] * (h.shape[1] // LANES), axis=1) > 0.0
                hb[e] = jnp.where(on, h, 0.0).astype(BF16)
            return carry

        lax.fori_loop(0, local, up, 0, unroll=True)

    arrived(wd, w_sem.at[2])
    parity = lax.rem(tp, 2)
    pairs = (tp + 1 - 2 * parity, y_target(tp_n - 1 + 2 * parity))
    group = slots // 2

    def span(u):
        return pl.ds(u * unit, unit)

    def mine(u):
        return pl.ds(pl.multiple_of(u * unit + parity * LANES, LANES), LANES)

    def theirs(u):
        return pl.ds(pl.multiple_of(u * unit + (1 - parity) * LANES, LANES), LANES)

    def packed(u):
        return pl.ds((u - STRAIGHT) * LANES, LANES)

    def down(u):
        cols = span(u)
        total = None
        for e in range(local):
            o = dot(hb[e], wd[e, :, cols]) * jnp.concatenate([gb[e]] * (unit // LANES), axis=1)
            total = o if total is None else total + o
        ob[:, cols] = total
        if u < STRAIGHT:
            for p in x_peers:
                to = x_target(p)
                send(ob.at[slots_of(to), cols], zr.at[my_slots, cols], out_sem.at[5], cx_rs.at[u], device(to, tp))
            zr[my_slots, cols] = ob[my_slots, cols]
        else:
            for g, to in enumerate(pairs):
                part = pl.ds(g * group, group)
                send(ob.at[part, theirs(u)], pr.at[part, packed(u)], out_sem.at[6], pr_rs.at[u], device(ep, to))

    def pair_sum(u):
        arrived(pr.at[:, packed(u)], pr_rs.at[u])
        zs[:, packed(u)] = ob[:, mine(u)] + pr[:, packed(u)]
        for p in x_peers:
            to = x_target(p)
            send(zs.at[slots_of(to), packed(u)], zr.at[my_slots, mine(u)], out_sem.at[5], cx_rs.at[u], device(to, tp))
        zr[my_slots, mine(u)] = zs[my_slots, packed(u)]

    def combine(u):
        cols, width = (span(u), unit) if u < STRAIGHT else (mine(u), LANES)
        arrived(zr.at[pl.ds(0, len(x_peers) * cap), pl.ds(0, width)], cx_rs.at[u])
        z1, z2, z3 = split3(zr[:, cols])
        pick = row_of[...]
        yb[:, cols] = dot(pick, z3) + dot(pick, z2) + dot(pick, z1)
        for dt in (2, 1, 3):
            to = y_target(dt)
            send(yb.at[rows_at(to, rows), cols], yr.at[dt - 1, :, cols], out_sem.at[7], cy_rs.at[u], device(ep, to))

    def finish(u):
        width = unit if u < STRAIGHT else LANES
        arrived(yr.at[:, :, pl.ds(0, width)], cy_rs.at[u])
        if u < STRAIGHT:
            cols = span(u)
            out_ref[:, cols] = (yb[my_rows, cols] + yr[0, :, cols] + yr[1, :, cols] + yr[2, :, cols]).astype(BF16)
        else:
            out_ref[:, mine(u)] = (yb[my_rows, mine(u)] + yr[1, :, mine(u)]).astype(BF16)
            out_ref[:, theirs(u)] = (yr[0, :, theirs(u)] + yr[2, :, theirs(u)]).astype(BF16)

    for u in (0, 2, 3, 1, 4, 5, 6, 7):
        down(u)
    for step, u in ((pair_sum, 2), (combine, 0), (pair_sum, 3), (pair_sum, 4), (combine, 1), (pair_sum, 5),
                    (combine, 2), (pair_sum, 6), (combine, 3), (pair_sum, 7), (combine, 4), (combine, 5),
                    (combine, 6), (combine, 7)):
        step(u)
    for u in range(units):
        finish(u)

    arrived(idg.at[pl.ds(0, others)], id_sem.at[0])
    arrived(gg.at[pl.ds(0, others)], id_sem.at[2])
    arrived(xg.at[pl.ds(0, others * rows)], out_sem.at[0])
    arrived(gr.at[pl.ds(0, len(x_peers))], out_sem.at[1])
    arrived(xs.at[pl.ds(0, 2 * cap), pl.ds(0, kw)], out_sem.at[2])
    arrived(xs.at[near_rows], out_sem.at[3])
    arrived(xs.at[pl.ds(0, others * 2 * cap), pl.ds(0, kw)], out_sem.at[4])
    paired = units - STRAIGHT
    sent = pl.ds(0, STRAIGHT * unit + paired * LANES)
    arrived(ob.at[pl.ds(0, len(x_peers) * cap), sent], out_sem.at[5])
    arrived(pr, out_sem.at[6])
    arrived(yr.at[:, :, sent], out_sem.at[7])


def solution(mesh):
    ep_n = mesh.shape['ep']
    tp_n = mesh.shape['tp']
    names = tuple(mesh.axis_names)

    def block(tok, ids, gates, w_gate, w_up, w_down):
        rows, d = tok.shape
        local, _, hid = w_gate.shape
        choices = ids.shape[1]
        shard_rows = rows * tp_n
        slots = 2 * shard_rows
        cap = slots // ep_n
        ny = tp_n - 1
        units = d // (2 * LANES)
        any_spec = pl.BlockSpec(memory_space=pl.ANY)
        dma = pltpu.SemaphoreType.DMA
        return pl.pallas_call(
            functools.partial(moe_kernel, names, ep_n, tp_n),
            out_shape=pltpu.VMEM((rows, d), BF16),
            in_specs=[any_spec] * 6,
            out_specs=pl.BlockSpec(memory_space=pltpu.VMEM),
            scratch_shapes=[
                pltpu.VMEM((local, d, hid), BF16),
                pltpu.VMEM((local, d, hid), BF16),
                pltpu.VMEM((local, hid, d), BF16),
                pltpu.VMEM((shard_rows, d), BF16),
                pltpu.VMEM((tp_n, choices, rows), jnp.int32),
                pltpu.VMEM((tp_n, choices, rows), F32),
                pltpu.VMEM((slots, d), BF16),
                pltpu.VMEM((ep_n * local, slots), F32),
                pltpu.VMEM((slots, d), BF16),
                pltpu.VMEM((ep_n, local, LANES), F32),
                pltpu.VMEM((local, slots, hid), F32),
                pltpu.VMEM((local, slots, hid), F32),
                pltpu.VMEM((local, slots, hid), BF16),
                pltpu.VMEM((local, slots, LANES), F32),
                pltpu.VMEM((slots, d), F32),
                pltpu.VMEM((slots, d), F32),
                pltpu.VMEM((shard_rows, d), F32),
                pltpu.VMEM((ny, rows, d), F32),
                pltpu.VMEM((slots, d // 2 - STRAIGHT * LANES), F32),
                pltpu.VMEM((slots, d // 2 - STRAIGHT * LANES), F32),
                pltpu.VMEM((slots, shard_rows), BF16),
                pltpu.VMEM((shard_rows, slots), BF16),
                pltpu.VMEM((LANES, LANES), F32),
                dma((3,)), dma((3,)), dma((4,)), dma((CHUNKS + 1,)), dma((1,)), dma((2,)), dma((CHUNKS,)), dma((ny,)),
                dma((units,)), dma((units,)), dma((units,)), dma((8,)),
            ],
            compiler_params=pltpu.CompilerParams(collective_id=0, has_side_effects=True,
                                                 vmem_limit_bytes=60 * 1024 * 1024),
        )(tok, ids.T, gates.T, w_gate, w_up, w_down)

    return jax.shard_map(
        block,
        mesh=mesh,
        in_specs=(P(TOKEN_AXES, None), P(TOKEN_AXES, None), P(TOKEN_AXES, None),
                  P('ep', None, 'tp'), P('ep', None, 'tp'), P('ep', 'tp', None)),
        out_specs=P(TOKEN_AXES, None),
        check_vma=False,
    )
```

```python
import functools

import jax
import jax.numpy as jnp
from jax import lax
from jax.experimental import pallas as pl
from jax.experimental.pallas import tpu as pltpu
from jax.sharding import PartitionSpec as P

TOKEN_AXES = ('dp', 'ep', 'tp')
LANES = 128
CHUNKS = 4
STRAIGHT = 2
F32 = jnp.float32
BF16 = jnp.bfloat16
MESH = pl.DeviceIdType.MESH


def split3(v):
    hi = v.astype(BF16)
    rest = v - hi.astype(F32)
    mid = rest.astype(BF16)
    low = (rest - mid.astype(F32)).astype(BF16)
    return hi, mid, low


def dot(a, b):
    return lax.dot_general(a, b, (((1,), (0,)), ((), ())), preferred_element_type=F32)


def dot_nt(a, b):
    return lax.dot_general(a, b, (((1,), (1,)), ((), ())), preferred_element_type=F32)


def arrived(ref, sem):
    pltpu.make_async_copy(ref, ref, sem).wait()


def moe_kernel(names, ep_n, tp_n, tok_hbm, ids_hbm, gate_hbm, wg_hbm, wu_hbm, wd_hbm, out_ref,
               wg, wu, wd, xg, idg, gg, xs, gs, xr, gr, acc_g, acc_u, hb, gb, ob, zr, yb, yr, pr, zs,
               slot_of, row_of, gcols,
               w_sem, in_sem, id_sem, ag_rs, dg_rs, df_rs, dx_rs, dq_rs, pr_rs, cx_rs, cy_rs, out_sem):
    rows, d = tok_hbm.shape
    local = wg_hbm.shape[0]
    choices = ids_hbm.shape[0]
    shard_rows = rows * tp_n
    cap = 2 * shard_rows // ep_n
    slots = cap * ep_n
    per_tile = LANES // cap
    kw = d // CHUNKS
    unit = 2 * LANES
    units = d // unit
    chips = ep_n // 2

    ep = lax.axis_index('ep')
    tp = lax.axis_index('tp')

    def device(ep_i, tp_i):
        at = {'dp': lax.axis_index('dp'), 'ep': ep_i, 'tp': tp_i}
        return tuple(at[n] for n in names)

    far = [(chips // 2, 0), (chips // 2, 1)]
    near = [(1, 0), (1, 1), (chips - 1, 0), (chips - 1, 1), (0, 1)]
    x_peers = far + near
    parity = lax.rem(tp, 2)
    sign = 1 - 2 * parity

    def turn(k, s):
        return (0, s, -s, 2)[k]

    peers = ((sign, -sign), (-sign, -sign), (2, sign))

    def x_target(p):
        return lax.rem(ep // 2 + p[0], chips) * 2 + lax.rem(ep + p[1], 2)

    def y_target(dt):
        return lax.rem(tp + dt + tp_n, tp_n)

    def send(src, dst, ss, rs, dev):
        pltpu.make_async_remote_copy(src_ref=src, dst_ref=dst, send_sem=ss, recv_sem=rs,
                                     device_id=dev, device_id_type=MESH).start()

    def rows_at(i, n):
        return pl.ds(pl.multiple_of(i * n, n), n)

    def slots_of(e):
        return rows_at(e, cap)

    def chunk(t):
        return pl.ds(pl.multiple_of(t * kw, kw), kw)

    def half(t, h):
        return pl.ds(pl.multiple_of(t * kw + h * (kw // 2), kw // 2), kw // 2)

    my_rows = rows_at(tp, rows)
    my_slots = slots_of(ep)
    far_slots = rows_at(lax.rem(ep // 2 + chips // 2, chips), 2 * cap)
    near_rows = pl.ds(0, len(near) * cap)
    others = tp_n - 1

    own = [pltpu.make_async_copy(ids_hbm, idg.at[tp], in_sem.at[0]),
           pltpu.make_async_copy(gate_hbm, gg.at[tp], in_sem.at[1]),
           pltpu.make_async_copy(tok_hbm, xg.at[my_rows], in_sem.at[2])]
    for c in own:
        c.start()

    bar = pltpu.get_barrier_semaphore()
    for dt in range(1, tp_n):
        pl.semaphore_signal(bar, inc=1, device_id=device(ep, y_target(dt)), device_id_type=MESH)
    for p in x_peers:
        pl.semaphore_signal(bar, inc=1, device_id=device(x_target(p), tp), device_id_type=MESH)
    for c in own:
        c.wait()
    pl.semaphore_wait(bar, others + len(x_peers))

    for dt in range(1, tp_n):
        dev = device(ep, y_target(dt))
        send(idg.at[tp], idg.at[tp], id_sem.at[0], id_sem.at[1], dev)
        send(gg.at[tp], gg.at[tp], id_sem.at[2], id_sem.at[3], dev)
    for h in range(2):
        for dt, _ in peers:
            part = xg.at[my_rows, half(y_target(dt), h)]
            send(part, part, out_sem.at[0], ag_rs.at[h], device(ep, y_target(dt)))
    for kc in range(1, CHUNKS):
        for dt, s in peers:
            part = xg.at[my_rows, chunk(y_target(dt + turn(kc, s)))]
            send(part, part, out_sem.at[0], ag_rs.at[kc + 1], device(ep, y_target(dt)))
    for i, (src, dst) in enumerate(((wg_hbm, wg), (wu_hbm, wu), (wd_hbm, wd))):
        for e in range(local):
            pltpu.make_async_copy(src.at[e], dst.at[e], w_sem.at[i]).start()
    arrived(idg.at[pl.ds(0, others)], id_sem.at[1])
    arrived(gg.at[pl.ds(0, others)], id_sem.at[3])

    ids = jnp.concatenate([idg[q] for q in range(tp_n)], axis=1)
    gates = jnp.concatenate([gg[q] for q in range(tp_n)], axis=1)
    b_iota = lax.broadcasted_iota(jnp.int32, (ep_n, shard_rows), 0)
    used = jnp.zeros((ep_n, shard_rows), F32)
    for j in range(choices):
        used = jnp.where(ids[j:j + 1, :] // local == b_iota, 1.0, used)
    before = (lax.broadcasted_iota(jnp.int32, (shard_rows, shard_rows), 0)
              < lax.broadcasted_iota(jnp.int32, (shard_rows, shard_rows), 1)).astype(F32).astype(BF16)
    rank = dot(used.astype(BF16), before)
    place = jnp.where(used > 0.0, rank, -1.0)
    in_slot = lax.broadcasted_iota(jnp.int32, (cap, shard_rows), 0).astype(F32)
    for b in range(ep_n):
        hit = jnp.where(place[b:b + 1, :] == in_slot, 1.0, 0.0)
        slot_of[pl.ds(b * cap, cap), :] = hit.astype(BF16)

    e_iota = lax.broadcasted_iota(jnp.int32, (ep_n * local, shard_rows), 0)
    gate_of = jnp.zeros((ep_n * local, shard_rows), F32)
    for j in range(choices):
        gate_of = jnp.where(ids[j:j + 1, :] == e_iota, gates[j:j + 1, :], gate_of)
    g1, g2, g3 = split3(gate_of)
    gs[...] = dot_nt(g3, slot_of[...]) + dot_nt(g2, slot_of[...]) + dot_nt(g1, slot_of[...])

    def gate_tile(b):
        return (rows_at(b, local), rows_at(b // per_tile, LANES))

    for p in x_peers:
        to = x_target(p)
        send(gs.at[gate_tile(to)], gr.at[ep], out_sem.at[1], dg_rs.at[0], device(to, tp))
    gr[ep] = gs[gate_tile(ep)]

    for h in range(2):
        cols = half(tp, h)
        arrived(xg.at[pl.ds(0, others * rows), pl.ds(0, kw // 2)], ag_rs.at[h])
        xs[:, cols] = dot(slot_of[...], xg[:, cols]).astype(BF16)
        for p in far:
            to = x_target(p)
            send(xs.at[slots_of(to), cols], xr.at[my_slots, cols], out_sem.at[2], df_rs.at[h], device(to, tp))
    def pack(kc):
        cols = chunk(y_target(turn(kc, sign)))
        if kc > 0:
            arrived(xg.at[pl.ds(0, others * rows), pl.ds(0, kw)], ag_rs.at[kc + 1])
            xs[:, cols] = dot(slot_of[...], xg[:, cols]).astype(BF16)
        for p in near:
            to = x_target(p)
            send(xs.at[slots_of(to), cols], xr.at[my_slots, cols], out_sem.at[3], dx_rs.at[kc], device(to, tp))
        xr[my_slots, cols] = xs[my_slots, cols]

    def spread(cols, ks):
        for k in ks:
            part = xr.at[far_slots, cols]
            send(part, part, out_sem.at[4], dq_rs.at[k - 1], device(ep, y_target(turn(k, sign))))

    for kc in range(CHUNKS):
        pack(kc)
    for h in range(2):
        arrived(xs.at[pl.ds(0, 2 * cap), pl.ds(0, kw // 2)], df_rs.at[h])
        spread(half(tp, h), (1, 2))
    spread(chunk(tp), (3,))
    row_of[...] = jnp.transpose(slot_of[...].astype(F32)).astype(BF16)

    arrived(gr.at[pl.ds(0, len(x_peers))], dg_rs.at[0])
    lanes_of_mine = rows_at(lax.rem(ep, per_tile), cap)
    for a in range(ep_n):
        gcols[...] = jnp.transpose(jnp.concatenate([gr[a]] * (LANES // local), axis=0))
        cols_a = gcols[lanes_of_mine, :]
        for e in range(local):
            gb[e, pl.ds(a * cap, cap), :] = jnp.broadcast_to(cols_a[:, e:e + 1], (cap, LANES))

    arrived(wg, w_sem.at[0])
    arrived(wu, w_sem.at[1])
    for kcs in ((0,), (1,), (2, 3)):
        for kc in kcs:
            arrived(xr.at[near_rows, pl.ds(0, kw)], dx_rs.at[kc])
            if kc > 0:
                arrived(xr.at[pl.ds(0, 2 * cap), pl.ds(0, kw)], dq_rs.at[kc - 1])

        def up(e, carry, kcs=kcs):
            a = b = None
            for kc in kcs:
                cols = chunk(y_target(turn(kc, sign)))
                x = xr[:, cols]
                a_k = dot(x, wg[e, cols, :])
                b_k = dot(x, wu[e, cols, :])
                a = a_k if a is None else a + a_k
                b = b_k if b is None else b + b_k
            if kcs[0] > 0:
                a = a + acc_g[e]
                b = b + acc_u[e]
            if kcs[-1] < CHUNKS - 1:
                acc_g[e] = a
                acc_u[e] = b
            else:
                h = a * jax.nn.sigmoid(a) * b
                on = jnp.concatenate([gb[e]] * (h.shape[1] // LANES), axis=1) > 0.0
                hb[e] = jnp.where(on, h, 0.0).astype(BF16)
            return carry

        lax.fori_loop(0, local, up, 0, unroll=True)

    arrived(wd, w_sem.at[2])
    pairs = (tp + 1 - 2 * parity, y_target(tp_n - 1 + 2 * parity))
    group = slots // 2

    def span(u):
        return pl.ds(u * unit, unit)

    def mine(u):
        return pl.ds(pl.multiple_of(u * unit + parity * LANES, LANES), LANES)

    def theirs(u):
        return pl.ds(pl.multiple_of(u * unit + (1 - parity) * LANES, LANES), LANES)

    def packed(u):
        return pl.ds((u - STRAIGHT) * LANES, LANES)

    def down(u):
        cols = span(u)
        total = None
        for e in range(local):
            o = dot(hb[e], wd[e, :, cols]) * jnp.concatenate([gb[e]] * (unit // LANES), axis=1)
            total = o if total is None else total + o
        ob[:, cols] = total
        if u < STRAIGHT:
            for p in x_peers:
                to = x_target(p)
                send(ob.at[slots_of(to), cols], zr.at[my_slots, cols], out_sem.at[5], cx_rs.at[u], device(to, tp))
            zr[my_slots, cols] = ob[my_slots, cols]
        else:
            for g, to in enumerate(pairs):
                part = pl.ds(g * group, group)
                send(ob.at[part, theirs(u)], pr.at[part, packed(u)], out_sem.at[6], pr_rs.at[u], device(ep, to))

    def pair_sum(u):
        arrived(pr.at[:, packed(u)], pr_rs.at[u])
        zs[:, packed(u)] = ob[:, mine(u)] + pr[:, packed(u)]
        for p in x_peers:
            to = x_target(p)
            send(zs.at[slots_of(to), packed(u)], zr.at[my_slots, mine(u)], out_sem.at[5], cx_rs.at[u], device(to, tp))
        zr[my_slots, mine(u)] = zs[my_slots, packed(u)]

    def combine(u):
        cols, width = (span(u), unit) if u < STRAIGHT else (mine(u), LANES)
        arrived(zr.at[pl.ds(0, len(x_peers) * cap), pl.ds(0, width)], cx_rs.at[u])
        z1, z2, z3 = split3(zr[:, cols])
        pick = row_of[...]
        yb[:, cols] = dot(pick, z3) + dot(pick, z2) + dot(pick, z1)
        for dt in (2, 1, 3):
            to = y_target(dt)
            send(yb.at[rows_at(to, rows), cols], yr.at[dt - 1, :, cols], out_sem.at[7], cy_rs.at[u], device(ep, to))

    def finish(u):
        width = unit if u < STRAIGHT else LANES
        arrived(yr.at[:, :, pl.ds(0, width)], cy_rs.at[u])
        if u < STRAIGHT:
            cols = span(u)
            out_ref[:, cols] = (yb[my_rows, cols] + yr[0, :, cols] + yr[1, :, cols] + yr[2, :, cols]).astype(BF16)
        else:
            out_ref[:, mine(u)] = (yb[my_rows, mine(u)] + yr[1, :, mine(u)]).astype(BF16)
            out_ref[:, theirs(u)] = (yr[0, :, theirs(u)] + yr[2, :, theirs(u)]).astype(BF16)

    for u in (0, 2, 3, 1, 4, 5, 6, 7):
        down(u)
    for step, u in ((pair_sum, 2), (combine, 0), (pair_sum, 3), (pair_sum, 4), (combine, 1), (pair_sum, 5),
                    (combine, 2), (pair_sum, 6), (combine, 3), (pair_sum, 7), (combine, 4), (combine, 5),
                    (combine, 6), (combine, 7)):
        step(u)
    for u in range(units):
        finish(u)

    arrived(idg.at[pl.ds(0, others)], id_sem.at[0])
    arrived(gg.at[pl.ds(0, others)], id_sem.at[2])
    arrived(xg.at[pl.ds(0, others * rows)], out_sem.at[0])
    arrived(gr.at[pl.ds(0, len(x_peers))], out_sem.at[1])
    arrived(xs.at[pl.ds(0, 2 * cap), pl.ds(0, kw)], out_sem.at[2])
    arrived(xs.at[near_rows], out_sem.at[3])
    arrived(xs.at[pl.ds(0, others * 2 * cap), pl.ds(0, kw)], out_sem.at[4])
    paired = units - STRAIGHT
    sent = pl.ds(0, STRAIGHT * unit + paired * LANES)
    arrived(ob.at[pl.ds(0, len(x_peers) * cap), sent], out_sem.at[5])
    arrived(pr, out_sem.at[6])
    arrived(yr.at[:, :, sent], out_sem.at[7])


def solution(mesh):
    ep_n = mesh.shape['ep']
    tp_n = mesh.shape['tp']
    names = tuple(mesh.axis_names)

    def block(tok, ids, gates, w_gate, w_up, w_down):
        rows, d = tok.shape
        local, _, hid = w_gate.shape
        choices = ids.shape[1]
        shard_rows = rows * tp_n
        slots = 2 * shard_rows
        cap = slots // ep_n
        ny = tp_n - 1
        units = d // (2 * LANES)
        any_spec = pl.BlockSpec(memory_space=pl.ANY)
        dma = pltpu.SemaphoreType.DMA
        return pl.pallas_call(
            functools.partial(moe_kernel, names, ep_n, tp_n),
            out_shape=pltpu.VMEM((rows, d), BF16),
            in_specs=[any_spec] * 6,
            out_specs=pl.BlockSpec(memory_space=pltpu.VMEM),
            scratch_shapes=[
                pltpu.VMEM((local, d, hid), BF16),
                pltpu.VMEM((local, d, hid), BF16),
                pltpu.VMEM((local, hid, d), BF16),
                pltpu.VMEM((shard_rows, d), BF16),
                pltpu.VMEM((tp_n, choices, rows), jnp.int32),
                pltpu.VMEM((tp_n, choices, rows), F32),
                pltpu.VMEM((slots, d), BF16),
                pltpu.VMEM((ep_n * local, slots), F32),
                pltpu.VMEM((slots, d), BF16),
                pltpu.VMEM((ep_n, local, LANES), F32),
                pltpu.VMEM((local, slots, hid), F32),
                pltpu.VMEM((local, slots, hid), F32),
                pltpu.VMEM((local, slots, hid), BF16),
                pltpu.VMEM((local, slots, LANES), F32),
                pltpu.VMEM((slots, d), F32),
                pltpu.VMEM((slots, d), F32),
                pltpu.VMEM((shard_rows, d), F32),
                pltpu.VMEM((ny, rows, d), F32),
                pltpu.VMEM((slots, d // 2 - STRAIGHT * LANES), F32),
                pltpu.VMEM((slots, d // 2 - STRAIGHT * LANES), F32),
                pltpu.VMEM((slots, shard_rows), BF16),
                pltpu.VMEM((shard_rows, slots), BF16),
                pltpu.VMEM((LANES, LANES), F32),
                dma((3,)), dma((3,)), dma((4,)), dma((CHUNKS + 1,)), dma((1,)), dma((2,)), dma((CHUNKS,)), dma((ny,)),
                dma((units,)), dma((units,)), dma((units,)), dma((8,)),
            ],
            compiler_params=pltpu.CompilerParams(collective_id=0, has_side_effects=True,
                                                 vmem_limit_bytes=60 * 1024 * 1024),
        )(tok, ids.T, gates.T, w_gate, w_up, w_down)

    return jax.shard_map(
        block,
        mesh=mesh,
        in_specs=(P(TOKEN_AXES, None), P(TOKEN_AXES, None), P(TOKEN_AXES, None),
                  P('ep', None, 'tp'), P('ep', None, 'tp'), P('ep', 'tp', None)),
        out_specs=P(TOKEN_AXES, None),
        check_vma=False,
    )
```

```python
import functools

import jax
import jax.numpy as jnp
from jax import lax
from jax.experimental import pallas as pl
from jax.experimental.pallas import tpu as pltpu
from jax.sharding import PartitionSpec as P

TOKEN_AXES = ('dp', 'ep', 'tp')
LANES = 128
CHUNKS = 4
STRAIGHT = 2
F32 = jnp.float32
BF16 = jnp.bfloat16
MESH = pl.DeviceIdType.MESH


def split3(v):
    hi = v.astype(BF16)
    rest = v - hi.astype(F32)
    mid = rest.astype(BF16)
    low = (rest - mid.astype(F32)).astype(BF16)
    return hi, mid, low


def dot(a, b):
    return lax.dot_general(a, b, (((1,), (0,)), ((), ())), preferred_element_type=F32)


def dot_nt(a, b):
    return lax.dot_general(a, b, (((1,), (1,)), ((), ())), preferred_element_type=F32)


def arrived(ref, sem):
    pltpu.make_async_copy(ref, ref, sem).wait()


def moe_kernel(names, ep_n, tp_n, tok_hbm, ids_hbm, gate_hbm, wg_hbm, wu_hbm, wd_hbm, out_ref,
               wg, wu, wd, xg, idg, gg, xs, gs, xr, gr, acc_g, acc_u, hb, gb, ob, zr, yb, yr, pr, zs,
               slot_of, row_of, gcols,
               w_sem, in_sem, id_sem, ag_rs, dg_rs, df_rs, dx_rs, dq_rs, pr_rs, cx_rs, cy_rs, out_sem):
    rows, d = tok_hbm.shape
    local = wg_hbm.shape[0]
    choices = ids_hbm.shape[0]
    shard_rows = rows * tp_n
    cap = 2 * shard_rows // ep_n
    slots = cap * ep_n
    per_tile = LANES // cap
    kw = d // CHUNKS
    unit = 2 * LANES
    units = d // unit
    chips = ep_n // 2

    ep = lax.axis_index('ep')
    tp = lax.axis_index('tp')

    def device(ep_i, tp_i):
        at = {'dp': lax.axis_index('dp'), 'ep': ep_i, 'tp': tp_i}
        return tuple(at[n] for n in names)

    far = [(chips // 2, 0), (chips // 2, 1)]
    near = [(1, 0), (1, 1), (chips - 1, 0), (chips - 1, 1), (0, 1)]
    x_peers = far + near
    parity = lax.rem(tp, 2)
    sign = 1 - 2 * parity

    def turn(k, s):
        return (0, s, -s, 2)[k]

    peers = ((sign, -sign), (-sign, -sign), (2, sign))

    def x_target(p):
        return lax.rem(ep // 2 + p[0], chips) * 2 + lax.rem(ep + p[1], 2)

    def y_target(dt):
        return lax.rem(tp + dt + tp_n, tp_n)

    def send(src, dst, ss, rs, dev):
        pltpu.make_async_remote_copy(src_ref=src, dst_ref=dst, send_sem=ss, recv_sem=rs,
                                     device_id=dev, device_id_type=MESH).start()

    def rows_at(i, n):
        return pl.ds(pl.multiple_of(i * n, n), n)

    def slots_of(e):
        return rows_at(e, cap)

    def chunk(t):
        return pl.ds(pl.multiple_of(t * kw, kw), kw)

    def half(t, h):
        return pl.ds(pl.multiple_of(t * kw + h * (kw // 2), kw // 2), kw // 2)

    my_rows = rows_at(tp, rows)
    my_slots = slots_of(ep)
    far_slots = rows_at(lax.rem(ep // 2 + chips // 2, chips), 2 * cap)
    near_rows = pl.ds(0, len(near) * cap)
    others = tp_n - 1

    own = [pltpu.make_async_copy(ids_hbm, idg.at[tp], in_sem.at[0]),
           pltpu.make_async_copy(gate_hbm, gg.at[tp], in_sem.at[1]),
           pltpu.make_async_copy(tok_hbm, xg.at[my_rows], in_sem.at[2])]
    for c in own:
        c.start()

    bar = pltpu.get_barrier_semaphore()
    for dt in range(1, tp_n):
        pl.semaphore_signal(bar, inc=1, device_id=device(ep, y_target(dt)), device_id_type=MESH)
    for p in x_peers:
        pl.semaphore_signal(bar, inc=1, device_id=device(x_target(p), tp), device_id_type=MESH)
    for c in own:
        c.wait()
    pl.semaphore_wait(bar, others + len(x_peers))

    for dt in range(1, tp_n):
        dev = device(ep, y_target(dt))
        send(idg.at[tp], idg.at[tp], id_sem.at[0], id_sem.at[1], dev)
        send(gg.at[tp], gg.at[tp], id_sem.at[2], id_sem.at[3], dev)
    for h in range(2):
        for dt, _ in peers:
            part = xg.at[my_rows, half(y_target(dt), h)]
            send(part, part, out_sem.at[0], ag_rs.at[h], device(ep, y_target(dt)))
    for kc in range(1, CHUNKS):
        for dt, s in peers:
            part = xg.at[my_rows, chunk(y_target(dt + turn(kc, s)))]
            send(part, part, out_sem.at[0], ag_rs.at[kc + 1], device(ep, y_target(dt)))
    for i, (src, dst) in enumerate(((wg_hbm, wg), (wu_hbm, wu), (wd_hbm, wd))):
        for e in range(local):
            pltpu.make_async_copy(src.at[e], dst.at[e], w_sem.at[i]).start()
    arrived(idg.at[pl.ds(0, others)], id_sem.at[1])
    arrived(gg.at[pl.ds(0, others)], id_sem.at[3])

    ids = jnp.concatenate([idg[q] for q in range(tp_n)], axis=1)
    gates = jnp.concatenate([gg[q] for q in range(tp_n)], axis=1)
    b_iota = lax.broadcasted_iota(jnp.int32, (ep_n, shard_rows), 0)
    used = jnp.zeros((ep_n, shard_rows), F32)
    for j in range(choices):
        used = jnp.where(ids[j:j + 1, :] // local == b_iota, 1.0, used)
    before = (lax.broadcasted_iota(jnp.int32, (shard_rows, shard_rows), 0)
              < lax.broadcasted_iota(jnp.int32, (shard_rows, shard_rows), 1)).astype(F32).astype(BF16)
    rank = dot(used.astype(BF16), before)
    place = jnp.where(used > 0.0, rank, -1.0)
    in_slot = lax.broadcasted_iota(jnp.int32, (cap, shard_rows), 0).astype(F32)
    for b in range(ep_n):
        hit = jnp.where(place[b:b + 1, :] == in_slot, 1.0, 0.0)
        slot_of[pl.ds(b * cap, cap), :] = hit.astype(BF16)

    e_iota = lax.broadcasted_iota(jnp.int32, (ep_n * local, shard_rows), 0)
    gate_of = jnp.zeros((ep_n * local, shard_rows), F32)
    for j in range(choices):
        gate_of = jnp.where(ids[j:j + 1, :] == e_iota, gates[j:j + 1, :], gate_of)
    g1, g2, g3 = split3(gate_of)
    gs[...] = dot_nt(g3, slot_of[...]) + dot_nt(g2, slot_of[...]) + dot_nt(g1, slot_of[...])

    def gate_tile(b):
        return (rows_at(b, local), rows_at(b // per_tile, LANES))

    for p in x_peers:
        to = x_target(p)
        send(gs.at[gate_tile(to)], gr.at[ep], out_sem.at[1], dg_rs.at[0], device(to, tp))
    gr[ep] = gs[gate_tile(ep)]

    for h in range(2):
        cols = half(tp, h)
        arrived(xg.at[pl.ds(0, others * rows), pl.ds(0, kw // 2)], ag_rs.at[h])
        xs[:, cols] = dot(slot_of[...], xg[:, cols]).astype(BF16)
        for p in far:
            to = x_target(p)
            send(xs.at[slots_of(to), cols], xr.at[my_slots, cols], out_sem.at[2], df_rs.at[h], device(to, tp))
    def pack(kc):
        cols = chunk(y_target(turn(kc, sign)))
        if kc > 0:
            arrived(xg.at[pl.ds(0, others * rows), pl.ds(0, kw)], ag_rs.at[kc + 1])
            xs[:, cols] = dot(slot_of[...], xg[:, cols]).astype(BF16)
        for p in near:
            to = x_target(p)
            send(xs.at[slots_of(to), cols], xr.at[my_slots, cols], out_sem.at[3], dx_rs.at[kc], device(to, tp))
        xr[my_slots, cols] = xs[my_slots, cols]

    def spread(cols, ks):
        for k in ks:
            part = xr.at[far_slots, cols]
            send(part, part, out_sem.at[4], dq_rs.at[k - 1], device(ep, y_target(turn(k, sign))))

    for kc in range(CHUNKS):
        pack(kc)
    for h in range(2):
        arrived(xs.at[pl.ds(0, 2 * cap), pl.ds(0, kw // 2)], df_rs.at[h])
        spread(half(tp, h), (1, 2))
    spread(chunk(tp), (3,))
    row_of[...] = jnp.transpose(slot_of[...].astype(F32)).astype(BF16)

    arrived(gr.at[pl.ds(0, len(x_peers))], dg_rs.at[0])
    lanes_of_mine = rows_at(lax.rem(ep, per_tile), cap)
    for a in range(ep_n):
        gcols[...] = jnp.transpose(jnp.concatenate([gr[a]] * (LANES // local), axis=0))
        cols_a = gcols[lanes_of_mine, :]
        for e in range(local):
            gb[e, pl.ds(a * cap, cap), :] = jnp.broadcast_to(cols_a[:, e:e + 1], (cap, LANES))

    arrived(wg, w_sem.at[0])
    arrived(wu, w_sem.at[1])
    for kcs in ((0,), (1,), (2,), (3,)):
        for kc in kcs:
            arrived(xr.at[near_rows, pl.ds(0, kw)], dx_rs.at[kc])
            if kc > 0:
                arrived(xr.at[pl.ds(0, 2 * cap), pl.ds(0, kw)], dq_rs.at[kc - 1])

        def up(e, carry, kcs=kcs):
            a = b = None
            for kc in kcs:
                cols = chunk(y_target(turn(kc, sign)))
                x = xr[:, cols]
                a_k = dot(x, wg[e, cols, :])
                b_k = dot(x, wu[e, cols, :])
                a = a_k if a is None else a + a_k
                b = b_k if b is None else b + b_k
            if kcs[0] > 0:
                a = a + acc_g[e]
                b = b + acc_u[e]
            if kcs[-1] < CHUNKS - 1:
                acc_g[e] = a
                acc_u[e] = b
            else:
                h = a * jax.nn.sigmoid(a) * b
                on = jnp.concatenate([gb[e]] * (h.shape[1] // LANES), axis=1) > 0.0
                hb[e] = jnp.where(on, h, 0.0).astype(BF16)
            return carry

        lax.fori_loop(0, local, up, 0, unroll=True)

    arrived(wd, w_sem.at[2])
    pairs = (tp + 1 - 2 * parity, y_target(tp_n - 1 + 2 * parity))
    group = slots // 2

    def span(u):
        return pl.ds(u * unit, unit)

    def mine(u):
        return pl.ds(pl.multiple_of(u * unit + parity * LANES, LANES), LANES)

    def theirs(u):
        return pl.ds(pl.multiple_of(u * unit + (1 - parity) * LANES, LANES), LANES)

    def packed(u):
        return pl.ds((u - STRAIGHT) * LANES, LANES)

    def down(u):
        cols = span(u)
        total = None
        for e in range(local):
            o = dot(hb[e], wd[e, :, cols]) * jnp.concatenate([gb[e]] * (unit // LANES), axis=1)
            total = o if total is None else total + o
        ob[:, cols] = total
        if u < STRAIGHT:
            for p in x_peers:
                to = x_target(p)
                send(ob.at[slots_of(to), cols], zr.at[my_slots, cols], out_sem.at[5], cx_rs.at[u], device(to, tp))
            zr[my_slots, cols] = ob[my_slots, cols]
        else:
            for g, to in enumerate(pairs):
                part = pl.ds(g * group, group)
                send(ob.at[part, theirs(u)], pr.at[part, packed(u)], out_sem.at[6], pr_rs.at[u], device(ep, to))

    def pair_sum(u):
        arrived(pr.at[:, packed(u)], pr_rs.at[u])
        zs[:, packed(u)] = ob[:, mine(u)] + pr[:, packed(u)]
        for p in x_peers:
            to = x_target(p)
            send(zs.at[slots_of(to), packed(u)], zr.at[my_slots, mine(u)], out_sem.at[5], cx_rs.at[u], device(to, tp))
        zr[my_slots, mine(u)] = zs[my_slots, packed(u)]

    def combine(u):
        cols, width = (span(u), unit) if u < STRAIGHT else (mine(u), LANES)
        arrived(zr.at[pl.ds(0, len(x_peers) * cap), pl.ds(0, width)], cx_rs.at[u])
        z1, z2, z3 = split3(zr[:, cols])
        pick = row_of[...]
        yb[:, cols] = dot(pick, z3) + dot(pick, z2) + dot(pick, z1)
        for dt in (2, 1, 3):
            to = y_target(dt)
            send(yb.at[rows_at(to, rows), cols], yr.at[dt - 1, :, cols], out_sem.at[7], cy_rs.at[u], device(ep, to))

    def finish(u):
        width = unit if u < STRAIGHT else LANES
        arrived(yr.at[:, :, pl.ds(0, width)], cy_rs.at[u])
        if u < STRAIGHT:
            cols = span(u)
            out_ref[:, cols] = (yb[my_rows, cols] + yr[0, :, cols] + yr[1, :, cols] + yr[2, :, cols]).astype(BF16)
        else:
            out_ref[:, mine(u)] = (yb[my_rows, mine(u)] + yr[1, :, mine(u)]).astype(BF16)
            out_ref[:, theirs(u)] = (yr[0, :, theirs(u)] + yr[2, :, theirs(u)]).astype(BF16)

    for u in (0, 2, 3, 1, 4, 5, 6, 7):
        down(u)
    for step, u in ((pair_sum, 2), (combine, 0), (pair_sum, 3), (pair_sum, 4), (combine, 1), (pair_sum, 5),
                    (combine, 2), (pair_sum, 6), (combine, 3), (pair_sum, 7), (combine, 4), (combine, 5),
                    (combine, 6), (combine, 7)):
        step(u)
    for u in range(units):
        finish(u)

    arrived(idg.at[pl.ds(0, others)], id_sem.at[0])
    arrived(gg.at[pl.ds(0, others)], id_sem.at[2])
    arrived(xg.at[pl.ds(0, others * rows)], out_sem.at[0])
    arrived(gr.at[pl.ds(0, len(x_peers))], out_sem.at[1])
    arrived(xs.at[pl.ds(0, 2 * cap), pl.ds(0, kw)], out_sem.at[2])
    arrived(xs.at[near_rows], out_sem.at[3])
    arrived(xs.at[pl.ds(0, others * 2 * cap), pl.ds(0, kw)], out_sem.at[4])
    paired = units - STRAIGHT
    sent = pl.ds(0, STRAIGHT * unit + paired * LANES)
    arrived(ob.at[pl.ds(0, len(x_peers) * cap), sent], out_sem.at[5])
    arrived(pr, out_sem.at[6])
    arrived(yr.at[:, :, sent], out_sem.at[7])


def solution(mesh):
    ep_n = mesh.shape['ep']
    tp_n = mesh.shape['tp']
    names = tuple(mesh.axis_names)

    def block(tok, ids, gates, w_gate, w_up, w_down):
        rows, d = tok.shape
        local, _, hid = w_gate.shape
        choices = ids.shape[1]
        shard_rows = rows * tp_n
        slots = 2 * shard_rows
        cap = slots // ep_n
        ny = tp_n - 1
        units = d // (2 * LANES)
        any_spec = pl.BlockSpec(memory_space=pl.ANY)
        dma = pltpu.SemaphoreType.DMA
        return pl.pallas_call(
            functools.partial(moe_kernel, names, ep_n, tp_n),
            out_shape=pltpu.VMEM((rows, d), BF16),
            in_specs=[any_spec] * 6,
            out_specs=pl.BlockSpec(memory_space=pltpu.VMEM),
            scratch_shapes=[
                pltpu.VMEM((local, d, hid), BF16),
                pltpu.VMEM((local, d, hid), BF16),
                pltpu.VMEM((local, hid, d), BF16),
                pltpu.VMEM((shard_rows, d), BF16),
                pltpu.VMEM((tp_n, choices, rows), jnp.int32),
                pltpu.VMEM((tp_n, choices, rows), F32),
                pltpu.VMEM((slots, d), BF16),
                pltpu.VMEM((ep_n * local, slots), F32),
                pltpu.VMEM((slots, d), BF16),
                pltpu.VMEM((ep_n, local, LANES), F32),
                pltpu.VMEM((local, slots, hid), F32),
                pltpu.VMEM((local, slots, hid), F32),
                pltpu.VMEM((local, slots, hid), BF16),
                pltpu.VMEM((local, slots, LANES), F32),
                pltpu.VMEM((slots, d), F32),
                pltpu.VMEM((slots, d), F32),
                pltpu.VMEM((shard_rows, d), F32),
                pltpu.VMEM((ny, rows, d), F32),
                pltpu.VMEM((slots, d // 2 - STRAIGHT * LANES), F32),
                pltpu.VMEM((slots, d // 2 - STRAIGHT * LANES), F32),
                pltpu.VMEM((slots, shard_rows), BF16),
                pltpu.VMEM((shard_rows, slots), BF16),
                pltpu.VMEM((LANES, LANES), F32),
                dma((3,)), dma((3,)), dma((4,)), dma((CHUNKS + 1,)), dma((1,)), dma((2,)), dma((CHUNKS,)), dma((ny,)),
                dma((units,)), dma((units,)), dma((units,)), dma((8,)),
            ],
            compiler_params=pltpu.CompilerParams(collective_id=0, has_side_effects=True,
                                                 vmem_limit_bytes=60 * 1024 * 1024),
        )(tok, ids.T, gates.T, w_gate, w_up, w_down)

    return jax.shard_map(
        block,
        mesh=mesh,
        in_specs=(P(TOKEN_AXES, None), P(TOKEN_AXES, None), P(TOKEN_AXES, None),
                  P('ep', None, 'tp'), P('ep', None, 'tp'), P('ep', 'tp', None)),
        out_specs=P(TOKEN_AXES, None),
        check_vma=False,
    )
```

```python
import functools

import jax
import jax.numpy as jnp
from jax import lax
from jax.experimental import pallas as pl
from jax.experimental.pallas import tpu as pltpu
from jax.sharding import PartitionSpec as P

TOKEN_AXES = ('dp', 'ep', 'tp')
LANES = 128
CHUNKS = 4
STRAIGHT = 2
F32 = jnp.float32
BF16 = jnp.bfloat16
MESH = pl.DeviceIdType.MESH


def split3(v):
    hi = v.astype(BF16)
    rest = v - hi.astype(F32)
    mid = rest.astype(BF16)
    low = (rest - mid.astype(F32)).astype(BF16)
    return hi, mid, low


def dot(a, b):
    return lax.dot_general(a, b, (((1,), (0,)), ((), ())), preferred_element_type=F32)


def dot_nt(a, b):
    return lax.dot_general(a, b, (((1,), (1,)), ((), ())), preferred_element_type=F32)


def arrived(ref, sem):
    pltpu.make_async_copy(ref, ref, sem).wait()


def moe_kernel(names, ep_n, tp_n, tok_hbm, ids_hbm, gate_hbm, wg_hbm, wu_hbm, wd_hbm, out_ref,
               wg, wu, wd, xg, idg, gg, xs, gs, xr, gr, acc_g, acc_u, hb, gb, ob, zr, yb, yr, pr, zs,
               slot_of, row_of, gcols,
               w_sem, in_sem, id_sem, ag_rs, dg_rs, df_rs, dx_rs, dq_rs, pr_rs, cx_rs, cy_rs, out_sem):
    rows, d = tok_hbm.shape
    local = wg_hbm.shape[0]
    choices = ids_hbm.shape[0]
    shard_rows = rows * tp_n
    cap = 2 * shard_rows // ep_n
    slots = cap * ep_n
    per_tile = LANES // cap
    kw = d // CHUNKS
    unit = 2 * LANES
    units = d // unit
    chips = ep_n // 2

    ep = lax.axis_index('ep')
    tp = lax.axis_index('tp')

    def device(ep_i, tp_i):
        at = {'dp': lax.axis_index('dp'), 'ep': ep_i, 'tp': tp_i}
        return tuple(at[n] for n in names)

    far = [(chips // 2, 0), (chips // 2, 1)]
    near = [(1, 0), (1, 1), (chips - 1, 0), (chips - 1, 1), (0, 1)]
    x_peers = far + near
    parity = lax.rem(tp, 2)
    sign = 1 - 2 * parity

    def turn(k, s):
        return (0, s, -s, 2)[k]

    peers = ((2, sign), (sign, -sign), (-sign, -sign))

    def x_target(p):
        return lax.rem(ep // 2 + p[0], chips) * 2 + lax.rem(ep + p[1], 2)

    def y_target(dt):
        return lax.rem(tp + dt + tp_n, tp_n)

    def send(src, dst, ss, rs, dev):
        pltpu.make_async_remote_copy(src_ref=src, dst_ref=dst, send_sem=ss, recv_sem=rs,
                                     device_id=dev, device_id_type=MESH).start()

    def rows_at(i, n):
        return pl.ds(pl.multiple_of(i * n, n), n)

    def slots_of(e):
        return rows_at(e, cap)

    def chunk(t):
        return pl.ds(pl.multiple_of(t * kw, kw), kw)

    def half(t, h):
        return pl.ds(pl.multiple_of(t * kw + h * (kw // 2), kw // 2), kw // 2)

    my_rows = rows_at(tp, rows)
    my_slots = slots_of(ep)
    far_slots = rows_at(lax.rem(ep // 2 + chips // 2, chips), 2 * cap)
    near_rows = pl.ds(0, len(near) * cap)
    others = tp_n - 1

    own = [pltpu.make_async_copy(ids_hbm, idg.at[tp], in_sem.at[0]),
           pltpu.make_async_copy(gate_hbm, gg.at[tp], in_sem.at[1]),
           pltpu.make_async_copy(tok_hbm, xg.at[my_rows], in_sem.at[2])]
    for c in own:
        c.start()

    bar = pltpu.get_barrier_semaphore()
    for dt in range(1, tp_n):
        pl.semaphore_signal(bar, inc=1, device_id=device(ep, y_target(dt)), device_id_type=MESH)
    for p in x_peers:
        pl.semaphore_signal(bar, inc=1, device_id=device(x_target(p), tp), device_id_type=MESH)
    for c in own:
        c.wait()
    pl.semaphore_wait(bar, others + len(x_peers))

    for dt in range(1, tp_n):
        dev = device(ep, y_target(dt))
        send(idg.at[tp], idg.at[tp], id_sem.at[0], id_sem.at[1], dev)
        send(gg.at[tp], gg.at[tp], id_sem.at[2], id_sem.at[3], dev)
    for h in range(2):
        for dt, _ in peers:
            part = xg.at[my_rows, half(y_target(dt), h)]
            send(part, part, out_sem.at[0], ag_rs.at[h], device(ep, y_target(dt)))
    for kc in range(1, CHUNKS):
        for dt, s in peers:
            part = xg.at[my_rows, chunk(y_target(dt + turn(kc, s)))]
            send(part, part, out_sem.at[0], ag_rs.at[kc + 1], device(ep, y_target(dt)))
    for i, (src, dst) in enumerate(((wg_hbm, wg), (wu_hbm, wu), (wd_hbm, wd))):
        for e in range(local):
            pltpu.make_async_copy(src.at[e], dst.at[e], w_sem.at[i]).start()
    arrived(idg.at[pl.ds(0, others)], id_sem.at[1])
    arrived(gg.at[pl.ds(0, others)], id_sem.at[3])

    ids = jnp.concatenate([idg[q] for q in range(tp_n)], axis=1)
    gates = jnp.concatenate([gg[q] for q in range(tp_n)], axis=1)
    b_iota = lax.broadcasted_iota(jnp.int32, (ep_n, shard_rows), 0)
    used = jnp.zeros((ep_n, shard_rows), F32)
    for j in range(choices):
        used = jnp.where(ids[j:j + 1, :] // local == b_iota, 1.0, used)
    before = (lax.broadcasted_iota(jnp.int32, (shard_rows, shard_rows), 0)
              < lax.broadcasted_iota(jnp.int32, (shard_rows, shard_rows), 1)).astype(F32).astype(BF16)
    rank = dot(used.astype(BF16), before)
    place = jnp.where(used > 0.0, rank, -1.0)
    in_slot = lax.broadcasted_iota(jnp.int32, (cap, shard_rows), 0).astype(F32)
    for b in range(ep_n):
        hit = jnp.where(place[b:b + 1, :] == in_slot, 1.0, 0.0)
        slot_of[pl.ds(b * cap, cap), :] = hit.astype(BF16)

    e_iota = lax.broadcasted_iota(jnp.int32, (ep_n * local, shard_rows), 0)
    gate_of = jnp.zeros((ep_n * local, shard_rows), F32)
    for j in range(choices):
        gate_of = jnp.where(ids[j:j + 1, :] == e_iota, gates[j:j + 1, :], gate_of)
    g1, g2, g3 = split3(gate_of)
    gs[...] = dot_nt(g3, slot_of[...]) + dot_nt(g2, slot_of[...]) + dot_nt(g1, slot_of[...])

    def gate_tile(b):
        return (rows_at(b, local), rows_at(b // per_tile, LANES))

    for p in x_peers:
        to = x_target(p)
        send(gs.at[gate_tile(to)], gr.at[ep], out_sem.at[1], dg_rs.at[0], device(to, tp))
    gr[ep] = gs[gate_tile(ep)]

    for h in range(2):
        cols = half(tp, h)
        arrived(xg.at[pl.ds(0, others * rows), pl.ds(0, kw // 2)], ag_rs.at[h])
        xs[:, cols] = dot(slot_of[...], xg[:, cols]).astype(BF16)
        for p in far:
            to = x_target(p)
            send(xs.at[slots_of(to), cols], xr.at[my_slots, cols], out_sem.at[2], df_rs.at[h], device(to, tp))
    def pack(kc):
        cols = chunk(y_target(turn(kc, sign)))
        if kc > 0:
            arrived(xg.at[pl.ds(0, others * rows), pl.ds(0, kw)], ag_rs.at[kc + 1])
            xs[:, cols] = dot(slot_of[...], xg[:, cols]).astype(BF16)
        for p in near:
            to = x_target(p)
            send(xs.at[slots_of(to), cols], xr.at[my_slots, cols], out_sem.at[3], dx_rs.at[kc], device(to, tp))
        xr[my_slots, cols] = xs[my_slots, cols]

    def spread(cols, ks):
        for k in ks:
            part = xr.at[far_slots, cols]
            send(part, part, out_sem.at[4], dq_rs.at[k - 1], device(ep, y_target(turn(k, sign))))

    for kc in range(CHUNKS):
        pack(kc)
    for h in range(2):
        arrived(xs.at[pl.ds(0, 2 * cap), pl.ds(0, kw // 2)], df_rs.at[h])
        spread(half(tp, h), (1, 2))
    spread(chunk(tp), (3,))
    row_of[...] = jnp.transpose(slot_of[...].astype(F32)).astype(BF16)

    arrived(gr.at[pl.ds(0, len(x_peers))], dg_rs.at[0])
    lanes_of_mine = rows_at(lax.rem(ep, per_tile), cap)
    for a in range(ep_n):
        gcols[...] = jnp.transpose(jnp.concatenate([gr[a]] * (LANES // local), axis=0))
        cols_a = gcols[lanes_of_mine, :]
        for e in range(local):
            gb[e, pl.ds(a * cap, cap), :] = jnp.broadcast_to(cols_a[:, e:e + 1], (cap, LANES))

    arrived(wg, w_sem.at[0])
    arrived(wu, w_sem.at[1])
    for kcs in ((0,), (1,), (2,), (3,)):
        for kc in kcs:
            arrived(xr.at[near_rows, pl.ds(0, kw)], dx_rs.at[kc])
            if kc > 0:
                arrived(xr.at[pl.ds(0, 2 * cap), pl.ds(0, kw)], dq_rs.at[kc - 1])

        def up(e, carry, kcs=kcs):
            a = b = None
            for kc in kcs:
                cols = chunk(y_target(turn(kc, sign)))
                x = xr[:, cols]
                a_k = dot(x, wg[e, cols, :])
                b_k = dot(x, wu[e, cols, :])
                a = a_k if a is None else a + a_k
                b = b_k if b is None else b + b_k
            if kcs[0] > 0:
                a = a + acc_g[e]
                b = b + acc_u[e]
            if kcs[-1] < CHUNKS - 1:
                acc_g[e] = a
                acc_u[e] = b
            else:
                h = a * jax.nn.sigmoid(a) * b
                on = jnp.concatenate([gb[e]] * (h.shape[1] // LANES), axis=1) > 0.0
                hb[e] = jnp.where(on, h, 0.0).astype(BF16)
            return carry

        lax.fori_loop(0, local, up, 0, unroll=True)

    arrived(wd, w_sem.at[2])
    pairs = (tp + 1 - 2 * parity, y_target(tp_n - 1 + 2 * parity))
    group = slots // 2

    def span(u):
        return pl.ds(u * unit, unit)

    def mine(u):
        return pl.ds(pl.multiple_of(u * unit + parity * LANES, LANES), LANES)

    def theirs(u):
        return pl.ds(pl.multiple_of(u * unit + (1 - parity) * LANES, LANES), LANES)

    def packed(u):
        return pl.ds((u - STRAIGHT) * LANES, LANES)

    def down(u):
        cols = span(u)
        total = None
        for e in range(local):
            o = dot(hb[e], wd[e, :, cols]) * jnp.concatenate([gb[e]] * (unit // LANES), axis=1)
            total = o if total is None else total + o
        ob[:, cols] = total
        if u < STRAIGHT:
            for p in x_peers:
                to = x_target(p)
                send(ob.at[slots_of(to), cols], zr.at[my_slots, cols], out_sem.at[5], cx_rs.at[u], device(to, tp))
            zr[my_slots, cols] = ob[my_slots, cols]
        else:
            for g, to in enumerate(pairs):
                part = pl.ds(g * group, group)
                send(ob.at[part, theirs(u)], pr.at[part, packed(u)], out_sem.at[6], pr_rs.at[u], device(ep, to))

    def pair_sum(u):
        arrived(pr.at[:, packed(u)], pr_rs.at[u])
        zs[:, packed(u)] = ob[:, mine(u)] + pr[:, packed(u)]
        for p in x_peers:
            to = x_target(p)
            send(zs.at[slots_of(to), packed(u)], zr.at[my_slots, mine(u)], out_sem.at[5], cx_rs.at[u], device(to, tp))
        zr[my_slots, mine(u)] = zs[my_slots, packed(u)]

    def combine(u):
        cols, width = (span(u), unit) if u < STRAIGHT else (mine(u), LANES)
        arrived(zr.at[pl.ds(0, len(x_peers) * cap), pl.ds(0, width)], cx_rs.at[u])
        z1, z2, z3 = split3(zr[:, cols])
        pick = row_of[...]
        yb[:, cols] = dot(pick, z3) + dot(pick, z2) + dot(pick, z1)
        for dt in (2, 1, 3):
            to = y_target(dt)
            send(yb.at[rows_at(to, rows), cols], yr.at[dt - 1, :, cols], out_sem.at[7], cy_rs.at[u], device(ep, to))

    def finish(u):
        width = unit if u < STRAIGHT else LANES
        arrived(yr.at[:, :, pl.ds(0, width)], cy_rs.at[u])
        if u < STRAIGHT:
            cols = span(u)
            out_ref[:, cols] = (yb[my_rows, cols] + yr[0, :, cols] + yr[1, :, cols] + yr[2, :, cols]).astype(BF16)
        else:
            out_ref[:, mine(u)] = (yb[my_rows, mine(u)] + yr[1, :, mine(u)]).astype(BF16)
            out_ref[:, theirs(u)] = (yr[0, :, theirs(u)] + yr[2, :, theirs(u)]).astype(BF16)

    for u in (0, 2, 3, 1, 4, 5, 6, 7):
        down(u)
    for step, u in ((pair_sum, 2), (pair_sum, 3), (combine, 0), (pair_sum, 4), (pair_sum, 5), (combine, 1),
                    (pair_sum, 6), (combine, 2), (pair_sum, 7), (combine, 3), (combine, 4), (combine, 5),
                    (combine, 6), (combine, 7)):
        step(u)
    for u in range(units):
        finish(u)

    arrived(idg.at[pl.ds(0, others)], id_sem.at[0])
    arrived(gg.at[pl.ds(0, others)], id_sem.at[2])
    arrived(xg.at[pl.ds(0, others * rows)], out_sem.at[0])
    arrived(gr.at[pl.ds(0, len(x_peers))], out_sem.at[1])
    arrived(xs.at[pl.ds(0, 2 * cap), pl.ds(0, kw)], out_sem.at[2])
    arrived(xs.at[near_rows], out_sem.at[3])
    arrived(xs.at[pl.ds(0, others * 2 * cap), pl.ds(0, kw)], out_sem.at[4])
    paired = units - STRAIGHT
    sent = pl.ds(0, STRAIGHT * unit + paired * LANES)
    arrived(ob.at[pl.ds(0, len(x_peers) * cap), sent], out_sem.at[5])
    arrived(pr, out_sem.at[6])
    arrived(yr.at[:, :, sent], out_sem.at[7])


def solution(mesh):
    ep_n = mesh.shape['ep']
    tp_n = mesh.shape['tp']
    names = tuple(mesh.axis_names)

    def block(tok, ids, gates, w_gate, w_up, w_down):
        rows, d = tok.shape
        local, _, hid = w_gate.shape
        choices = ids.shape[1]
        shard_rows = rows * tp_n
        slots = 2 * shard_rows
        cap = slots // ep_n
        ny = tp_n - 1
        units = d // (2 * LANES)
        any_spec = pl.BlockSpec(memory_space=pl.ANY)
        dma = pltpu.SemaphoreType.DMA
        return pl.pallas_call(
            functools.partial(moe_kernel, names, ep_n, tp_n),
            out_shape=pltpu.VMEM((rows, d), BF16),
            in_specs=[any_spec] * 6,
            out_specs=pl.BlockSpec(memory_space=pltpu.VMEM),
            scratch_shapes=[
                pltpu.VMEM((local, d, hid), BF16),
                pltpu.VMEM((local, d, hid), BF16),
                pltpu.VMEM((local, hid, d), BF16),
                pltpu.VMEM((shard_rows, d), BF16),
                pltpu.VMEM((tp_n, choices, rows), jnp.int32),
                pltpu.VMEM((tp_n, choices, rows), F32),
                pltpu.VMEM((slots, d), BF16),
                pltpu.VMEM((ep_n * local, slots), F32),
                pltpu.VMEM((slots, d), BF16),
                pltpu.VMEM((ep_n, local, LANES), F32),
                pltpu.VMEM((local, slots, hid), F32),
                pltpu.VMEM((local, slots, hid), F32),
                pltpu.VMEM((local, slots, hid), BF16),
                pltpu.VMEM((local, slots, LANES), F32),
                pltpu.VMEM((slots, d), F32),
                pltpu.VMEM((slots, d), F32),
                pltpu.VMEM((shard_rows, d), F32),
                pltpu.VMEM((ny, rows, d), F32),
                pltpu.VMEM((slots, d // 2 - STRAIGHT * LANES), F32),
                pltpu.VMEM((slots, d // 2 - STRAIGHT * LANES), F32),
                pltpu.VMEM((slots, shard_rows), BF16),
                pltpu.VMEM((shard_rows, slots), BF16),
                pltpu.VMEM((LANES, LANES), F32),
                dma((3,)), dma((3,)), dma((4,)), dma((CHUNKS + 1,)), dma((1,)), dma((2,)), dma((CHUNKS,)), dma((ny,)),
                dma((units,)), dma((units,)), dma((units,)), dma((8,)),
            ],
            compiler_params=pltpu.CompilerParams(collective_id=0, has_side_effects=True,
                                                 vmem_limit_bytes=60 * 1024 * 1024),
        )(tok, ids.T, gates.T, w_gate, w_up, w_down)

    return jax.shard_map(
        block,
        mesh=mesh,
        in_specs=(P(TOKEN_AXES, None), P(TOKEN_AXES, None), P(TOKEN_AXES, None),
                  P('ep', None, 'tp'), P('ep', None, 'tp'), P('ep', 'tp', None)),
        out_specs=P(TOKEN_AXES, None),
        check_vma=False,
    )
```

```python
import functools

import jax
import jax.numpy as jnp
from jax import lax
from jax.experimental import pallas as pl
from jax.experimental.pallas import tpu as pltpu
from jax.sharding import PartitionSpec as P

TOKEN_AXES = ('dp', 'ep', 'tp')
LANES = 128
CHUNKS = 4
STRAIGHT = 2
F32 = jnp.float32
BF16 = jnp.bfloat16
MESH = pl.DeviceIdType.MESH


def split3(v):
    hi = v.astype(BF16)
    rest = v - hi.astype(F32)
    mid = rest.astype(BF16)
    low = (rest - mid.astype(F32)).astype(BF16)
    return hi, mid, low


def dot(a, b):
    return lax.dot_general(a, b, (((1,), (0,)), ((), ())), preferred_element_type=F32)


def dot_nt(a, b):
    return lax.dot_general(a, b, (((1,), (1,)), ((), ())), preferred_element_type=F32)


def arrived(ref, sem):
    pltpu.make_async_copy(ref, ref, sem).wait()


def moe_kernel(names, ep_n, tp_n, tok_hbm, ids_hbm, gate_hbm, wg_hbm, wu_hbm, wd_hbm, out_ref,
               wg, wu, wd, xg, idg, gg, xs, gs, xr, gr, acc_g, acc_u, hb, gb, ob, zr, yb, yr, pr, zs,
               slot_of, row_of, gcols,
               w_sem, in_sem, id_sem, ag_rs, dg_rs, df_rs, dx_rs, dq_rs, pr_rs, cx_rs, cf_rs, cy_rs, out_sem):
    rows, d = tok_hbm.shape
    local = wg_hbm.shape[0]
    choices = ids_hbm.shape[0]
    shard_rows = rows * tp_n
    cap = 2 * shard_rows // ep_n
    slots = cap * ep_n
    per_tile = LANES // cap
    kw = d // CHUNKS
    unit = 2 * LANES
    units = d // unit
    chips = ep_n // 2

    ep = lax.axis_index('ep')
    tp = lax.axis_index('tp')

    def device(ep_i, tp_i):
        at = {'dp': lax.axis_index('dp'), 'ep': ep_i, 'tp': tp_i}
        return tuple(at[n] for n in names)

    far = [(chips // 2, 0), (chips // 2, 1)]
    near = [(1, 0), (1, 1), (chips - 1, 0), (chips - 1, 1), (0, 1)]
    x_peers = far + near
    parity = lax.rem(tp, 2)
    sign = 1 - 2 * parity

    def turn(k, s):
        return (0, s, -s, 2)[k]

    peers = ((2, sign), (sign, -sign), (-sign, -sign))

    def x_target(p):
        return lax.rem(ep // 2 + p[0], chips) * 2 + lax.rem(ep + p[1], 2)

    def y_target(dt):
        return lax.rem(tp + dt + tp_n, tp_n)

    def send(src, dst, ss, rs, dev):
        pltpu.make_async_remote_copy(src_ref=src, dst_ref=dst, send_sem=ss, recv_sem=rs,
                                     device_id=dev, device_id_type=MESH).start()

    def rows_at(i, n):
        return pl.ds(pl.multiple_of(i * n, n), n)

    def slots_of(e):
        return rows_at(e, cap)

    def chunk(t):
        return pl.ds(pl.multiple_of(t * kw, kw), kw)

    def half(t, h):
        return pl.ds(pl.multiple_of(t * kw + h * (kw // 2), kw // 2), kw // 2)

    my_rows = rows_at(tp, rows)
    my_slots = slots_of(ep)
    far_slots = rows_at(lax.rem(ep // 2 + chips // 2, chips), 2 * cap)
    near_rows = pl.ds(0, len(near) * cap)
    others = tp_n - 1

    own = [pltpu.make_async_copy(ids_hbm, idg.at[tp], in_sem.at[0]),
           pltpu.make_async_copy(gate_hbm, gg.at[tp], in_sem.at[1]),
           pltpu.make_async_copy(tok_hbm, xg.at[my_rows], in_sem.at[2])]
    for c in own:
        c.start()

    pairs = (tp + 1 - 2 * parity, y_target(tp_n - 1 + 2 * parity))

    def span(u):
        return pl.ds(u * unit, unit)

    def mine(u):
        return pl.ds(pl.multiple_of(u * unit + parity * LANES, LANES), LANES)

    def theirs(u):
        return pl.ds(pl.multiple_of(u * unit + (1 - parity) * LANES, LANES), LANES)

    def packed(u):
        return pl.ds(u * LANES, LANES)

    for u in range(STRAIGHT):
        zr[far_slots, theirs(u)] = jnp.zeros((2 * cap, LANES), F32)

    bar = pltpu.get_barrier_semaphore()
    for dt in range(1, tp_n):
        pl.semaphore_signal(bar, inc=1, device_id=device(ep, y_target(dt)), device_id_type=MESH)
    for p in x_peers:
        pl.semaphore_signal(bar, inc=1, device_id=device(x_target(p), tp), device_id_type=MESH)
    for c in own:
        c.wait()
    pl.semaphore_wait(bar, others + len(x_peers))

    for dt in range(1, tp_n):
        dev = device(ep, y_target(dt))
        send(idg.at[tp], idg.at[tp], id_sem.at[0], id_sem.at[1], dev)
        send(gg.at[tp], gg.at[tp], id_sem.at[2], id_sem.at[3], dev)
    for h in range(2):
        for dt, _ in peers:
            part = xg.at[my_rows, half(y_target(dt), h)]
            send(part, part, out_sem.at[0], ag_rs.at[h], device(ep, y_target(dt)))
    for kc in range(1, CHUNKS):
        for dt, s in peers:
            part = xg.at[my_rows, chunk(y_target(dt + turn(kc, s)))]
            send(part, part, out_sem.at[0], ag_rs.at[kc + 1], device(ep, y_target(dt)))
    for i, (src, dst) in enumerate(((wg_hbm, wg), (wu_hbm, wu), (wd_hbm, wd))):
        for e in range(local):
            pltpu.make_async_copy(src.at[e], dst.at[e], w_sem.at[i]).start()
    arrived(idg.at[pl.ds(0, others)], id_sem.at[1])
    arrived(gg.at[pl.ds(0, others)], id_sem.at[3])

    ids = jnp.concatenate([idg[q] for q in range(tp_n)], axis=1)
    gates = jnp.concatenate([gg[q] for q in range(tp_n)], axis=1)
    b_iota = lax.broadcasted_iota(jnp.int32, (ep_n, shard_rows), 0)
    used = jnp.zeros((ep_n, shard_rows), F32)
    for j in range(choices):
        used = jnp.where(ids[j:j + 1, :] // local == b_iota, 1.0, used)
    before = (lax.broadcasted_iota(jnp.int32, (shard_rows, shard_rows), 0)
              < lax.broadcasted_iota(jnp.int32, (shard_rows, shard_rows), 1)).astype(F32).astype(BF16)
    rank = dot(used.astype(BF16), before)
    place = jnp.where(used > 0.0, rank, -1.0)
    in_slot = lax.broadcasted_iota(jnp.int32, (cap, shard_rows), 0).astype(F32)
    for b in range(ep_n):
        hit = jnp.where(place[b:b + 1, :] == in_slot, 1.0, 0.0)
        slot_of[pl.ds(b * cap, cap), :] = hit.astype(BF16)

    e_iota = lax.broadcasted_iota(jnp.int32, (ep_n * local, shard_rows), 0)
    gate_of = jnp.zeros((ep_n * local, shard_rows), F32)
    for j in range(choices):
        gate_of = jnp.where(ids[j:j + 1, :] == e_iota, gates[j:j + 1, :], gate_of)
    g1, g2, g3 = split3(gate_of)
    gs[...] = dot_nt(g3, slot_of[...]) + dot_nt(g2, slot_of[...]) + dot_nt(g1, slot_of[...])

    def gate_tile(b):
        return (rows_at(b, local), rows_at(b // per_tile, LANES))

    for p in x_peers:
        to = x_target(p)
        send(gs.at[gate_tile(to)], gr.at[ep], out_sem.at[1], dg_rs.at[0], device(to, tp))
    gr[ep] = gs[gate_tile(ep)]

    for h in range(2):
        cols = half(tp, h)
        arrived(xg.at[pl.ds(0, others * rows), pl.ds(0, kw // 2)], ag_rs.at[h])
        xs[:, cols] = dot(slot_of[...], xg[:, cols]).astype(BF16)
        for p in far:
            to = x_target(p)
            send(xs.at[slots_of(to), cols], xr.at[my_slots, cols], out_sem.at[2], df_rs.at[h], device(to, tp))
    def pack(kc):
        cols = chunk(y_target(turn(kc, sign)))
        if kc > 0:
            arrived(xg.at[pl.ds(0, others * rows), pl.ds(0, kw)], ag_rs.at[kc + 1])
            xs[:, cols] = dot(slot_of[...], xg[:, cols]).astype(BF16)
        for p in near:
            to = x_target(p)
            send(xs.at[slots_of(to), cols], xr.at[my_slots, cols], out_sem.at[3], dx_rs.at[kc], device(to, tp))
        xr[my_slots, cols] = xs[my_slots, cols]

    def spread(cols, ks):
        for k in ks:
            part = xr.at[far_slots, cols]
            send(part, part, out_sem.at[4], dq_rs.at[k - 1], device(ep, y_target(turn(k, sign))))

    for kc in range(CHUNKS):
        pack(kc)
    for h in range(2):
        arrived(xs.at[pl.ds(0, 2 * cap), pl.ds(0, kw // 2)], df_rs.at[h])
        spread(half(tp, h), (1, 2))
    spread(chunk(tp), (3,))
    row_of[...] = jnp.transpose(slot_of[...].astype(F32)).astype(BF16)

    arrived(gr.at[pl.ds(0, len(x_peers))], dg_rs.at[0])
    lanes_of_mine = rows_at(lax.rem(ep, per_tile), cap)
    for a in range(ep_n):
        gcols[...] = jnp.transpose(jnp.concatenate([gr[a]] * (LANES // local), axis=0))
        cols_a = gcols[lanes_of_mine, :]
        for e in range(local):
            gb[e, pl.ds(a * cap, cap), :] = jnp.broadcast_to(cols_a[:, e:e + 1], (cap, LANES))

    arrived(wg, w_sem.at[0])
    arrived(wu, w_sem.at[1])
    for kcs in ((0,), (1,), (2,), (3,)):
        for kc in kcs:
            arrived(xr.at[near_rows, pl.ds(0, kw)], dx_rs.at[kc])
            if kc > 0:
                arrived(xr.at[pl.ds(0, 2 * cap), pl.ds(0, kw)], dq_rs.at[kc - 1])

        def up(e, carry, kcs=kcs):
            a = b = None
            for kc in kcs:
                cols = chunk(y_target(turn(kc, sign)))
                x = xr[:, cols]
                a_k = dot(x, wg[e, cols, :])
                b_k = dot(x, wu[e, cols, :])
                a = a_k if a is None else a + a_k
                b = b_k if b is None else b + b_k
            if kcs[0] > 0:
                a = a + acc_g[e]
                b = b + acc_u[e]
            if kcs[-1] < CHUNKS - 1:
                acc_g[e] = a
                acc_u[e] = b
            else:
                h = a * jax.nn.sigmoid(a) * b
                on = jnp.concatenate([gb[e]] * (h.shape[1] // LANES), axis=1) > 0.0
                hb[e] = jnp.where(on, h, 0.0).astype(BF16)
            return carry

        lax.fori_loop(0, local, up, 0, unroll=True)

    arrived(wd, w_sem.at[2])
    group = slots // 2

    def down(u):
        cols = span(u)
        total = None
        for e in range(local):
            o = dot(hb[e], wd[e, :, cols]) * jnp.concatenate([gb[e]] * (unit // LANES), axis=1)
            total = o if total is None else total + o
        ob[:, cols] = total
        if u < STRAIGHT:
            for p in near:
                to = x_target(p)
                send(ob.at[slots_of(to), cols], zr.at[my_slots, cols], out_sem.at[5], cx_rs.at[u], device(to, tp))
            for p, to in zip(far, pairs):
                part = slots_of(x_target(p))
                send(ob.at[part, theirs(u)], pr.at[part, packed(u)], out_sem.at[8], pr_rs.at[u], device(ep, to))
            zr[my_slots, cols] = ob[my_slots, cols]
        else:
            for g, to in enumerate(pairs):
                part = pl.ds(g * group, group)
                send(ob.at[part, theirs(u)], pr.at[part, packed(u)], out_sem.at[6], pr_rs.at[u], device(ep, to))

    def far_sum(u):
        arrived(pr.at[pl.ds(0, 2 * cap), packed(u)], pr_rs.at[u])
        for p in far:
            to = x_target(p)
            zs[slots_of(to), packed(u)] = ob[slots_of(to), mine(u)] + pr[slots_of(to), packed(u)]
            send(zs.at[slots_of(to), packed(u)], zr.at[my_slots, mine(u)], out_sem.at[9], cf_rs.at[u], device(to, tp))

    def pair_sum(u):
        arrived(pr.at[:, packed(u)], pr_rs.at[u])
        zs[:, packed(u)] = ob[:, mine(u)] + pr[:, packed(u)]
        for p in x_peers:
            to = x_target(p)
            send(zs.at[slots_of(to), packed(u)], zr.at[my_slots, mine(u)], out_sem.at[10], cx_rs.at[u], device(to, tp))
        zr[my_slots, mine(u)] = zs[my_slots, packed(u)]

    def combine(u):
        cols = span(u) if u < STRAIGHT else mine(u)
        if u < STRAIGHT:
            arrived(zr.at[near_rows, pl.ds(0, unit)], cx_rs.at[u])
            arrived(zr.at[pl.ds(0, 2 * cap), pl.ds(0, LANES)], cf_rs.at[u])
        else:
            arrived(zr.at[pl.ds(0, len(x_peers) * cap), pl.ds(0, LANES)], cx_rs.at[u])
        z1, z2, z3 = split3(zr[:, cols])
        pick = row_of[...]
        yb[:, cols] = dot(pick, z3) + dot(pick, z2) + dot(pick, z1)
        for dt in (2, 1, 3):
            to = y_target(dt)
            send(yb.at[rows_at(to, rows), cols], yr.at[dt - 1, :, cols], out_sem.at[7], cy_rs.at[u], device(ep, to))

    def finish(u):
        width = unit if u < STRAIGHT else LANES
        arrived(yr.at[:, :, pl.ds(0, width)], cy_rs.at[u])
        if u < STRAIGHT:
            cols = span(u)
            out_ref[:, cols] = (yb[my_rows, cols] + yr[0, :, cols] + yr[1, :, cols] + yr[2, :, cols]).astype(BF16)
        else:
            out_ref[:, mine(u)] = (yb[my_rows, mine(u)] + yr[1, :, mine(u)]).astype(BF16)
            out_ref[:, theirs(u)] = (yr[0, :, theirs(u)] + yr[2, :, theirs(u)]).astype(BF16)

    for u in (0, 2, 3, 1, 4, 5, 6, 7):
        down(u)
    for step, u in ((far_sum, 0), (pair_sum, 2), (pair_sum, 3), (far_sum, 1), (combine, 0), (pair_sum, 4),
                    (pair_sum, 5), (combine, 1), (pair_sum, 6), (combine, 2), (pair_sum, 7), (combine, 3),
                    (combine, 4), (combine, 5), (combine, 6), (combine, 7)):
        step(u)
    for u in range(units):
        finish(u)

    arrived(idg.at[pl.ds(0, others)], id_sem.at[0])
    arrived(gg.at[pl.ds(0, others)], id_sem.at[2])
    arrived(xg.at[pl.ds(0, others * rows)], out_sem.at[0])
    arrived(gr.at[pl.ds(0, len(x_peers))], out_sem.at[1])
    arrived(xs.at[pl.ds(0, 2 * cap), pl.ds(0, kw)], out_sem.at[2])
    arrived(xs.at[near_rows], out_sem.at[3])
    arrived(xs.at[pl.ds(0, others * 2 * cap), pl.ds(0, kw)], out_sem.at[4])
    paired = units - STRAIGHT
    sent = pl.ds(0, STRAIGHT * unit + paired * LANES)
    arrived(ob.at[near_rows, pl.ds(0, STRAIGHT * unit)], out_sem.at[5])
    arrived(pr.at[:, pl.ds(0, paired * LANES)], out_sem.at[6])
    arrived(pr.at[pl.ds(0, 2 * cap), pl.ds(0, STRAIGHT * LANES)], out_sem.at[8])
    arrived(pr.at[pl.ds(0, 2 * cap), pl.ds(0, STRAIGHT * LANES)], out_sem.at[9])
    arrived(ob.at[pl.ds(0, len(x_peers) * cap), pl.ds(0, paired * LANES)], out_sem.at[10])
    arrived(yr.at[:, :, sent], out_sem.at[7])


def solution(mesh):
    ep_n = mesh.shape['ep']
    tp_n = mesh.shape['tp']
    names = tuple(mesh.axis_names)

    def block(tok, ids, gates, w_gate, w_up, w_down):
        rows, d = tok.shape
        local, _, hid = w_gate.shape
        choices = ids.shape[1]
        shard_rows = rows * tp_n
        slots = 2 * shard_rows
        cap = slots // ep_n
        ny = tp_n - 1
        units = d // (2 * LANES)
        any_spec = pl.BlockSpec(memory_space=pl.ANY)
        dma = pltpu.SemaphoreType.DMA
        return pl.pallas_call(
            functools.partial(moe_kernel, names, ep_n, tp_n),
            out_shape=pltpu.VMEM((rows, d), BF16),
            in_specs=[any_spec] * 6,
            out_specs=pl.BlockSpec(memory_space=pltpu.VMEM),
            scratch_shapes=[
                pltpu.VMEM((local, d, hid), BF16),
                pltpu.VMEM((local, d, hid), BF16),
                pltpu.VMEM((local, hid, d), BF16),
                pltpu.VMEM((shard_rows, d), BF16),
                pltpu.VMEM((tp_n, choices, rows), jnp.int32),
                pltpu.VMEM((tp_n, choices, rows), F32),
                pltpu.VMEM((slots, d), BF16),
                pltpu.VMEM((ep_n * local, slots), F32),
                pltpu.VMEM((slots, d), BF16),
                pltpu.VMEM((ep_n, local, LANES), F32),
                pltpu.VMEM((local, slots, hid), F32),
                pltpu.VMEM((local, slots, hid), F32),
                pltpu.VMEM((local, slots, hid), BF16),
                pltpu.VMEM((local, slots, LANES), F32),
                pltpu.VMEM((slots, d), F32),
                pltpu.VMEM((slots, d), F32),
                pltpu.VMEM((shard_rows, d), F32),
                pltpu.VMEM((ny, rows, d), F32),
                pltpu.VMEM((slots, d // 2), F32),
                pltpu.VMEM((slots, d // 2), F32),
                pltpu.VMEM((slots, shard_rows), BF16),
                pltpu.VMEM((shard_rows, slots), BF16),
                pltpu.VMEM((LANES, LANES), F32),
                dma((3,)), dma((3,)), dma((4,)), dma((CHUNKS + 1,)), dma((1,)), dma((2,)), dma((CHUNKS,)), dma((ny,)),
                dma((units,)), dma((units,)), dma((STRAIGHT,)), dma((units,)), dma((11,)),
            ],
            compiler_params=pltpu.CompilerParams(collective_id=0, has_side_effects=True,
                                                 vmem_limit_bytes=60 * 1024 * 1024),
        )(tok, ids.T, gates.T, w_gate, w_up, w_down)

    return jax.shard_map(
        block,
        mesh=mesh,
        in_specs=(P(TOKEN_AXES, None), P(TOKEN_AXES, None), P(TOKEN_AXES, None),
                  P('ep', None, 'tp'), P('ep', None, 'tp'), P('ep', 'tp', None)),
        out_specs=P(TOKEN_AXES, None),
        check_vma=False,
    )
```
